32 devices in a mesh: stn: 8 (over z, x), pts: 2 (over core), freq: 2 (over y).
Axes of the slice: x: 2, y: 2, z: 4, core: 2. Of those that a mesh axis runs over, the one named last changes fastest.
Arguments:
- greens: bfloat16 [2, 4, 2048, 4096], P(None, 'freq', 'stn', 'pts'), may hold values from -6 to 6
- noise_weights: bfloat16 [2, 4, 2048, 2048], P(None, 'freq', 'stn'), may hold values from -12 to 12, as said below
Outputs:
- kernel: float32 [4096], P('pts')
The draws below stay inside these ranges and needn't reach their ends.
Inputs may be any that keep to these rules, and one draw needn't show every extreme that they name: For every frequency, noise_weights[0] is symmetric and noise_weights[1] antisymmetric in the two station dimensions, so each frequency's matrix is Hermitian.
All inputs are finite; a program needn't handle non-finite values. Where the reference program divides by a largest or mean magnitude, that divisor is 1e-20 or more.
Results may differ from the reference program's by a relative error of at most 0.0003.
Values may be sent and summed in bfloat16 or wider, within the bound.
A program may use at most 192 MiB of HBM per device.

```python
import jax
import jax.numpy as jnp
from jax import lax

S = 2048
F = 4
P_SIZE = 4096


def draw_noise_weights(key, part):
    base = jax.random.fold_in(key, 11)
    key_real, key_imag = jax.random.split(base, 2)
    rough_real = jax.random.truncated_normal(key_real, -4.0, 4.0, (F, S, S), jnp.float32) * 0.5
    rough_imag = jax.random.truncated_normal(key_imag, -4.0, 4.0, (F, S, S), jnp.float32) * 0.5
    symmetric = (rough_real + jnp.swapaxes(rough_real, 1, 2)) * 0.7071
    antisymmetric = (rough_imag - jnp.swapaxes(rough_imag, 1, 2)) * 0.7071
    return jnp.stack([symmetric, antisymmetric]).astype(jnp.bfloat16)


def levels(own_key, shape, shards, least, high):
    def one(position, blocks):
        steps = jax.random.uniform(jax.random.fold_in(jax.random.fold_in(own_key, 6), position), (blocks,), jnp.float32, least / len(shards), high / len(shards))
        return jnp.repeat(jnp.exp(steps), shape[position] // blocks).reshape((-1,) + (1,) * (len(shape) - position - 1))

    factor_of = one(*shards[0])
    for cut in shards[1:]:
        factor_of = factor_of * one(*cut)
    return factor_of


def noise(key, dims, deviation, most, pieces=(), kind=jnp.bfloat16):
    level = levels(key, dims, pieces, -0.22, 0.18) if pieces else 1.0
    result = jax.random.normal(key, dims, jnp.float32) * deviation * level
    return jnp.minimum(jnp.maximum(result, -most), most).astype(kind)


def setup_inputs(seed: int = 0) -> dict:
    seeds = jax.random.split(jax.random.key(seed), 3)
    greens = noise(seeds[0], (2, F, S, P_SIZE), 1.0, 6.0, ((1, 2), (2, 8), (3, 2)))
    noise_weights = draw_noise_weights(jax.random.fold_in(seeds[2], 71), 0)
    return {"greens": greens, "noise_weights": noise_weights}


def per_frequency(operands):
    green_block, weight_block = operands
    product_real = jnp.dot(weight_block[0], green_block[0], preferred_element_type=jnp.float32) - jnp.dot(weight_block[1], green_block[1], preferred_element_type=jnp.float32)
    product_imag = jnp.dot(weight_block[0], green_block[1], preferred_element_type=jnp.float32) + jnp.dot(weight_block[1], green_block[0], preferred_element_type=jnp.float32)
    green_real = green_block[0].astype(jnp.float32)
    green_imag = green_block[1].astype(jnp.float32)
    return jnp.sum(green_real * product_real + green_imag * product_imag, axis=0)


def reference(greens, noise_weights):
    stacked = lax.map(per_frequency, (jnp.moveaxis(greens, 1, 0), jnp.moveaxis(noise_weights, 1, 0)))
    raw_kernel = jnp.sum(stacked, axis=0) / S
    largest = jnp.max(jnp.abs(raw_kernel))
    return raw_kernel / (largest + 1e-6)
```

```python
import functools

import jax
import jax.numpy as jnp
from jax import lax
from jax.experimental import pallas as pl
from jax.experimental.pallas import tpu as pltpu
from jax.sharding import PartitionSpec as P

MESH = pl.DeviceIdType.MESH
LANES = 128


def remote(src, dst, send_sem, recv_sem, target):
    return pltpu.make_async_remote_copy(
        src_ref=src, dst_ref=dst, send_sem=send_sem, recv_sem=recv_sem,
        device_id=target, device_id_type=MESH,
    )


def ring_kernel(
    n, n_freq, h, stations, chunk, nq, blocked,
    greens, weights, out,
    g_own, g_pair, near, far, w_own, w_pair, acc, red, max_out, max_in,
    own_sem, w_own_sem, pair_send, pair_recv, wp_send, wp_recv, sib_sem,
    in_send, in_recv, out_send, far_recv, red_send, red_recv, max_sem, hello_sem, pair_hello,
):
    m = n // 2
    side_len = m // 2
    sub = chunk // LANES
    half_rows = h // 2
    me = lax.axis_index("stn")
    core = lax.axis_index("pts")
    fq = lax.axis_index("freq")
    parity = lax.rem(me, 2)
    z = me // 2
    hi = (z >= side_len).astype(jnp.int32)
    edge = jnp.where(hi == 1, m - 1 - z, z)
    inward = jnp.where(hi == 1, -2, 2)
    inner = edge == side_len - 1
    s_base = hi * nq
    r_base = (1 - hi) * nq
    pair_dev = {"stn": me + 1 - 2 * parity}
    in_dev = {"stn": me + inward}
    out_dev = {"stn": me - inward}
    n_far = side_len * 2 * nq
    n_near = edge * 4 * nq
    n_near_max = (side_len - 1) * 4 * nq
    steps = max(n_far, n_near_max, 3 * nq + 2)
    spread = side_len == 2
    catch_up = 2 * nq + 1 if spread else max((steps * 25) // 32, 3 * nq + 1)
    left = steps - catch_up
    per_step = -(-steps // (steps - catch_up))

    def columns(q):
        return pl.ds(pl.multiple_of(q * chunk, LANES), chunk)

    def w_src(freq, j, rows):
        if blocked:
            return weights.at[:, freq, j, rows, :]
        return weights.at[:, freq, rows, pl.ds(pl.multiple_of(j * h, LANES), h)]

    def global_block(e, opposite):
        low = jnp.where(opposite, 1 - hi, hi) == 0
        return jnp.where(low, e, m - 1 - e)

    def near_slot(receiver_edge, p, half, b, c):
        return ((p * 2 + half) * receiver_edge + (receiver_edge - 1 - b)) * nq + c

    def far_slot(p, b, c):
        return (p * side_len + (side_len - 1 - b)) * nq + c

    def send_inward(src, p, half, b, c):
        q = jnp.where(half == 0, s_base, r_base) + c

        if side_len > 1:
            @pl.when(jnp.logical_not(inner))
            def _():
                slot = near_slot(edge + 1, p, half, b, c)
                remote(src, near.at[b, p, q], in_send.at[slot], in_recv.at[slot], in_dev).start()

        @pl.when(jnp.logical_and(inner, half == 0))
        def _():
            slot = far_slot(p, b, c)
            remote(src, far.at[b, p, c], in_send.at[slot], far_recv.at[slot], in_dev).start()

    freq_dev = {"freq": n_freq - 1 - fq}
    barrier = pltpu.get_barrier_semaphore()
    up, down = z < m - 1, z > 0
    greeted = [pair_dev, {"pts": 1 - core}, freq_dev]

    def greet(sem, device):
        pl.semaphore_signal(sem, inc=1, device_id=device, device_id_type=MESH)

    def along_z(sem_down, sem_up):
        @pl.when(up)
        def _():
            greet(sem_up, {"stn": me + 2})

        @pl.when(down)
        def _():
            greet(sem_down, {"stn": me - 2})

    for device in greeted:
        greet(barrier, device)
    along_z(barrier, barrier)
    pl.semaphore_wait(barrier, len(greeted) + up.astype(jnp.int32) + down.astype(jnp.int32))

    def hello():
        @pl.loop(0, m - 1)
        def _(r):
            along_z(hello_sem.at[0, r], hello_sem.at[1, r])

            @pl.when(up)
            def _():
                pl.semaphore_wait(hello_sem.at[0, r], 1)

            @pl.when(down)
            def _():
                pl.semaphore_wait(hello_sem.at[1, r], 1)

        for i, device in enumerate((pair_dev, freq_dev)):
            greet(pair_hello.at[i], device)
            pl.semaphore_wait(pair_hello.at[i], 1)

    every_row = pl.ds(0, h)
    pair_rows = pl.ds(pl.multiple_of(core * half_rows, 8), half_rows)

    def pair_q(i):
        return jnp.where(i < nq, s_base + i, r_base + i - nq)

    def pair_copy(i):
        q = pair_q(i)
        return remote(
            greens.at[:, 1 - parity, :, columns(q)], g_pair.at[q],
            pair_send.at[i], pair_recv.at[i], pair_dev,
        )

    def w_pair_copy(j):
        return remote(
            w_src(1 - parity, j, pair_rows), w_pair.at[j, :, pair_rows, :],
            wp_send.at[j], wp_recv.at[j], pair_dev,
        )

    def sibling_copy(rows):
        return remote(
            w_pair.at[:, :, rows, :], w_pair.at[:, :, rows, :],
            sib_sem.at[0], sib_sem.at[1], {"pts": 1 - core},
        )

    def own_copy(q):
        return pltpu.make_async_copy(
            greens.at[:, parity, :, columns(q)], g_own.at[q], own_sem.at[q]
        )

    def w_own_copy(j):
        return pltpu.make_async_copy(w_src(parity, j, every_row), w_own.at[j], w_own_sem.at[j])

    @pl.loop(0, 2 * nq)
    def _(i):
        @pl.when(i < nq)
        def _():
            pair_copy(i).start()

        half = i // nq
        c = lax.rem(i, nq)
        send_inward(greens.at[:, parity, :, columns(pair_q(i))], 0, half, edge, c)
        own_copy(i).start()

    @pl.loop(0, n)
    def _(j):
        w_pair_copy(j).start()
        w_own_copy(j).start()

    @pl.loop(nq, 2 * nq)
    def _(i):
        pair_copy(i).start()

    hello()

    acc[...] = jnp.zeros_like(acc)

    @pl.loop(0, 2 * nq)
    def _(q):
        own_copy(q).wait()

    @pl.loop(0, n)
    def _(j):
        w_own_copy(j).wait()

    def contribute(w, gi, gj, q, weight):
        for s in range(sub):
            part = slice(s * LANES, (s + 1) * LANES)
            both = jnp.concatenate([gj[0, :, part], gj[1, :, part]], axis=1)
            ab = jnp.dot(w[...].reshape(2 * h, h), both, preferred_element_type=jnp.float32)
            a, b = ab[:h], ab[h:]
            t = gi[0, :, part].astype(jnp.float32) * (a[:, :LANES] - b[:, LANES:])
            t = t + gi[1, :, part].astype(jnp.float32) * (a[:, LANES:] + b[:, :LANES])
            t = jnp.sum(t.reshape(h // 8, 8, LANES), axis=0)
            acc[q * sub + s] += t * weight

    def far_at(t):
        p = t // (side_len * nq)
        rest = lax.rem(t, side_len * nq)
        return p, side_len - 1 - rest // nq, lax.rem(rest, nq)

    def near_at(t):
        width = jnp.maximum(edge, 1) * nq
        p = t // (2 * width)
        half = lax.rem(t // width, 2)
        rest = lax.rem(t, width)
        return p, half, jnp.maximum(edge, 1) - 1 - rest // nq, lax.rem(rest, nq)

    def part_of(p):
        return jnp.where(p == 0, parity, 1 - parity)

    def far_work(t, w, g):
        p, b, c = far_at(t)
        q = r_base + c
        j = global_block(b, True) * 2 + part_of(p)
        contribute(w.at[j], g.at[q], far.at[b, p, c], q, 2.0)

    def near_work(t, w, g):
        p, half, b, c = near_at(t)
        q = jnp.where(half == 0, s_base, r_base) + c
        j = global_block(b, False) * 2 + part_of(p)
        contribute(w.at[j], g.at[q], near.at[b, p, q], q, 2.0)

    def far_wait(t):
        p, b, c = far_at(t)
        ref = far.at[b, p, c]
        remote(ref, ref, out_send.at[t], far_recv.at[t], in_dev).wait_recv()

        @pl.when(edge > 0)
        def _():
            remote(ref, ref, out_send.at[t], far_recv.at[t], out_dev).start()

    def near_wait(t):
        p, half, b, c = near_at(t)
        q = jnp.where(half == 0, s_base, r_base) + c
        ref = near.at[b, p, q]
        remote(ref, ref, in_send.at[t], in_recv.at[t], out_dev).wait_recv()
        send_inward(ref, p, half, b, c)

    def newest(u):
        far_work(u, w_pair, g_pair)

        @pl.when(u < n_near)
        def _():
            near_work(u, w_pair, g_pair)

    @pl.loop(0, steps)
    def _(t):
        has_pair = jnp.logical_and(jnp.logical_and(t >= nq, t <= 3 * nq), t != 2 * nq)
        turn = t - nq - (t > 2 * nq).astype(jnp.int32)

        @pl.when(has_pair)
        def _():
            i = turn
            pair_copy(i).wait_recv()
            send_inward(g_pair.at[pair_q(i)], 1, i // nq, edge, lax.rem(i, nq))

        @pl.when(t < n_far)
        def _():
            far_wait(t)

        if side_len > 1:
            @pl.when(t < n_near)
            def _():
                near_wait(t)

        @pl.when(t == catch_up - 1)
        def _():
            @pl.loop(0, n)
            def _(j):
                w_pair_copy(j).wait_recv()

            sibling_copy(pair_rows).start()

        @pl.when(t < 2 * nq)
        def _():
            contribute(w_own.at[2 * z + parity], g_own.at[t], g_own.at[t], t, 1.0)

        @pl.when(has_pair)
        def _():
            q = pair_q(turn)
            contribute(w_own.at[2 * z + 1 - parity], g_own.at[q], g_pair.at[q], q, 2.0)

        @pl.when(t < n_far)
        def _():
            far_work(t, w_own, g_own)

        if side_len > 1:
            @pl.when(t < n_near)
            def _():
                near_work(t, w_own, g_own)

        @pl.when(t == catch_up)
        def _():
            sibling_copy(pl.ds(pl.multiple_of((1 - core) * half_rows, 8), half_rows)).wait_recv()

        @pl.when(t >= catch_up)
        def _():
            first = (t - catch_up) * per_step
            last = jnp.minimum(first + per_step, steps)
            if spread:
                first = ((t - catch_up) * 2 * nq) // left
                last = ((t - catch_up + 1) * 2 * nq) // left

            @pl.loop(first, last)
            def _(u):
                @pl.when(u < 2 * nq)
                def _():
                    q = pair_q(u)
                    contribute(w_pair.at[2 * z + 1 - parity], g_pair.at[q], g_pair.at[q], q, 1.0)

                if spread:
                    far_work(lax.rem(u, side_len) * nq + u // side_len, w_pair, g_pair)
                else:
                    @pl.when(u < n_far)
                    def _():
                        far_work(u, w_pair, g_pair)

                if side_len > 1:
                    @pl.when(u < n_near)
                    def _():
                        near_work(u, w_pair, g_pair)

            if spread:
                newest(t - 1)

    if spread:
        newest(steps - 1)

    total = n * n_freq
    rank = me * n_freq + fq
    red[rank] = jnp.sum(acc[...], axis=1) / stations

    def share_copy(k, source):
        target = lax.rem(rank + k, total)
        return remote(
            red.at[source], red.at[source], red_send.at[k - 1], red_recv.at[k - 1],
            {"stn": target // n_freq, "freq": lax.rem(target, n_freq)},
        )

    @pl.loop(1, total)
    def _(k):
        share_copy(k, rank).start()

    @pl.loop(1, total)
    def _(k):
        share_copy(k, lax.rem(rank - k + total, total)).wait_recv()

    raw = red[0]
    for d in range(1, total):
        raw = raw + red[d]
    max_out[...] = jnp.broadcast_to(jnp.max(jnp.abs(raw)), max_out.shape)
    max_copy = remote(max_out, max_in, max_sem.at[0], max_sem.at[1], {"pts": 1 - core})
    max_copy.start()

    @pl.loop(1, total)
    def _(k):
        share_copy(k, rank).wait_send()

    @pl.loop(0, 2 * nq)
    def _(i):
        pair_copy(i).wait_send()

    @pl.loop(0, n)
    def _(j):
        w_pair_copy(j).wait_send()

    sibling_copy(pair_rows).wait_send()
    ref = far.at[0, 0, 0]

    @pl.loop(0, jnp.where(inner, n_far, (edge + 1) * 4 * nq))
    def _(t):
        remote(ref, ref, in_send.at[t], far_recv.at[0], in_dev).wait_send()

    @pl.when(edge > 0)
    def _():
        @pl.loop(0, n_far)
        def _(t):
            remote(ref, ref, out_send.at[t], far_recv.at[0], out_dev).wait_send()

    max_copy.wait()
    largest = jnp.maximum(max_out[0:1, 0:1], max_in[0:1, 0:1])
    out[...] = raw / (largest + 1e-6)


def kernel_body(n, n_freq, greens, weights):
    _, _, h, points = greens.shape
    stations = weights.shape[3]
    half = points // 2
    chunk = LANES
    while chunk * 2 * h <= 32768 and half % (chunk * 2) == 0:
        chunk *= 2
    nq = half // chunk
    side_len = n // 4
    n_far = side_len * 2 * nq
    n_near = max(side_len - 1, 1) * 4 * nq
    blocked = h % LANES != 0
    if blocked:
        weights = weights.reshape(2, weights.shape[1], h, n, h).swapaxes(2, 3)
    if side_len == 2 and nq >= 4:
        return line_body(n_freq, chunk, nq, blocked, greens, weights)
    dma = pltpu.SemaphoreType.DMA
    bf16, f32 = jnp.bfloat16, jnp.float32
    rows = points // LANES
    out = pl.pallas_call(
        functools.partial(ring_kernel, n, n_freq, h, stations, chunk, nq, blocked),
        out_shape=jax.ShapeDtypeStruct((rows, LANES), f32),
        in_specs=[pl.BlockSpec(memory_space=pl.ANY)] * 2,
        out_specs=pl.BlockSpec(memory_space=pltpu.VMEM),
        scratch_shapes=[
            pltpu.VMEM((2 * nq, 2, h, chunk), bf16),
            pltpu.VMEM((2 * nq, 2, h, chunk), bf16),
            pltpu.VMEM((max(side_len - 1, 1), 2, 2 * nq, 2, h, chunk), bf16),
            pltpu.VMEM((side_len, 2, nq, 2, h, chunk), bf16),
            pltpu.VMEM((n, 2, h, h), bf16),
            pltpu.VMEM((n, 2, h, h), bf16),
            pltpu.VMEM((rows, 8, LANES), f32),
            pltpu.VMEM((n * n_freq, rows, LANES), f32),
            pltpu.VMEM((8, LANES), f32),
            pltpu.VMEM((8, LANES), f32),
            dma((2 * nq,)), dma((n,)), dma((2 * nq,)), dma((2 * nq,)), dma((n,)), dma((n,)), dma((2,)),
            dma((max(n_near, n_far),)), dma((n_near,)), dma((n_far,)), dma((n_far,)),
            dma((n * n_freq - 1,)), dma((n * n_freq - 1,)), dma((2,)),
            pltpu.SemaphoreType.REGULAR((2, n // 2 - 1)), pltpu.SemaphoreType.REGULAR((2,)),
        ],
        compiler_params=pltpu.CompilerParams(
            collective_id=0, has_side_effects=True, vmem_limit_bytes=60 * 1024 * 1024
        ),
    )(greens, weights)
    return out.reshape(points)


def line_kernel(
    n_freq, h, stations, chunk, nq, kept, late, blocked,
    greens, weights, out,
    g_own, g_pair, near, far, w_own, w_pair, w_edge, acc, part, side, extra, extras, max_out, max_in,
    own_sem, w_own_sem, pair_send, pair_recv, wp_send, wp_recv, sib_sem, we_send, we_recv, we_sib,
    in_send, near_recv, far_recv, down_send, back_send, part_send, part_recv, side_sem,
    extra_send, extra_recv, max_sem, hello_sem, pair_hello,
):
    n = 8
    sub = chunk // LANES
    half_rows = h // 2
    steps = 4 * nq
    me = lax.axis_index("stn")
    core = lax.axis_index("pts")
    fq = lax.axis_index("freq")
    parity = lax.rem(me, 2)
    z = me // 2
    hi = z // 2
    inner = jnp.logical_or(z == 1, z == 2)
    outer = jnp.logical_not(inner)
    s_base = hi * nq
    r_base = (1 - hi) * nq
    rank = me * n_freq + fq
    total = n * n_freq
    inward = jnp.where(hi == 1, -2, 2)
    pair_dev = {"stn": me + 1 - 2 * parity}
    in_dev = {"stn": me + inward}
    out_dev = {"stn": me - inward}
    core_dev = {"pts": 1 - core}
    freq_dev = {"freq": n_freq - 1 - fq}
    across_dev = {"stn": lax.rem(me + n // 2, n)}
    other_inner = 2 - hi
    other_edge = 3 - 3 * hi
    near_z = jnp.where(inner, z - inward // 2, z + inward // 2)

    def columns(q):
        return pl.ds(pl.multiple_of(q * chunk, LANES), chunk)

    def w_src(freq, j, rows):
        if blocked:
            return weights.at[:, freq, j, rows, :]
        return weights.at[:, freq, rows, pl.ds(pl.multiple_of(j * h, LANES), h)]

    def block_of(where, p):
        return 2 * where + jnp.where(p == 0, parity, 1 - parity)

    def far_block(e):
        return block_of(jnp.where(lax.rem(e, 2) == 0, other_inner, other_edge), e // 2)

    last_block = block_of(other_edge, 1)
    every_row = pl.ds(0, h)
    my_rows = pl.ds(pl.multiple_of(core * half_rows, 8), half_rows)
    sib_rows = pl.ds(pl.multiple_of((1 - core) * half_rows, 8), half_rows)

    def pair_q(i):
        return jnp.where(i < nq, s_base + i, r_base + i - nq)

    def own_copy(q):
        return pltpu.make_async_copy(
            greens.at[:, parity, :, columns(q)], g_own.at[q], own_sem.at[q]
        )

    def w_own_copy(j):
        return pltpu.make_async_copy(w_src(parity, j, every_row), w_own.at[j], w_own_sem.at[j])

    def pair_copy(i):
        q = pair_q(i)
        return remote(
            greens.at[:, 1 - parity, :, columns(q)], g_pair.at[q],
            pair_send.at[i], pair_recv.at[i], pair_dev,
        )

    def w_pair_copy(j):
        return remote(
            w_src(1 - parity, j, my_rows), w_pair.at[j, :, my_rows, :],
            wp_send.at[j], wp_recv.at[j], pair_dev,
        )

    def sibling_copy(rows):
        part_of_w = w_pair.at[:, :, rows, :]
        return remote(part_of_w, part_of_w, sib_sem.at[0], sib_sem.at[1], core_dev)

    def edge_sibling_copy(rows):
        part_of_w = w_edge.at[:, :, rows, :]
        return remote(part_of_w, part_of_w, we_sib.at[0], we_sib.at[1], core_dev)

    def up_copy(src, p, i):
        slot = p * 2 * nq + i
        return remote(src, near.at[p, pair_q(i)], in_send.at[slot], near_recv.at[slot], in_dev)

    def up_weights(src, p):
        return remote(src, w_edge.at[p, :, my_rows, :], we_send.at[p], we_recv.at[p], in_dev)

    def mid_copy(src, slot):
        return remote(src, far.at[slot], in_send.at[slot], far_recv.at[slot], in_dev)

    def down_copy(slot):
        return remote(far.at[slot], far.at[slot], down_send.at[slot], far_recv.at[slot], out_dev)

    def back_copy(src, p, c):
        return remote(
            src, near.at[p, (1 - hi) * nq + c], back_send.at[p * kept + c],
            near_recv.at[p * 2 * nq + nq + c], out_dev,
        )

    @pl.loop(0, 2 * nq)
    def _(i):
        own_copy(pair_q(i)).start()

    @pl.loop(0, n)
    def _(j):
        w_own_copy(j).start()

    barrier = pltpu.get_barrier_semaphore()
    up, down = z < 3, z > 0
    greeted = [pair_dev, core_dev, freq_dev]

    def greet(sem, device):
        pl.semaphore_signal(sem, inc=1, device_id=device, device_id_type=MESH)

    def along_z(sem_down, sem_up):
        @pl.when(up)
        def _():
            greet(sem_up, {"stn": me + 2})

        @pl.when(down)
        def _():
            greet(sem_down, {"stn": me - 2})

    along_z(barrier, barrier)
    for device in greeted:
        greet(barrier, device)
    pl.semaphore_wait(barrier, len(greeted) + up.astype(jnp.int32) + down.astype(jnp.int32))

    @pl.loop(0, nq)
    def _(i):
        q = pair_q(i)
        own_copy(q).wait()

        @pl.when(inner)
        def _():
            mid_copy(g_own.at[q], i).start()

        @pl.when(outer)
        def _():
            up_copy(g_own.at[q], 0, i).start()

        @pl.when(i < n)
        def _():
            w_pair_copy(i).start()

    for j in range(nq, n):
        w_pair_copy(j).start()

    @pl.loop(0, 2 * nq)
    def _(i):
        pair_copy(i).start()

    @pl.loop(nq, 2 * nq)
    def _(i):
        q = pair_q(i)
        own_copy(q).wait()

        @pl.when(jnp.logical_and(inner, i < nq + kept))
        def _():
            back_copy(g_own.at[q], 0, i - nq).start()

        @pl.when(jnp.logical_and(outer, i >= nq + kept))
        def _():
            up_copy(g_own.at[q], 0, i).start()

    @pl.loop(0, n)
    def _(j):
        w_own_copy(j).wait()

    @pl.when(outer)
    def _():
        up_weights(w_own.at[last_block, :, my_rows, :], 0).start()

    @pl.loop(0, 3)
    def _(r):
        along_z(hello_sem.at[0, r], hello_sem.at[1, r])

        @pl.when(up)
        def _():
            pl.semaphore_wait(hello_sem.at[0, r], 1)

        @pl.when(down)
        def _():
            pl.semaphore_wait(hello_sem.at[1, r], 1)

    for i, device in enumerate((pair_dev, freq_dev)):
        greet(pair_hello.at[i], device)
        pl.semaphore_wait(pair_hello.at[i], 1)

    acc[...] = jnp.zeros_like(acc)

    def contribute(w, gi, gj, q, weight):
        for s in range(sub):
            lanes = slice(s * LANES, (s + 1) * LANES)
            both = jnp.concatenate([gj[0, :, lanes], gj[1, :, lanes]], axis=1)
            ab = jnp.dot(w[...].reshape(2 * h, h), both, preferred_element_type=jnp.float32)
            a, b = ab[:h], ab[h:]
            t = gi[0, :, lanes].astype(jnp.float32) * (a[:, :LANES] - b[:, LANES:])
            t = t + gi[1, :, lanes].astype(jnp.float32) * (a[:, LANES:] + b[:, :LANES])
            t = jnp.sum(t.reshape(h // 8, 8, LANES), axis=0)
            acc[q * sub + s] += t * weight

    own_pair_block = block_of(z, 1)

    def own_work(q):
        contribute(w_own.at[me], g_own.at[q], g_own.at[q], q, 1.0)

    def cross_work(q):
        contribute(w_own.at[own_pair_block], g_own.at[q], g_pair.at[q], q, 2.0)

    def pair_work(q):
        contribute(w_pair.at[own_pair_block], g_pair.at[q], g_pair.at[q], q, 1.0)

    def far_work(slot, w, g):
        q = r_base + lax.rem(slot, nq)
        contribute(w.at[far_block(slot // nq)], g.at[q], far.at[slot], q, 2.0)

    def near_work(p, q, w, g):
        contribute(w.at[block_of(near_z, p)], g.at[q], near.at[p, q], q, 2.0)

    def edge_work(c):
        q = r_base + c

        @pl.loop(0, 2)
        def _(p):
            contribute(w_edge.at[p], near.at[p, q], far.at[3 * nq + c], q, 2.0)

    def wait_far(t):
        ref = far.at[t]
        remote(ref, ref, down_send.at[t], far_recv.at[t], in_dev).wait_recv()

    def wait_near(p, i):
        slot = p * 2 * nq + i
        ref = near.at[p, pair_q(i)]
        remote(ref, ref, in_send.at[slot], near_recv.at[slot], in_dev).wait_recv()

    def wait_w_pair():
        @pl.loop(0, n)
        def _(j):
            w_pair_copy(j).wait_recv()

        sibling_copy(my_rows).start()

    def share_part():
        part[rank] = jnp.sum(acc[...], axis=1) / stations

        @pl.loop(0, total // 2 - 1)
        def _(k):
            part_copy(total // 2 - 1 - k, rank).start()

    def at_rank(target):
        return {"stn": target // n_freq, "freq": lax.rem(target, n_freq)}

    def flipped(k):
        bit, flip = total // 2, jnp.int32(0)
        while bit:
            mine = lax.rem(rank // bit, 2)
            turn = lax.rem(k // bit, 2)
            flip = flip + bit * (mine + turn - 2 * mine * turn)
            bit //= 2
        return flip

    def part_copy(k, source):
        ref = part.at[source]
        return remote(ref, ref, part_send.at[k - 1], part_recv.at[k - 1], at_rank(flipped(k)))

    near_second = 2 * nq - kept + 1
    near_third = 3 * nq - kept + 2
    near_end = 4 * nq - 2 * kept + 2

    def near_at(t):
        second = t >= near_second
        third = t >= near_third
        i = jnp.where(t < nq, t, t + kept)
        i = jnp.where(second, t - near_second, i)
        i = jnp.where(third, t - near_third + nq + kept, i)
        present = jnp.logical_and(t != near_second - 1, t != near_third - 1)
        return jnp.logical_and(present, t < near_end), second.astype(jnp.int32), i

    @pl.when(inner)
    def _():
        @pl.loop(0, steps)
        def _(t):
            has_near, p, i = near_at(t)
            has_pair = jnp.logical_and(t >= nq, t < 3 * nq)
            turn = t - nq
            wait_far(t)

            @pl.when(t < 3 * nq + kept)
            def _():
                down_copy(t).start()

            @pl.when(has_near)
            def _():
                wait_near(p, i)

                @pl.when(i < nq)
                def _():
                    mid_copy(near.at[p, pair_q(i)], (2 * p + 1) * nq + i).start()

            @pl.when(t == nq)
            def _():
                wait_w_pair()

            @pl.when(has_pair)
            def _():
                pair_copy(turn).wait_recv()

                @pl.when(turn < nq)
                def _():
                    mid_copy(g_pair.at[pair_q(turn)], 2 * nq + turn).start()

                @pl.when(jnp.logical_and(turn >= nq, turn < nq + kept))
                def _():
                    back_copy(g_pair.at[pair_q(turn)], 1, turn - nq).start()

            @pl.when(t == nq + 2)
            def _():
                sibling_copy(sib_rows).wait_recv()

            @pl.when(t == 3 * nq + kept - 1)
            def _():
                for r in range(2):
                    up_weights(w_edge.at[r, :, my_rows, :], r).wait_recv()
                edge_sibling_copy(my_rows).start()

            @pl.when(t == 3 * nq + kept)
            def _():
                edge_sibling_copy(sib_rows).wait_recv()

            far_work(t, w_own, g_own)

            @pl.when(t < 2 * nq)
            def _():
                own_work(t)

            @pl.when(has_near)
            def _():
                q = pair_q(i)
                near_work(p, q, w_own, g_own)

                @pl.when(p == 1)
                def _():
                    near_work(p, q, w_pair, g_pair)

            @pl.when(has_pair)
            def _():
                cross_work(pair_q(turn))

            lag = t - nq - 2

            @pl.when(jnp.logical_and(lag >= 0, lag < 2 * nq))
            def _():
                pair_work(pair_q(lag))

                @pl.when(lag < nq)
                def _():
                    near_work(0, pair_q(lag), w_pair, g_pair)

            @pl.when(jnp.logical_and(t >= 2 * nq, t < 3 * nq))
            def _():
                @pl.loop(0, 3)
                def _(e):
                    far_work(e * nq + t - 2 * nq, w_pair, g_pair)

                @pl.when(t >= 2 * nq + kept)
                def _():
                    near_work(0, r_base + t - 2 * nq, w_pair, g_pair)

            @pl.when(t >= 3 * nq)
            def _():
                far_work(t, w_pair, g_pair)

            @pl.when(t >= 3 * nq + kept)
            def _():
                edge_work(t - 3 * nq)

            @pl.when(t == steps - late - 1)
            def _():
                share_part()

                @pl.loop((nq - late) * sub, nq * sub)
                def _(c):
                    acc[r_base * sub + c] = jnp.zeros((8, LANES), jnp.float32)

    @pl.when(outer)
    def _():
        @pl.loop(0, 3 * nq + kept)
        def _(t):
            turn = t - nq + 2
            has_pair = jnp.logical_and(turn >= 0, turn < 2 * nq)
            back = t - 2 * nq - 4

            @pl.when(turn == 0)
            def _():
                wait_w_pair()

            @pl.when(has_pair)
            def _():
                pair_copy(turn).wait_recv()

                @pl.when(jnp.logical_or(turn < nq, turn >= nq + kept))
                def _():
                    up_copy(g_pair.at[pair_q(turn)], 1, turn).start()

                @pl.when(turn == nq - 1)
                def _():
                    up_weights(w_pair.at[last_block, :, my_rows, :], 1).start()

            @pl.when(t == nq)
            def _():
                sibling_copy(sib_rows).wait_recv()

            @pl.when(t < kept)
            def _():
                wait_near(0, nq + t)

            @pl.when(jnp.logical_and(back >= 0, back < kept))
            def _():
                wait_near(1, nq + back)

            wait_far(t)
            far_work(t, w_own, g_own)

            @pl.when(t < 2 * nq)
            def _():
                own_work(t)

            @pl.when(t < kept)
            def _():
                near_work(0, r_base + t, w_own, g_own)

            @pl.when(jnp.logical_and(back >= 0, back < kept))
            def _():
                q = r_base + back
                near_work(0, q, w_pair, g_pair)
                near_work(1, q, w_own, g_own)
                near_work(1, q, w_pair, g_pair)

            @pl.when(has_pair)
            def _():
                cross_work(pair_q(turn))

            @pl.when(jnp.logical_and(t >= nq, t < 3 * nq))
            def _():
                pair_work(pair_q(t - nq))

            @pl.when(jnp.logical_and(t >= 2 * nq, t < 3 * nq))
            def _():
                @pl.loop(0, 3)
                def _(e):
                    far_work(e * nq + t - 2 * nq, w_pair, g_pair)

            @pl.when(t >= 3 * nq)
            def _():
                far_work(t, w_pair, g_pair)

        share_part()

    my_group = hi * 2 * n_freq + parity * n_freq + fq
    late_rows = late * sub

    def extra_copy(k, group):
        ref = extras.at[group]
        return remote(
            extras.at[my_group], ref, extra_send.at[k - 1], extra_recv.at[group],
            at_rank(flipped(k)),
        )

    @pl.when(inner)
    def _():
        for c in range(late_rows):
            row = jnp.sum(acc[(r_base + nq - late) * sub + c], axis=0, keepdims=True) / stations
            extras[my_group, c] = row

        @pl.loop(0, total - 1)
        def _(k):
            extra_copy(total - 1 - k, my_group).start()

    @pl.loop(1, total // 2)
    def _(k):
        part_copy(k, flipped(k)).wait_recv()

    base = hi * (total // 2)
    mine = part[base]
    for d in range(1, total // 2):
        mine = mine + part[base + d]
    side[hi] = mine

    def side_copy(which):
        ref = side.at[which]
        return remote(ref, ref, side_sem.at[0], side_sem.at[1], across_dev)

    side_copy(hi).start()
    side_copy(1 - hi).wait_recv()
    extra[...] = side[0] + side[1]

    @pl.loop(0, 4 * n_freq)
    def _(g):
        @pl.when(jnp.logical_or(outer, g != my_group))
        def _():
            ref = extras.at[g]
            remote(ref, ref, extra_send.at[0], extra_recv.at[g], pair_dev).wait_recv()

    for low in range(2):
        for c in range(late_rows):
            row = extras[low * 2 * n_freq, c]
            for g in range(1, 2 * n_freq):
                row = row + extras[low * 2 * n_freq + g, c]
            at = ((1 - low) * nq + nq - late) * sub + c
            extra[at:at + 1, :] += row

    raw = extra[...]
    max_out[...] = jnp.broadcast_to(jnp.max(jnp.abs(raw)), max_out.shape)
    max_copy = remote(max_out, max_in, max_sem.at[0], max_sem.at[1], core_dev)
    max_copy.start()

    @pl.loop(0, 2 * nq)
    def _(i):
        pair_copy(i).wait_send()

    @pl.loop(0, n)
    def _(j):
        w_pair_copy(j).wait_send()

    sibling_copy(my_rows).wait_send()
    side_copy(hi).wait_send()

    @pl.loop(1, total // 2)
    def _(k):
        part_copy(k, rank).wait_send()

    @pl.when(inner)
    def _():
        @pl.loop(0, steps)
        def _(t):
            mid_copy(far.at[t], t).wait_send()

            @pl.when(t < 3 * nq + kept)
            def _():
                down_copy(t).wait_send()

        @pl.loop(0, 2 * kept)
        def _(i):
            back_copy(g_own.at[0], i // kept, lax.rem(i, kept)).wait_send()

        @pl.loop(1, total)
        def _(k):
            extra_copy(k, my_group).wait_send()

        edge_sibling_copy(my_rows).wait_send()

    @pl.when(outer)
    def _():
        @pl.loop(0, 4 * nq)
        def _(s):
            i = lax.rem(s, 2 * nq)

            @pl.when(jnp.logical_or(i < nq, i >= nq + kept))
            def _():
                up_copy(g_own.at[0], s // (2 * nq), i).wait_send()

        for r in range(2):
            up_weights(w_edge.at[r, :, my_rows, :], r).wait_send()

    max_copy.wait()
    largest = jnp.maximum(max_out[0:1, 0:1], max_in[0:1, 0:1])
    out[...] = raw / (largest + 1e-6)


def line_body(n_freq, chunk, nq, blocked, greens, weights):
    _, _, h, points = greens.shape
    n = 8
    kept, late = nq // 4, 3
    stations = n * h
    dma = pltpu.SemaphoreType.DMA
    regular = pltpu.SemaphoreType.REGULAR
    bf16, f32 = jnp.bfloat16, jnp.float32
    rows = points // LANES
    late_rows = late * (chunk // LANES)
    total = n * n_freq
    out = pl.pallas_call(
        functools.partial(line_kernel, n_freq, h, stations, chunk, nq, kept, late, blocked),
        out_shape=jax.ShapeDtypeStruct((rows, LANES), f32),
        in_specs=[pl.BlockSpec(memory_space=pl.ANY)] * 2,
        out_specs=pl.BlockSpec(memory_space=pltpu.VMEM),
        scratch_shapes=[
            pltpu.VMEM((2 * nq, 2, h, chunk), bf16),
            pltpu.VMEM((2 * nq, 2, h, chunk), bf16),
            pltpu.VMEM((2, 2 * nq, 2, h, chunk), bf16),
            pltpu.VMEM((4 * nq, 2, h, chunk), bf16),
            pltpu.VMEM((n, 2, h, h), bf16),
            pltpu.VMEM((n, 2, h, h), bf16),
            pltpu.VMEM((2, 2, h, h), bf16),
            pltpu.VMEM((rows, 8, LANES), f32),
            pltpu.VMEM((total, rows, LANES), f32),
            pltpu.VMEM((2, rows, LANES), f32),
            pltpu.VMEM((rows, LANES), f32),
            pltpu.VMEM((4 * n_freq, late_rows, 1, LANES), f32),
            pltpu.VMEM((8, LANES), f32),
            pltpu.VMEM((8, LANES), f32),
            dma((2 * nq,)), dma((n,)), dma((2 * nq,)), dma((2 * nq,)), dma((n,)), dma((n,)), dma((2,)),
            dma((2,)), dma((2,)), dma((2,)),
            dma((4 * nq,)), dma((4 * nq,)), dma((4 * nq,)), dma((4 * nq,)), dma((2 * kept,)),
            dma((total // 2 - 1,)), dma((total // 2 - 1,)), dma((2,)),
            dma((total - 1,)), dma((4 * n_freq,)), dma((2,)),
            regular((2, 3)), regular((2,)),
        ],
        compiler_params=pltpu.CompilerParams(
            collective_id=0, has_side_effects=True, vmem_limit_bytes=60 * 1024 * 1024
        ),
    )(greens, weights)
    return out.reshape(points)


def passed_along(x, axis, by):
    size = lax.axis_size(axis)
    return lax.ppermute(x, axis, [(i, (i + by) % size) for i in range(size)])


def mixing_of(weights):
    negated = -weights[1]
    return jnp.stack([jnp.stack([weights[0], negated]), jnp.stack([weights[1], weights[0]])])


def body(greens, noise_weights):
    station_rows = greens.shape[2]
    stations = noise_weights.shape[3]
    device_index = lax.axis_index("stn")
    cycle_length = lax.axis_size("stn")
    mixing = mixing_of(noise_weights)

    def block_product(columns_start, arriving):
        block_rows = arriving.shape[2]
        weights_block = lax.dynamic_slice_in_dim(mixing, columns_start, block_rows, 4)
        return jnp.einsum(
            "ocfin,cfnx->ofix", weights_block, arriving, preferred_element_type=jnp.float32
        )

    half_way = cycle_length // 2
    diagonal = block_product(device_index * station_rows, greens)

    def advance(offset, loop_state):
        running, current = loop_state
        current = passed_along(current, "stn", -1)
        source = (device_index + offset) % cycle_length
        weight = jnp.where(offset == half_way, 1.0, 2.0).astype(jnp.float32)
        running = running + weight * block_product(source * station_rows, current)
        return (running, current)

    summed, current = lax.fori_loop(1, half_way + 1, advance, (diagonal, greens))
    green_real = greens[0].astype(jnp.float32)
    green_imag = greens[1].astype(jnp.float32)
    partial_kernel = (
        jnp.sum(green_real * summed[0] + green_imag * summed[1], axis=(0, 1)) / stations
    )
    raw_kernel = lax.psum(partial_kernel, "stn")
    raw_kernel = lax.psum(raw_kernel, "freq")
    largest = lax.pmax(jnp.max(jnp.abs(raw_kernel)), "pts")
    return raw_kernel / (largest + 1e-06)


def solution(mesh):
    n, cores, n_freq = mesh.shape["stn"], mesh.shape["pts"], mesh.shape["freq"]

    def either(greens, noise_weights):
        _, freqs, rows, points = greens.shape
        fits = n % 4 == 0 and cores == 2 and freqs == 2 and n_freq == 2 and rows % 32 == 0 and points % (2 * LANES) == 0
        if fits:
            return kernel_body(n, n_freq, greens, noise_weights)
        return body(greens, noise_weights)

    in_specs = (P(None, "freq", "stn", "pts"), P(None, "freq", "stn", None))
    return jax.shard_map(either, mesh=mesh, in_specs=in_specs, out_specs=P("pts"), check_vma=False)
```

```python
import functools

import jax
import jax.numpy as jnp
from jax import lax
from jax.experimental import pallas as pl
from jax.experimental.pallas import tpu as pltpu
from jax.sharding import PartitionSpec as P

MESH = pl.DeviceIdType.MESH
LANES = 128


def remote(src, dst, send_sem, recv_sem, target):
    return pltpu.make_async_remote_copy(
        src_ref=src, dst_ref=dst, send_sem=send_sem, recv_sem=recv_sem,
        device_id=target, device_id_type=MESH,
    )


def ring_kernel(
    n, n_freq, h, stations, chunk, nq, blocked,
    greens, weights, out,
    g_own, g_pair, near, far, w_own, w_pair, acc, red, max_out, max_in,
    own_sem, w_own_sem, pair_send, pair_recv, wp_send, wp_recv, sib_sem,
    in_send, in_recv, out_send, far_recv, red_send, red_recv, max_sem, hello_sem, pair_hello,
):
    m = n // 2
    side_len = m // 2
    sub = chunk // LANES
    half_rows = h // 2
    me = lax.axis_index("stn")
    core = lax.axis_index("pts")
    fq = lax.axis_index("freq")
    parity = lax.rem(me, 2)
    z = me // 2
    hi = (z >= side_len).astype(jnp.int32)
    edge = jnp.where(hi == 1, m - 1 - z, z)
    inward = jnp.where(hi == 1, -2, 2)
    inner = edge == side_len - 1
    s_base = hi * nq
    r_base = (1 - hi) * nq
    pair_dev = {"stn": me + 1 - 2 * parity}
    in_dev = {"stn": me + inward}
    out_dev = {"stn": me - inward}
    n_far = side_len * 2 * nq
    n_near = edge * 4 * nq
    n_near_max = (side_len - 1) * 4 * nq
    steps = max(n_far, n_near_max, 3 * nq + 2)
    spread = side_len == 2
    catch_up = 2 * nq + 1 if spread else max((steps * 25) // 32, 3 * nq + 1)
    left = steps - catch_up
    per_step = -(-steps // (steps - catch_up))

    def columns(q):
        return pl.ds(pl.multiple_of(q * chunk, LANES), chunk)

    def w_src(freq, j, rows):
        if blocked:
            return weights.at[:, freq, j, rows, :]
        return weights.at[:, freq, rows, pl.ds(pl.multiple_of(j * h, LANES), h)]

    def global_block(e, opposite):
        low = jnp.where(opposite, 1 - hi, hi) == 0
        return jnp.where(low, e, m - 1 - e)

    def near_slot(receiver_edge, p, half, b, c):
        return ((p * 2 + half) * receiver_edge + (receiver_edge - 1 - b)) * nq + c

    def far_slot(p, b, c):
        return (p * side_len + (side_len - 1 - b)) * nq + c

    def send_inward(src, p, half, b, c):
        q = jnp.where(half == 0, s_base, r_base) + c

        if side_len > 1:
            @pl.when(jnp.logical_not(inner))
            def _():
                slot = near_slot(edge + 1, p, half, b, c)
                remote(src, near.at[b, p, q], in_send.at[slot], in_recv.at[slot], in_dev).start()

        @pl.when(jnp.logical_and(inner, half == 0))
        def _():
            slot = far_slot(p, b, c)
            remote(src, far.at[b, p, c], in_send.at[slot], far_recv.at[slot], in_dev).start()

    freq_dev = {"freq": n_freq - 1 - fq}
    barrier = pltpu.get_barrier_semaphore()
    up, down = z < m - 1, z > 0
    greeted = [pair_dev, {"pts": 1 - core}, freq_dev]

    def greet(sem, device):
        pl.semaphore_signal(sem, inc=1, device_id=device, device_id_type=MESH)

    def along_z(sem_down, sem_up):
        @pl.when(up)
        def _():
            greet(sem_up, {"stn": me + 2})

        @pl.when(down)
        def _():
            greet(sem_down, {"stn": me - 2})

    for device in greeted:
        greet(barrier, device)
    along_z(barrier, barrier)
    pl.semaphore_wait(barrier, len(greeted) + up.astype(jnp.int32) + down.astype(jnp.int32))

    def hello():
        @pl.loop(0, m - 1)
        def _(r):
            along_z(hello_sem.at[0, r], hello_sem.at[1, r])

            @pl.when(up)
            def _():
                pl.semaphore_wait(hello_sem.at[0, r], 1)

            @pl.when(down)
            def _():
                pl.semaphore_wait(hello_sem.at[1, r], 1)

        for i, device in enumerate((pair_dev, freq_dev)):
            greet(pair_hello.at[i], device)
            pl.semaphore_wait(pair_hello.at[i], 1)

    every_row = pl.ds(0, h)
    pair_rows = pl.ds(pl.multiple_of(core * half_rows, 8), half_rows)

    def pair_q(i):
        return jnp.where(i < nq, s_base + i, r_base + i - nq)

    def pair_copy(i):
        q = pair_q(i)
        return remote(
            greens.at[:, 1 - parity, :, columns(q)], g_pair.at[q],
            pair_send.at[i], pair_recv.at[i], pair_dev,
        )

    def w_pair_copy(j):
        return remote(
            w_src(1 - parity, j, pair_rows), w_pair.at[j, :, pair_rows, :],
            wp_send.at[j], wp_recv.at[j], pair_dev,
        )

    def sibling_copy(rows):
        return remote(
            w_pair.at[:, :, rows, :], w_pair.at[:, :, rows, :],
            sib_sem.at[0], sib_sem.at[1], {"pts": 1 - core},
        )

    def own_copy(q):
        return pltpu.make_async_copy(
            greens.at[:, parity, :, columns(q)], g_own.at[q], own_sem.at[q]
        )

    def w_own_copy(j):
        return pltpu.make_async_copy(w_src(parity, j, every_row), w_own.at[j], w_own_sem.at[j])

    @pl.loop(0, 2 * nq)
    def _(i):
        @pl.when(i < nq)
        def _():
            pair_copy(i).start()

        half = i // nq
        c = lax.rem(i, nq)
        send_inward(greens.at[:, parity, :, columns(pair_q(i))], 0, half, edge, c)
        own_copy(i).start()

    @pl.loop(0, n)
    def _(j):
        w_pair_copy(j).start()
        w_own_copy(j).start()

    @pl.loop(nq, 2 * nq)
    def _(i):
        pair_copy(i).start()

    hello()

    acc[...] = jnp.zeros_like(acc)

    @pl.loop(0, 2 * nq)
    def _(q):
        own_copy(q).wait()

    @pl.loop(0, n)
    def _(j):
        w_own_copy(j).wait()

    def contribute(w, gi, gj, q, weight):
        for s in range(sub):
            part = slice(s * LANES, (s + 1) * LANES)
            both = jnp.concatenate([gj[0, :, part], gj[1, :, part]], axis=1)
            ab = jnp.dot(w[...].reshape(2 * h, h), both, preferred_element_type=jnp.float32)
            a, b = ab[:h], ab[h:]
            t = gi[0, :, part].astype(jnp.float32) * (a[:, :LANES] - b[:, LANES:])
            t = t + gi[1, :, part].astype(jnp.float32) * (a[:, LANES:] + b[:, :LANES])
            t = jnp.sum(t.reshape(h // 8, 8, LANES), axis=0)
            acc[q * sub + s] += t * weight

    def far_at(t):
        p = t // (side_len * nq)
        rest = lax.rem(t, side_len * nq)
        return p, side_len - 1 - rest // nq, lax.rem(rest, nq)

    def near_at(t):
        width = jnp.maximum(edge, 1) * nq
        p = t // (2 * width)
        half = lax.rem(t // width, 2)
        rest = lax.rem(t, width)
        return p, half, jnp.maximum(edge, 1) - 1 - rest // nq, lax.rem(rest, nq)

    def part_of(p):
        return jnp.where(p == 0, parity, 1 - parity)

    def far_work(t, w, g):
        p, b, c = far_at(t)
        q = r_base + c
        j = global_block(b, True) * 2 + part_of(p)
        contribute(w.at[j], g.at[q], far.at[b, p, c], q, 2.0)

    def near_work(t, w, g):
        p, half, b, c = near_at(t)
        q = jnp.where(half == 0, s_base, r_base) + c
        j = global_block(b, False) * 2 + part_of(p)
        contribute(w.at[j], g.at[q], near.at[b, p, q], q, 2.0)

    def far_wait(t):
        p, b, c = far_at(t)
        ref = far.at[b, p, c]
        remote(ref, ref, out_send.at[t], far_recv.at[t], in_dev).wait_recv()

        @pl.when(edge > 0)
        def _():
            remote(ref, ref, out_send.at[t], far_recv.at[t], out_dev).start()

    def near_wait(t):
        p, half, b, c = near_at(t)
        q = jnp.where(half == 0, s_base, r_base) + c
        ref = near.at[b, p, q]
        remote(ref, ref, in_send.at[t], in_recv.at[t], out_dev).wait_recv()
        send_inward(ref, p, half, b, c)

    def newest(u):
        far_work(u, w_pair, g_pair)

        @pl.when(u < n_near)
        def _():
            near_work(u, w_pair, g_pair)

    @pl.loop(0, steps)
    def _(t):
        has_pair = jnp.logical_and(jnp.logical_and(t >= nq, t <= 3 * nq), t != 2 * nq)
        turn = t - nq - (t > 2 * nq).astype(jnp.int32)

        @pl.when(has_pair)
        def _():
            i = turn
            pair_copy(i).wait_recv()
            send_inward(g_pair.at[pair_q(i)], 1, i // nq, edge, lax.rem(i, nq))

        @pl.when(t < n_far)
        def _():
            far_wait(t)

        if side_len > 1:
            @pl.when(t < n_near)
            def _():
                near_wait(t)

        @pl.when(t == catch_up - 1)
        def _():
            @pl.loop(0, n)
            def _(j):
                w_pair_copy(j).wait_recv()

            sibling_copy(pair_rows).start()

        @pl.when(t < 2 * nq)
        def _():
            contribute(w_own.at[2 * z + parity], g_own.at[t], g_own.at[t], t, 1.0)

        @pl.when(has_pair)
        def _():
            q = pair_q(turn)
            contribute(w_own.at[2 * z + 1 - parity], g_own.at[q], g_pair.at[q], q, 2.0)

        @pl.when(t < n_far)
        def _():
            far_work(t, w_own, g_own)

        if side_len > 1:
            @pl.when(t < n_near)
            def _():
                near_work(t, w_own, g_own)

        @pl.when(t == catch_up)
        def _():
            sibling_copy(pl.ds(pl.multiple_of((1 - core) * half_rows, 8), half_rows)).wait_recv()

        @pl.when(t >= catch_up)
        def _():
            first = (t - catch_up) * per_step
            last = jnp.minimum(first + per_step, steps)
            if spread:
                first = ((t - catch_up) * 2 * nq) // left
                last = ((t - catch_up + 1) * 2 * nq) // left

            @pl.loop(first, last)
            def _(u):
                @pl.when(u < 2 * nq)
                def _():
                    q = pair_q(u)
                    contribute(w_pair.at[2 * z + 1 - parity], g_pair.at[q], g_pair.at[q], q, 1.0)

                if spread:
                    far_work(lax.rem(u, side_len) * nq + u // side_len, w_pair, g_pair)
                else:
                    @pl.when(u < n_far)
                    def _():
                        far_work(u, w_pair, g_pair)

                if side_len > 1:
                    @pl.when(u < n_near)
                    def _():
                        near_work(u, w_pair, g_pair)

            if spread:
                newest(t - 1)

    if spread:
        newest(steps - 1)

    total = n * n_freq
    rank = me * n_freq + fq
    red[rank] = jnp.sum(acc[...], axis=1) / stations

    def share_copy(k, source):
        target = lax.rem(rank + k, total)
        return remote(
            red.at[source], red.at[source], red_send.at[k - 1], red_recv.at[k - 1],
            {"stn": target // n_freq, "freq": lax.rem(target, n_freq)},
        )

    @pl.loop(1, total)
    def _(k):
        share_copy(k, rank).start()

    @pl.loop(1, total)
    def _(k):
        share_copy(k, lax.rem(rank - k + total, total)).wait_recv()

    raw = red[0]
    for d in range(1, total):
        raw = raw + red[d]
    max_out[...] = jnp.broadcast_to(jnp.max(jnp.abs(raw)), max_out.shape)
    max_copy = remote(max_out, max_in, max_sem.at[0], max_sem.at[1], {"pts": 1 - core})
    max_copy.start()

    @pl.loop(1, total)
    def _(k):
        share_copy(k, rank).wait_send()

    @pl.loop(0, 2 * nq)
    def _(i):
        pair_copy(i).wait_send()

    @pl.loop(0, n)
    def _(j):
        w_pair_copy(j).wait_send()

    sibling_copy(pair_rows).wait_send()
    ref = far.at[0, 0, 0]

    @pl.loop(0, jnp.where(inner, n_far, (edge + 1) * 4 * nq))
    def _(t):
        remote(ref, ref, in_send.at[t], far_recv.at[0], in_dev).wait_send()

    @pl.when(edge > 0)
    def _():
        @pl.loop(0, n_far)
        def _(t):
            remote(ref, ref, out_send.at[t], far_recv.at[0], out_dev).wait_send()

    max_copy.wait()
    largest = jnp.maximum(max_out[0:1, 0:1], max_in[0:1, 0:1])
    out[...] = raw / (largest + 1e-6)


def kernel_body(n, n_freq, greens, weights):
    _, _, h, points = greens.shape
    stations = weights.shape[3]
    half = points // 2
    chunk = LANES
    while chunk * 2 * h <= 32768 and half % (chunk * 2) == 0:
        chunk *= 2
    nq = half // chunk
    side_len = n // 4
    n_far = side_len * 2 * nq
    n_near = max(side_len - 1, 1) * 4 * nq
    blocked = h % LANES != 0
    if blocked:
        weights = weights.reshape(2, weights.shape[1], h, n, h).swapaxes(2, 3)
    if side_len == 2 and nq >= 4:
        return line_body(n_freq, chunk, nq, blocked, greens, weights)
    dma = pltpu.SemaphoreType.DMA
    bf16, f32 = jnp.bfloat16, jnp.float32
    rows = points // LANES
    out = pl.pallas_call(
        functools.partial(ring_kernel, n, n_freq, h, stations, chunk, nq, blocked),
        out_shape=jax.ShapeDtypeStruct((rows, LANES), f32),
        in_specs=[pl.BlockSpec(memory_space=pl.ANY)] * 2,
        out_specs=pl.BlockSpec(memory_space=pltpu.VMEM),
        scratch_shapes=[
            pltpu.VMEM((2 * nq, 2, h, chunk), bf16),
            pltpu.VMEM((2 * nq, 2, h, chunk), bf16),
            pltpu.VMEM((max(side_len - 1, 1), 2, 2 * nq, 2, h, chunk), bf16),
            pltpu.VMEM((side_len, 2, nq, 2, h, chunk), bf16),
            pltpu.VMEM((n, 2, h, h), bf16),
            pltpu.VMEM((n, 2, h, h), bf16),
            pltpu.VMEM((rows, 8, LANES), f32),
            pltpu.VMEM((n * n_freq, rows, LANES), f32),
            pltpu.VMEM((8, LANES), f32),
            pltpu.VMEM((8, LANES), f32),
            dma((2 * nq,)), dma((n,)), dma((2 * nq,)), dma((2 * nq,)), dma((n,)), dma((n,)), dma((2,)),
            dma((max(n_near, n_far),)), dma((n_near,)), dma((n_far,)), dma((n_far,)),
            dma((n * n_freq - 1,)), dma((n * n_freq - 1,)), dma((2,)),
            pltpu.SemaphoreType.REGULAR((2, n // 2 - 1)), pltpu.SemaphoreType.REGULAR((2,)),
        ],
        compiler_params=pltpu.CompilerParams(
            collective_id=0, has_side_effects=True, vmem_limit_bytes=60 * 1024 * 1024
        ),
    )(greens, weights)
    return out.reshape(points)


FAR_FIRST = (11, 9, 10, 8, 15, 7, 13, 14, 5, 6, 12, 4, 3, 1, 2)


def line_kernel(
    n_freq, h, stations, chunk, nq, kept, late, blocked,
    greens, weights, out,
    g_own, g_pair, near, far, w_own, w_pair, w_edge, acc, part, side, extra, extras, max_out, max_in,
    own_sem, w_own_sem, pair_send, pair_recv, wp_send, wp_recv, sib_sem, we_send, we_recv, we_sib,
    in_send, near_recv, far_recv, down_send, back_send, part_send, part_recv, side_sem,
    extra_send, extra_recv, max_sem, hello_sem, pair_hello,
):
    n = 8
    sub = chunk // LANES
    half_rows = h // 2
    steps = 4 * nq
    me = lax.axis_index("stn")
    core = lax.axis_index("pts")
    fq = lax.axis_index("freq")
    parity = lax.rem(me, 2)
    z = me // 2
    hi = z // 2
    inner = jnp.logical_or(z == 1, z == 2)
    outer = jnp.logical_not(inner)
    s_base = hi * nq
    r_base = (1 - hi) * nq
    rank = me * n_freq + fq
    total = n * n_freq
    inward = jnp.where(hi == 1, -2, 2)
    pair_dev = {"stn": me + 1 - 2 * parity}
    in_dev = {"stn": me + inward}
    out_dev = {"stn": me - inward}
    core_dev = {"pts": 1 - core}
    freq_dev = {"freq": n_freq - 1 - fq}
    across_dev = {"stn": lax.rem(me + n // 2, n)}
    other_inner = 2 - hi
    other_edge = 3 - 3 * hi
    near_z = jnp.where(inner, z - inward // 2, z + inward // 2)

    def columns(q):
        return pl.ds(pl.multiple_of(q * chunk, LANES), chunk)

    def w_src(freq, j, rows):
        if blocked:
            return weights.at[:, freq, j, rows, :]
        return weights.at[:, freq, rows, pl.ds(pl.multiple_of(j * h, LANES), h)]

    def block_of(where, p):
        return 2 * where + jnp.where(p == 0, parity, 1 - parity)

    def far_block(e):
        return block_of(jnp.where(lax.rem(e, 2) == 0, other_inner, other_edge), e // 2)

    last_block = block_of(other_edge, 1)
    every_row = pl.ds(0, h)
    my_rows = pl.ds(pl.multiple_of(core * half_rows, 8), half_rows)
    sib_rows = pl.ds(pl.multiple_of((1 - core) * half_rows, 8), half_rows)

    def pair_q(i):
        return jnp.where(i < nq, s_base + i, r_base + i - nq)

    def g_src(q):
        return greens.at[:, parity, :, columns(q)]

    def own_copy(q):
        return pltpu.make_async_copy(g_src(q), g_own.at[q], own_sem.at[q])

    def w_own_copy(j):
        return pltpu.make_async_copy(w_src(parity, j, every_row), w_own.at[j], w_own_sem.at[j])

    def pair_copy(i):
        q = pair_q(i)
        return remote(
            greens.at[:, 1 - parity, :, columns(q)], g_pair.at[q],
            pair_send.at[i], pair_recv.at[i], pair_dev,
        )

    def w_pair_copy(j):
        return remote(
            w_src(1 - parity, j, my_rows), w_pair.at[j, :, my_rows, :],
            wp_send.at[j], wp_recv.at[j], pair_dev,
        )

    def sibling_copy(rows):
        part_of_w = w_pair.at[:, :, rows, :]
        return remote(part_of_w, part_of_w, sib_sem.at[0], sib_sem.at[1], core_dev)

    def edge_sibling_copy(rows):
        part_of_w = w_edge.at[:, :, rows, :]
        return remote(part_of_w, part_of_w, we_sib.at[0], we_sib.at[1], core_dev)

    def up_copy(src, p, i):
        slot = p * 2 * nq + i
        return remote(src, near.at[p, pair_q(i)], in_send.at[slot], near_recv.at[slot], in_dev)

    def up_weights(src, p):
        return remote(src, w_edge.at[p, :, my_rows, :], we_send.at[p], we_recv.at[p], in_dev)

    def mid_copy(src, slot):
        return remote(src, far.at[slot], in_send.at[slot], far_recv.at[slot], in_dev)

    def down_copy(slot):
        return remote(far.at[slot], far.at[slot], down_send.at[slot], far_recv.at[slot], out_dev)

    def back_copy(src, p, c):
        return remote(
            src, near.at[p, (1 - hi) * nq + c], back_send.at[p * kept + c],
            near_recv.at[p * 2 * nq + nq + c], out_dev,
        )

    barrier = pltpu.get_barrier_semaphore()
    up, down = z < 3, z > 0
    greeted = [pair_dev, core_dev, freq_dev]

    def greet(sem, device):
        pl.semaphore_signal(sem, inc=1, device_id=device, device_id_type=MESH)

    def along_z(sem_down, sem_up):
        @pl.when(up)
        def _():
            greet(sem_up, {"stn": me + 2})

        @pl.when(down)
        def _():
            greet(sem_down, {"stn": me - 2})

    along_z(barrier, barrier)
    for device in greeted:
        greet(barrier, device)
    pl.semaphore_wait(barrier, len(greeted) + up.astype(jnp.int32) + down.astype(jnp.int32))

    @pl.loop(0, nq)
    def _(i):
        src = g_src(pair_q(i))

        @pl.when(inner)
        def _():
            mid_copy(src, i).start()

        @pl.when(outer)
        def _():
            up_copy(src, 0, i).start()

    @pl.loop(0, n)
    def _(j):
        w_pair_copy(j).start()
        w_own_copy(j).start()

    @pl.loop(0, 2 * nq)
    def _(i):
        own_copy(pair_q(i)).start()
        pair_copy(i).start()

    @pl.loop(nq, 2 * nq)
    def _(i):
        src = g_src(pair_q(i))

        @pl.when(jnp.logical_and(inner, i < nq + kept))
        def _():
            back_copy(src, 0, i - nq).start()

        @pl.when(jnp.logical_and(outer, i >= nq + kept))
        def _():
            up_copy(src, 0, i).start()

    @pl.when(outer)
    def _():
        up_weights(w_src(parity, last_block, my_rows), 0).start()

    @pl.loop(0, 3)
    def _(r):
        along_z(hello_sem.at[0, r], hello_sem.at[1, r])

        @pl.when(up)
        def _():
            pl.semaphore_wait(hello_sem.at[0, r], 1)

        @pl.when(down)
        def _():
            pl.semaphore_wait(hello_sem.at[1, r], 1)

    for i, device in enumerate((pair_dev, freq_dev)):
        greet(pair_hello.at[i], device)
        pl.semaphore_wait(pair_hello.at[i], 1)

    acc[...] = jnp.zeros_like(acc)

    @pl.loop(0, 2 * nq)
    def _(q):
        own_copy(q).wait()

    @pl.loop(0, n)
    def _(j):
        w_own_copy(j).wait()

    def product(w, gi, gj, s):
        lanes = slice(s * LANES, (s + 1) * LANES)
        both = jnp.concatenate([gj[0, :, lanes], gj[1, :, lanes]], axis=1)
        ab = jnp.dot(w[...].reshape(2 * h, h), both, preferred_element_type=jnp.float32)
        a, b = ab[:h], ab[h:]
        t = gi[0, :, lanes].astype(jnp.float32) * (a[:, :LANES] - b[:, LANES:])
        t = t + gi[1, :, lanes].astype(jnp.float32) * (a[:, LANES:] + b[:, :LANES])
        return jnp.sum(t.reshape(h // 8, 8, LANES), axis=0)

    def contribute(w, gi, gj, q, weight):
        for s in range(sub):
            acc[q * sub + s] += product(w, gi, gj, s) * weight

    own_pair_block = block_of(z, 1)

    def own_work(q):
        contribute(w_own.at[me], g_own.at[q], g_own.at[q], q, 1.0)

    def cross_work(q):
        contribute(w_own.at[own_pair_block], g_own.at[q], g_pair.at[q], q, 2.0)

    def pair_work(q):
        contribute(w_pair.at[own_pair_block], g_pair.at[q], g_pair.at[q], q, 1.0)

    def far_work(slot, w, g):
        q = r_base + lax.rem(slot, nq)
        contribute(w.at[far_block(slot // nq)], g.at[q], far.at[slot], q, 2.0)

    def near_work(p, q, w, g):
        contribute(w.at[block_of(near_z, p)], g.at[q], near.at[p, q], q, 2.0)

    def edge_work(c):
        q = r_base + c

        @pl.loop(0, 2)
        def _(p):
            contribute(w_edge.at[p], near.at[p, q], far.at[3 * nq + c], q, 2.0)

    def wait_far(t):
        ref = far.at[t]
        remote(ref, ref, down_send.at[t], far_recv.at[t], in_dev).wait_recv()

    def wait_near(p, i):
        slot = p * 2 * nq + i
        ref = near.at[p, pair_q(i)]
        remote(ref, ref, in_send.at[slot], near_recv.at[slot], in_dev).wait_recv()

    def wait_w_pair():
        @pl.loop(0, n)
        def _(j):
            w_pair_copy(j).wait_recv()

        sibling_copy(my_rows).start()

    def share_part():
        part[rank] = jnp.sum(acc[...], axis=1) / stations

        @pl.loop(0, total // 2 - 1)
        def _(k):
            part_copy(total // 2 - 1 - k, rank).start()

    def at_rank(target):
        return {"stn": target // n_freq, "freq": lax.rem(target, n_freq)}

    def flipped(k):
        bit, flip = total // 2, jnp.int32(0)
        while bit:
            mine = lax.rem(rank // bit, 2)
            turn = lax.rem(k // bit, 2)
            flip = flip + bit * (mine + turn - 2 * mine * turn)
            bit //= 2
        return flip

    def part_copy(k, source):
        ref = part.at[source]
        return remote(ref, ref, part_send.at[k - 1], part_recv.at[k - 1], at_rank(flipped(k)))

    my_group = (hi * 2 + parity) * n_freq + fq
    late_rows = late * sub

    def extra_copy(k):
        def turned(v, bit):
            return 1 - v if k & bit else v

        target_z = 2 * turned(hi, 8) + turned(lax.rem(z, 2), 4)
        target = {"stn": 2 * target_z + turned(parity, 2), "freq": turned(fq, 1)}
        ref = extras.at[my_group]
        return remote(ref, ref, extra_send.at[k - 1], extra_recv.at[my_group], target)

    def finish():
        first = (r_base + nq - late) * sub
        q, slot = r_base + nq - 1, steps - 1
        j = far_block(3)
        for c in range(late_rows - sub):
            row = jnp.sum(acc[first + c], axis=0, keepdims=True) / stations
            extras[my_group, c] = row
        wait_far(slot)
        for s in range(sub):
            gj = far.at[slot]
            t = product(w_own.at[j], g_own.at[q], gj, s)
            t = t + product(w_pair.at[j], g_pair.at[q], gj, s)
            for p in range(2):
                t = t + product(w_edge.at[p], near.at[p, q], gj, s)
            t = acc[q * sub + s] + 2.0 * t
            row = jnp.sum(t, axis=0, keepdims=True) / stations
            extras[my_group, late_rows - sub + s] = row
        for k in FAR_FIRST:
            extra_copy(k).start()

    near_second = 2 * nq - kept + 1
    near_third = 3 * nq - kept + 2
    near_end = 4 * nq - 2 * kept + 2

    def near_at(t):
        second = t >= near_second
        third = t >= near_third
        i = jnp.where(t < nq, t, t + kept)
        i = jnp.where(second, t - near_second, i)
        i = jnp.where(third, t - near_third + nq + kept, i)
        present = jnp.logical_and(t != near_second - 1, t != near_third - 1)
        return jnp.logical_and(present, t < near_end), second.astype(jnp.int32), i

    @pl.when(inner)
    def _():
        @pl.loop(0, steps - 1)
        def _(t):
            has_near, p, i = near_at(t)
            has_pair = jnp.logical_and(t >= nq, t < 3 * nq)
            turn = t - nq
            wait_far(t)

            @pl.when(t < 3 * nq + kept)
            def _():
                down_copy(t).start()

            @pl.when(has_near)
            def _():
                wait_near(p, i)

                @pl.when(i < nq)
                def _():
                    mid_copy(near.at[p, pair_q(i)], (2 * p + 1) * nq + i).start()

            @pl.when(t == nq)
            def _():
                wait_w_pair()

            @pl.when(has_pair)
            def _():
                pair_copy(turn).wait_recv()

                @pl.when(turn < nq)
                def _():
                    mid_copy(g_pair.at[pair_q(turn)], 2 * nq + turn).start()

                @pl.when(jnp.logical_and(turn >= nq, turn < nq + kept))
                def _():
                    back_copy(g_pair.at[pair_q(turn)], 1, turn - nq).start()

            @pl.when(t == nq + 2)
            def _():
                sibling_copy(sib_rows).wait_recv()

            @pl.when(t == 3 * nq + kept - 1)
            def _():
                for r in range(2):
                    up_weights(w_edge.at[r, :, my_rows, :], r).wait_recv()
                edge_sibling_copy(my_rows).start()

            @pl.when(t == 3 * nq + kept)
            def _():
                edge_sibling_copy(sib_rows).wait_recv()

            far_work(t, w_own, g_own)

            @pl.when(t < 2 * nq)
            def _():
                own_work(t)

            @pl.when(has_near)
            def _():
                q = pair_q(i)
                near_work(p, q, w_own, g_own)

                @pl.when(p == 1)
                def _():
                    near_work(p, q, w_pair, g_pair)

            @pl.when(has_pair)
            def _():
                cross_work(pair_q(turn))

            lag = t - nq - 2

            @pl.when(jnp.logical_and(lag >= 0, lag < 2 * nq))
            def _():
                pair_work(pair_q(lag))

                @pl.when(lag < nq)
                def _():
                    near_work(0, pair_q(lag), w_pair, g_pair)

            @pl.when(jnp.logical_and(t >= 2 * nq, t < 3 * nq))
            def _():
                @pl.loop(0, 3)
                def _(e):
                    far_work(e * nq + t - 2 * nq, w_pair, g_pair)

                @pl.when(t >= 2 * nq + kept)
                def _():
                    near_work(0, r_base + t - 2 * nq, w_pair, g_pair)

            @pl.when(t >= 3 * nq)
            def _():
                far_work(t, w_pair, g_pair)

            @pl.when(t >= 3 * nq + kept)
            def _():
                edge_work(t - 3 * nq)

            @pl.when(t == steps - late - 1)
            def _():
                share_part()

                @pl.loop((nq - late) * sub, nq * sub)
                def _(c):
                    acc[r_base * sub + c] = jnp.zeros((8, LANES), jnp.float32)

        finish()

    @pl.when(outer)
    def _():
        @pl.loop(0, 3 * nq + kept)
        def _(t):
            turn = t - nq + 2
            has_pair = jnp.logical_and(turn >= 0, turn < 2 * nq)
            back = t - 2 * nq - 4

            @pl.when(turn == 0)
            def _():
                wait_w_pair()

            @pl.when(has_pair)
            def _():
                pair_copy(turn).wait_recv()

                @pl.when(jnp.logical_or(turn < nq, turn >= nq + kept))
                def _():
                    up_copy(g_pair.at[pair_q(turn)], 1, turn).start()

                @pl.when(turn == nq - 1)
                def _():
                    up_weights(w_pair.at[last_block, :, my_rows, :], 1).start()

            @pl.when(t == nq)
            def _():
                sibling_copy(sib_rows).wait_recv()

            @pl.when(t < kept)
            def _():
                wait_near(0, nq + t)

            @pl.when(jnp.logical_and(back >= 0, back < kept))
            def _():
                wait_near(1, nq + back)

            wait_far(t)
            far_work(t, w_own, g_own)

            @pl.when(t < 2 * nq)
            def _():
                own_work(t)

            @pl.when(t < kept)
            def _():
                near_work(0, r_base + t, w_own, g_own)

            @pl.when(jnp.logical_and(back >= 0, back < kept))
            def _():
                q = r_base + back
                near_work(0, q, w_pair, g_pair)
                near_work(1, q, w_own, g_own)
                near_work(1, q, w_pair, g_pair)

            @pl.when(has_pair)
            def _():
                cross_work(pair_q(turn))

            @pl.when(jnp.logical_and(t >= nq, t < 3 * nq))
            def _():
                pair_work(pair_q(t - nq))

            @pl.when(jnp.logical_and(t >= 2 * nq, t < 3 * nq))
            def _():
                @pl.loop(0, 3)
                def _(e):
                    far_work(e * nq + t - 2 * nq, w_pair, g_pair)

            @pl.when(t >= 3 * nq)
            def _():
                far_work(t, w_pair, g_pair)

        share_part()

    @pl.loop(1, total // 2)
    def _(k):
        part_copy(k, flipped(k)).wait_recv()

    base = hi * (total // 2)
    mine = part[base]
    for d in range(1, total // 2):
        mine = mine + part[base + d]
    side[hi] = mine

    def side_copy(which):
        ref = side.at[which]
        return remote(ref, ref, side_sem.at[0], side_sem.at[1], across_dev)

    side_copy(hi).start()

    @pl.loop(0, 2 * nq)
    def _(i):
        pair_copy(i).wait_send()

    @pl.loop(0, n)
    def _(j):
        w_pair_copy(j).wait_send()

    sibling_copy(my_rows).wait_send()

    @pl.loop(1, total // 2)
    def _(k):
        part_copy(k, rank).wait_send()

    @pl.when(inner)
    def _():
        @pl.loop(0, steps)
        def _(t):
            mid_copy(far.at[t], t).wait_send()

            @pl.when(t < 3 * nq + kept)
            def _():
                down_copy(t).wait_send()

        @pl.loop(0, 2 * kept)
        def _(i):
            back_copy(g_own.at[0], i // kept, lax.rem(i, kept)).wait_send()

        for k in FAR_FIRST:
            extra_copy(k).wait_send()

        edge_sibling_copy(my_rows).wait_send()

    @pl.when(outer)
    def _():
        @pl.loop(0, 4 * nq)
        def _(s):
            i = lax.rem(s, 2 * nq)

            @pl.when(jnp.logical_or(i < nq, i >= nq + kept))
            def _():
                up_copy(g_own.at[0], s // (2 * nq), i).wait_send()

        for r in range(2):
            up_weights(w_edge.at[r, :, my_rows, :], r).wait_send()

    side_copy(1 - hi).wait_recv()
    extra[...] = side[0] + side[1]

    @pl.loop(0, 4 * n_freq)
    def _(g):
        @pl.when(jnp.logical_or(outer, g != my_group))
        def _():
            ref = extras.at[g]
            remote(ref, ref, extra_send.at[0], extra_recv.at[g], pair_dev).wait_recv()

    for low in range(2):
        for c in range(late_rows):
            row = extras[low * 2 * n_freq, c]
            for g in range(1, 2 * n_freq):
                row = row + extras[low * 2 * n_freq + g, c]
            at = ((1 - low) * nq + nq - late) * sub + c
            extra[at:at + 1, :] += row

    raw = extra[...]
    max_out[...] = jnp.broadcast_to(jnp.max(jnp.abs(raw)), max_out.shape)
    max_copy = remote(max_out, max_in, max_sem.at[0], max_sem.at[1], core_dev)
    max_copy.start()

    side_copy(hi).wait_send()
    max_copy.wait()
    largest = jnp.maximum(max_out[0:1, 0:1], max_in[0:1, 0:1])
    out[...] = raw / (largest + 1e-6)


def line_body(n_freq, chunk, nq, blocked, greens, weights):
    _, _, h, points = greens.shape
    n = 8
    kept, late = nq // 4, 3
    stations = n * h
    dma = pltpu.SemaphoreType.DMA
    regular = pltpu.SemaphoreType.REGULAR
    bf16, f32 = jnp.bfloat16, jnp.float32
    rows = points // LANES
    late_rows = late * (chunk // LANES)
    total = n * n_freq
    out = pl.pallas_call(
        functools.partial(line_kernel, n_freq, h, stations, chunk, nq, kept, late, blocked),
        out_shape=pltpu.VMEM((rows, LANES), f32),
        in_specs=[pl.BlockSpec(memory_space=pl.ANY)] * 2,
        out_specs=pl.BlockSpec(memory_space=pltpu.VMEM),
        scratch_shapes=[
            pltpu.VMEM((2 * nq, 2, h, chunk), bf16),
            pltpu.VMEM((2 * nq, 2, h, chunk), bf16),
            pltpu.VMEM((2, 2 * nq, 2, h, chunk), bf16),
            pltpu.VMEM((4 * nq, 2, h, chunk), bf16),
            pltpu.VMEM((n, 2, h, h), bf16),
            pltpu.VMEM((n, 2, h, h), bf16),
            pltpu.VMEM((2, 2, h, h), bf16),
            pltpu.VMEM((rows, 8, LANES), f32),
            pltpu.VMEM((total, rows, LANES), f32),
            pltpu.VMEM((2, rows, LANES), f32),
            pltpu.VMEM((rows, LANES), f32),
            pltpu.VMEM((4 * n_freq, late_rows, 1, LANES), f32),
            pltpu.VMEM((8, LANES), f32),
            pltpu.VMEM((8, LANES), f32),
            dma((2 * nq,)), dma((n,)), dma((2 * nq,)), dma((2 * nq,)), dma((n,)), dma((n,)), dma((2,)),
            dma((2,)), dma((2,)), dma((2,)),
            dma((4 * nq,)), dma((4 * nq,)), dma((4 * nq,)), dma((4 * nq,)), dma((2 * kept,)),
            dma((total // 2 - 1,)), dma((total // 2 - 1,)), dma((2,)),
            dma((total - 1,)), dma((4 * n_freq,)), dma((2,)),
            regular((2, 3)), regular((2,)),
        ],
        compiler_params=pltpu.CompilerParams(
            collective_id=0, has_side_effects=True, vmem_limit_bytes=60 * 1024 * 1024
        ),
    )(greens, weights)
    return out.reshape(points)


def passed_along(x, axis, by):
    size = lax.axis_size(axis)
    return lax.ppermute(x, axis, [(i, (i + by) % size) for i in range(size)])


def mixing_of(weights):
    negated = -weights[1]
    return jnp.stack([jnp.stack([weights[0], negated]), jnp.stack([weights[1], weights[0]])])


def body(greens, noise_weights):
    station_rows = greens.shape[2]
    stations = noise_weights.shape[3]
    device_index = lax.axis_index("stn")
    cycle_length = lax.axis_size("stn")
    mixing = mixing_of(noise_weights)

    def block_product(columns_start, arriving):
        block_rows = arriving.shape[2]
        weights_block = lax.dynamic_slice_in_dim(mixing, columns_start, block_rows, 4)
        return jnp.einsum(
            "ocfin,cfnx->ofix", weights_block, arriving, preferred_element_type=jnp.float32
        )

    half_way = cycle_length // 2
    diagonal = block_product(device_index * station_rows, greens)

    def advance(offset, loop_state):
        running, current = loop_state
        current = passed_along(current, "stn", -1)
        source = (device_index + offset) % cycle_length
        weight = jnp.where(offset == half_way, 1.0, 2.0).astype(jnp.float32)
        running = running + weight * block_product(source * station_rows, current)
        return (running, current)

    summed, current = lax.fori_loop(1, half_way + 1, advance, (diagonal, greens))
    green_real = greens[0].astype(jnp.float32)
    green_imag = greens[1].astype(jnp.float32)
    partial_kernel = (
        jnp.sum(green_real * summed[0] + green_imag * summed[1], axis=(0, 1)) / stations
    )
    raw_kernel = lax.psum(partial_kernel, "stn")
    raw_kernel = lax.psum(raw_kernel, "freq")
    largest = lax.pmax(jnp.max(jnp.abs(raw_kernel)), "pts")
    return raw_kernel / (largest + 1e-06)


def solution(mesh):
    n, cores, n_freq = mesh.shape["stn"], mesh.shape["pts"], mesh.shape["freq"]

    def either(greens, noise_weights):
        _, freqs, rows, points = greens.shape
        fits = n % 4 == 0 and cores == 2 and freqs == 2 and n_freq == 2 and rows % 32 == 0 and points % (2 * LANES) == 0
        if fits:
            return kernel_body(n, n_freq, greens, noise_weights)
        return body(greens, noise_weights)

    in_specs = (P(None, "freq", "stn", "pts"), P(None, "freq", "stn", None))
    return jax.shard_map(either, mesh=mesh, in_specs=in_specs, out_specs=P("pts"), check_vma=False)
```

```python
import functools

import jax
import jax.numpy as jnp
from jax import lax
from jax.experimental import pallas as pl
from jax.experimental.pallas import tpu as pltpu
from jax.sharding import PartitionSpec as P

MESH = pl.DeviceIdType.MESH
LANES = 128


def remote(src, dst, send_sem, recv_sem, target):
    return pltpu.make_async_remote_copy(
        src_ref=src, dst_ref=dst, send_sem=send_sem, recv_sem=recv_sem,
        device_id=target, device_id_type=MESH,
    )


def ring_kernel(
    n, n_freq, h, stations, chunk, nq, blocked,
    greens, weights, out,
    g_own, g_pair, near, far, w_own, w_pair, acc, red, max_out, max_in,
    own_sem, w_own_sem, pair_send, pair_recv, wp_send, wp_recv, sib_sem,
    in_send, in_recv, out_send, far_recv, red_send, red_recv, max_sem, hello_sem, pair_hello,
):
    m = n // 2
    side_len = m // 2
    sub = chunk // LANES
    half_rows = h // 2
    me = lax.axis_index("stn")
    core = lax.axis_index("pts")
    fq = lax.axis_index("freq")
    parity = lax.rem(me, 2)
    z = me // 2
    hi = (z >= side_len).astype(jnp.int32)
    edge = jnp.where(hi == 1, m - 1 - z, z)
    inward = jnp.where(hi == 1, -2, 2)
    inner = edge == side_len - 1
    s_base = hi * nq
    r_base = (1 - hi) * nq
    pair_dev = {"stn": me + 1 - 2 * parity}
    in_dev = {"stn": me + inward}
    out_dev = {"stn": me - inward}
    n_far = side_len * 2 * nq
    n_near = edge * 4 * nq
    n_near_max = (side_len - 1) * 4 * nq
    steps = max(n_far, n_near_max, 3 * nq + 2)
    spread = side_len == 2
    catch_up = 2 * nq + 1 if spread else max((steps * 25) // 32, 3 * nq + 1)
    left = steps - catch_up
    per_step = -(-steps // (steps - catch_up))

    def columns(q):
        return pl.ds(pl.multiple_of(q * chunk, LANES), chunk)

    def w_src(freq, j, rows):
        if blocked:
            return weights.at[:, freq, j, rows, :]
        return weights.at[:, freq, rows, pl.ds(pl.multiple_of(j * h, LANES), h)]

    def global_block(e, opposite):
        low = jnp.where(opposite, 1 - hi, hi) == 0
        return jnp.where(low, e, m - 1 - e)

    def near_slot(receiver_edge, p, half, b, c):
        return ((p * 2 + half) * receiver_edge + (receiver_edge - 1 - b)) * nq + c

    def far_slot(p, b, c):
        return (p * side_len + (side_len - 1 - b)) * nq + c

    def send_inward(src, p, half, b, c):
        q = jnp.where(half == 0, s_base, r_base) + c

        if side_len > 1:
            @pl.when(jnp.logical_not(inner))
            def _():
                slot = near_slot(edge + 1, p, half, b, c)
                remote(src, near.at[b, p, q], in_send.at[slot], in_recv.at[slot], in_dev).start()

        @pl.when(jnp.logical_and(inner, half == 0))
        def _():
            slot = far_slot(p, b, c)
            remote(src, far.at[b, p, c], in_send.at[slot], far_recv.at[slot], in_dev).start()

    freq_dev = {"freq": n_freq - 1 - fq}
    barrier = pltpu.get_barrier_semaphore()
    up, down = z < m - 1, z > 0
    greeted = [pair_dev, {"pts": 1 - core}, freq_dev]

    def greet(sem, device):
        pl.semaphore_signal(sem, inc=1, device_id=device, device_id_type=MESH)

    def along_z(sem_down, sem_up):
        @pl.when(up)
        def _():
            greet(sem_up, {"stn": me + 2})

        @pl.when(down)
        def _():
            greet(sem_down, {"stn": me - 2})

    for device in greeted:
        greet(barrier, device)
    along_z(barrier, barrier)
    pl.semaphore_wait(barrier, len(greeted) + up.astype(jnp.int32) + down.astype(jnp.int32))

    def hello():
        @pl.loop(0, m - 1)
        def _(r):
            along_z(hello_sem.at[0, r], hello_sem.at[1, r])

            @pl.when(up)
            def _():
                pl.semaphore_wait(hello_sem.at[0, r], 1)

            @pl.when(down)
            def _():
                pl.semaphore_wait(hello_sem.at[1, r], 1)

        for i, device in enumerate((pair_dev, freq_dev)):
            greet(pair_hello.at[i], device)
            pl.semaphore_wait(pair_hello.at[i], 1)

    every_row = pl.ds(0, h)
    pair_rows = pl.ds(pl.multiple_of(core * half_rows, 8), half_rows)

    def pair_q(i):
        return jnp.where(i < nq, s_base + i, r_base + i - nq)

    def pair_copy(i):
        q = pair_q(i)
        return remote(
            greens.at[:, 1 - parity, :, columns(q)], g_pair.at[q],
            pair_send.at[i], pair_recv.at[i], pair_dev,
        )

    def w_pair_copy(j):
        return remote(
            w_src(1 - parity, j, pair_rows), w_pair.at[j, :, pair_rows, :],
            wp_send.at[j], wp_recv.at[j], pair_dev,
        )

    def sibling_copy(rows):
        return remote(
            w_pair.at[:, :, rows, :], w_pair.at[:, :, rows, :],
            sib_sem.at[0], sib_sem.at[1], {"pts": 1 - core},
        )

    def own_copy(q):
        return pltpu.make_async_copy(
            greens.at[:, parity, :, columns(q)], g_own.at[q], own_sem.at[q]
        )

    def w_own_copy(j):
        return pltpu.make_async_copy(w_src(parity, j, every_row), w_own.at[j], w_own_sem.at[j])

    @pl.loop(0, 2 * nq)
    def _(i):
        @pl.when(i < nq)
        def _():
            pair_copy(i).start()

        half = i // nq
        c = lax.rem(i, nq)
        send_inward(greens.at[:, parity, :, columns(pair_q(i))], 0, half, edge, c)
        own_copy(i).start()

    @pl.loop(0, n)
    def _(j):
        w_pair_copy(j).start()
        w_own_copy(j).start()

    @pl.loop(nq, 2 * nq)
    def _(i):
        pair_copy(i).start()

    hello()

    acc[...] = jnp.zeros_like(acc)

    @pl.loop(0, 2 * nq)
    def _(q):
        own_copy(q).wait()

    @pl.loop(0, n)
    def _(j):
        w_own_copy(j).wait()

    def contribute(w, gi, gj, q, weight):
        for s in range(sub):
            part = slice(s * LANES, (s + 1) * LANES)
            both = jnp.concatenate([gj[0, :, part], gj[1, :, part]], axis=1)
            ab = jnp.dot(w[...].reshape(2 * h, h), both, preferred_element_type=jnp.float32)
            a, b = ab[:h], ab[h:]
            t = gi[0, :, part].astype(jnp.float32) * (a[:, :LANES] - b[:, LANES:])
            t = t + gi[1, :, part].astype(jnp.float32) * (a[:, LANES:] + b[:, :LANES])
            t = jnp.sum(t.reshape(h // 8, 8, LANES), axis=0)
            acc[q * sub + s] += t * weight

    def far_at(t):
        p = t // (side_len * nq)
        rest = lax.rem(t, side_len * nq)
        return p, side_len - 1 - rest // nq, lax.rem(rest, nq)

    def near_at(t):
        width = jnp.maximum(edge, 1) * nq
        p = t // (2 * width)
        half = lax.rem(t // width, 2)
        rest = lax.rem(t, width)
        return p, half, jnp.maximum(edge, 1) - 1 - rest // nq, lax.rem(rest, nq)

    def part_of(p):
        return jnp.where(p == 0, parity, 1 - parity)

    def far_work(t, w, g):
        p, b, c = far_at(t)
        q = r_base + c
        j = global_block(b, True) * 2 + part_of(p)
        contribute(w.at[j], g.at[q], far.at[b, p, c], q, 2.0)

    def near_work(t, w, g):
        p, half, b, c = near_at(t)
        q = jnp.where(half == 0, s_base, r_base) + c
        j = global_block(b, False) * 2 + part_of(p)
        contribute(w.at[j], g.at[q], near.at[b, p, q], q, 2.0)

    def far_wait(t):
        p, b, c = far_at(t)
        ref = far.at[b, p, c]
        remote(ref, ref, out_send.at[t], far_recv.at[t], in_dev).wait_recv()

        @pl.when(edge > 0)
        def _():
            remote(ref, ref, out_send.at[t], far_recv.at[t], out_dev).start()

    def near_wait(t):
        p, half, b, c = near_at(t)
        q = jnp.where(half == 0, s_base, r_base) + c
        ref = near.at[b, p, q]
        remote(ref, ref, in_send.at[t], in_recv.at[t], out_dev).wait_recv()
        send_inward(ref, p, half, b, c)

    def newest(u):
        far_work(u, w_pair, g_pair)

        @pl.when(u < n_near)
        def _():
            near_work(u, w_pair, g_pair)

    @pl.loop(0, steps)
    def _(t):
        has_pair = jnp.logical_and(jnp.logical_and(t >= nq, t <= 3 * nq), t != 2 * nq)
        turn = t - nq - (t > 2 * nq).astype(jnp.int32)

        @pl.when(has_pair)
        def _():
            i = turn
            pair_copy(i).wait_recv()
            send_inward(g_pair.at[pair_q(i)], 1, i // nq, edge, lax.rem(i, nq))

        @pl.when(t < n_far)
        def _():
            far_wait(t)

        if side_len > 1:
            @pl.when(t < n_near)
            def _():
                near_wait(t)

        @pl.when(t == catch_up - 1)
        def _():
            @pl.loop(0, n)
            def _(j):
                w_pair_copy(j).wait_recv()

            sibling_copy(pair_rows).start()

        @pl.when(t < 2 * nq)
        def _():
            contribute(w_own.at[2 * z + parity], g_own.at[t], g_own.at[t], t, 1.0)

        @pl.when(has_pair)
        def _():
            q = pair_q(turn)
            contribute(w_own.at[2 * z + 1 - parity], g_own.at[q], g_pair.at[q], q, 2.0)

        @pl.when(t < n_far)
        def _():
            far_work(t, w_own, g_own)

        if side_len > 1:
            @pl.when(t < n_near)
            def _():
                near_work(t, w_own, g_own)

        @pl.when(t == catch_up)
        def _():
            sibling_copy(pl.ds(pl.multiple_of((1 - core) * half_rows, 8), half_rows)).wait_recv()

        @pl.when(t >= catch_up)
        def _():
            first = (t - catch_up) * per_step
            last = jnp.minimum(first + per_step, steps)
            if spread:
                first = ((t - catch_up) * 2 * nq) // left
                last = ((t - catch_up + 1) * 2 * nq) // left

            @pl.loop(first, last)
            def _(u):
                @pl.when(u < 2 * nq)
                def _():
                    q = pair_q(u)
                    contribute(w_pair.at[2 * z + 1 - parity], g_pair.at[q], g_pair.at[q], q, 1.0)

                if spread:
                    far_work(lax.rem(u, side_len) * nq + u // side_len, w_pair, g_pair)
                else:
                    @pl.when(u < n_far)
                    def _():
                        far_work(u, w_pair, g_pair)

                if side_len > 1:
                    @pl.when(u < n_near)
                    def _():
                        near_work(u, w_pair, g_pair)

            if spread:
                newest(t - 1)

    if spread:
        newest(steps - 1)

    total = n * n_freq
    rank = me * n_freq + fq
    red[rank] = jnp.sum(acc[...], axis=1) / stations

    def share_copy(k, source):
        target = lax.rem(rank + k, total)
        return remote(
            red.at[source], red.at[source], red_send.at[k - 1], red_recv.at[k - 1],
            {"stn": target // n_freq, "freq": lax.rem(target, n_freq)},
        )

    @pl.loop(1, total)
    def _(k):
        share_copy(k, rank).start()

    @pl.loop(1, total)
    def _(k):
        share_copy(k, lax.rem(rank - k + total, total)).wait_recv()

    raw = red[0]
    for d in range(1, total):
        raw = raw + red[d]
    max_out[...] = jnp.broadcast_to(jnp.max(jnp.abs(raw)), max_out.shape)
    max_copy = remote(max_out, max_in, max_sem.at[0], max_sem.at[1], {"pts": 1 - core})
    max_copy.start()

    @pl.loop(1, total)
    def _(k):
        share_copy(k, rank).wait_send()

    @pl.loop(0, 2 * nq)
    def _(i):
        pair_copy(i).wait_send()

    @pl.loop(0, n)
    def _(j):
        w_pair_copy(j).wait_send()

    sibling_copy(pair_rows).wait_send()
    ref = far.at[0, 0, 0]

    @pl.loop(0, jnp.where(inner, n_far, (edge + 1) * 4 * nq))
    def _(t):
        remote(ref, ref, in_send.at[t], far_recv.at[0], in_dev).wait_send()

    @pl.when(edge > 0)
    def _():
        @pl.loop(0, n_far)
        def _(t):
            remote(ref, ref, out_send.at[t], far_recv.at[0], out_dev).wait_send()

    max_copy.wait()
    largest = jnp.maximum(max_out[0:1, 0:1], max_in[0:1, 0:1])
    out[...] = raw / (largest + 1e-6)


def kernel_body(n, n_freq, greens, weights):
    _, _, h, points = greens.shape
    stations = weights.shape[3]
    half = points // 2
    chunk = LANES
    while chunk * 2 * h <= 32768 and half % (chunk * 2) == 0:
        chunk *= 2
    nq = half // chunk
    side_len = n // 4
    n_far = side_len * 2 * nq
    n_near = max(side_len - 1, 1) * 4 * nq
    blocked = h % LANES != 0
    if blocked:
        weights = weights.reshape(2, weights.shape[1], h, n, h).swapaxes(2, 3)
    if side_len == 2 and nq >= 4:
        return line_body(n_freq, chunk, nq, blocked, greens, weights)
    dma = pltpu.SemaphoreType.DMA
    bf16, f32 = jnp.bfloat16, jnp.float32
    rows = points // LANES
    out = pl.pallas_call(
        functools.partial(ring_kernel, n, n_freq, h, stations, chunk, nq, blocked),
        out_shape=jax.ShapeDtypeStruct((rows, LANES), f32),
        in_specs=[pl.BlockSpec(memory_space=pl.ANY)] * 2,
        out_specs=pl.BlockSpec(memory_space=pltpu.VMEM),
        scratch_shapes=[
            pltpu.VMEM((2 * nq, 2, h, chunk), bf16),
            pltpu.VMEM((2 * nq, 2, h, chunk), bf16),
            pltpu.VMEM((max(side_len - 1, 1), 2, 2 * nq, 2, h, chunk), bf16),
            pltpu.VMEM((side_len, 2, nq, 2, h, chunk), bf16),
            pltpu.VMEM((n, 2, h, h), bf16),
            pltpu.VMEM((n, 2, h, h), bf16),
            pltpu.VMEM((rows, 8, LANES), f32),
            pltpu.VMEM((n * n_freq, rows, LANES), f32),
            pltpu.VMEM((8, LANES), f32),
            pltpu.VMEM((8, LANES), f32),
            dma((2 * nq,)), dma((n,)), dma((2 * nq,)), dma((2 * nq,)), dma((n,)), dma((n,)), dma((2,)),
            dma((max(n_near, n_far),)), dma((n_near,)), dma((n_far,)), dma((n_far,)),
            dma((n * n_freq - 1,)), dma((n * n_freq - 1,)), dma((2,)),
            pltpu.SemaphoreType.REGULAR((2, n // 2 - 1)), pltpu.SemaphoreType.REGULAR((2,)),
        ],
        compiler_params=pltpu.CompilerParams(
            collective_id=0, has_side_effects=True, vmem_limit_bytes=60 * 1024 * 1024
        ),
    )(greens, weights)
    return out.reshape(points)


FAR_FIRST = (11, 9, 10, 8, 15, 7, 13, 14, 5, 6, 12, 4, 3, 1, 2, 0)


def line_kernel(
    n_freq, h, stations, chunk, nq, kept, late, blocked,
    greens, weights, out,
    g_own, g_pair, near, far, w_own, w_pair, w_edge, acc, part, side, sums, extras,
    own_sem, w_own_sem, pair_send, pair_recv, wp_send, wp_recv, sib_sem, we_send, we_recv, we_sib,
    in_send, near_recv, far_recv, down_send, back_send, part_send, part_recv, side_sem,
    extra_send, extra_recv, base_sem, hello_sem, pair_hello,
):
    n = 8
    sub = chunk // LANES
    half_rows = h // 2
    steps = 4 * nq
    me = lax.axis_index("stn")
    core = lax.axis_index("pts")
    fq = lax.axis_index("freq")
    parity = lax.rem(me, 2)
    z = me // 2
    hi = z // 2
    inner = jnp.logical_or(z == 1, z == 2)
    outer = jnp.logical_not(inner)
    s_base = hi * nq
    r_base = (1 - hi) * nq
    rank = me * n_freq + fq
    total = n * n_freq
    inward = jnp.where(hi == 1, -2, 2)
    pair_dev = {"stn": me + 1 - 2 * parity}
    in_dev = {"stn": me + inward}
    out_dev = {"stn": me - inward}
    core_dev = {"pts": 1 - core}
    freq_dev = {"freq": n_freq - 1 - fq}
    across_dev = {"stn": 2 * (3 - z) + parity}
    other_inner = 2 - hi
    other_edge = 3 - 3 * hi
    near_z = jnp.where(inner, z - inward // 2, z + inward // 2)

    def columns(q):
        return pl.ds(pl.multiple_of(q * chunk, LANES), chunk)

    def w_src(freq, j, rows):
        if blocked:
            return weights.at[:, freq, j, rows, :]
        return weights.at[:, freq, rows, pl.ds(pl.multiple_of(j * h, LANES), h)]

    def block_of(where, p):
        return 2 * where + jnp.where(p == 0, parity, 1 - parity)

    def far_block(e):
        return block_of(jnp.where(lax.rem(e, 2) == 0, other_inner, other_edge), e // 2)

    last_block = block_of(other_edge, 1)
    every_row = pl.ds(0, h)
    my_rows = pl.ds(pl.multiple_of(core * half_rows, 8), half_rows)
    sib_rows = pl.ds(pl.multiple_of((1 - core) * half_rows, 8), half_rows)

    def pair_q(i):
        return jnp.where(i < nq, s_base + i, r_base + i - nq)

    def g_src(q):
        return greens.at[:, parity, :, columns(q)]

    def own_copy(q):
        return pltpu.make_async_copy(g_src(q), g_own.at[q], own_sem.at[q])

    def w_own_copy(j):
        return pltpu.make_async_copy(w_src(parity, j, every_row), w_own.at[j], w_own_sem.at[j])

    def pair_copy(i):
        q = pair_q(i)
        return remote(
            greens.at[:, 1 - parity, :, columns(q)], g_pair.at[q],
            pair_send.at[i], pair_recv.at[i], pair_dev,
        )

    def w_pair_copy(j):
        return remote(
            w_src(1 - parity, j, my_rows), w_pair.at[j, :, my_rows, :],
            wp_send.at[j], wp_recv.at[j], pair_dev,
        )

    def sibling_copy(rows):
        part_of_w = w_pair.at[:, :, rows, :]
        return remote(part_of_w, part_of_w, sib_sem.at[0], sib_sem.at[1], core_dev)

    def edge_sibling_copy(rows):
        part_of_w = w_edge.at[:, :, rows, :]
        return remote(part_of_w, part_of_w, we_sib.at[0], we_sib.at[1], core_dev)

    def up_copy(src, p, i):
        slot = p * 2 * nq + i
        return remote(src, near.at[p, pair_q(i)], in_send.at[slot], near_recv.at[slot], in_dev)

    def up_weights(src, p):
        return remote(src, w_edge.at[p, :, my_rows, :], we_send.at[p], we_recv.at[p], in_dev)

    def mid_copy(src, slot):
        return remote(src, far.at[slot], in_send.at[slot], far_recv.at[slot], in_dev)

    def down_copy(slot):
        return remote(far.at[slot], far.at[slot], down_send.at[slot], far_recv.at[slot], out_dev)

    def back_copy(src, p, c):
        return remote(
            src, near.at[p, (1 - hi) * nq + c], back_send.at[p * kept + c],
            near_recv.at[p * 2 * nq + nq + c], out_dev,
        )

    barrier = pltpu.get_barrier_semaphore()
    up, down = z < 3, z > 0
    greeted = [pair_dev, core_dev, freq_dev]

    def greet(sem, device):
        pl.semaphore_signal(sem, inc=1, device_id=device, device_id_type=MESH)

    def along_z(sem_down, sem_up):
        @pl.when(up)
        def _():
            greet(sem_up, {"stn": me + 2})

        @pl.when(down)
        def _():
            greet(sem_down, {"stn": me - 2})

    along_z(barrier, barrier)
    for device in greeted:
        greet(barrier, device)
    pl.semaphore_wait(barrier, len(greeted) + up.astype(jnp.int32) + down.astype(jnp.int32))

    @pl.loop(0, nq)
    def _(i):
        src = g_src(pair_q(i))

        @pl.when(inner)
        def _():
            mid_copy(src, i).start()

        @pl.when(outer)
        def _():
            up_copy(src, 0, i).start()

    @pl.loop(0, n)
    def _(j):
        w_pair_copy(j).start()
        w_own_copy(j).start()

    @pl.loop(0, 2 * nq)
    def _(i):
        own_copy(pair_q(i)).start()
        pair_copy(i).start()

    @pl.loop(nq, 2 * nq)
    def _(i):
        src = g_src(pair_q(i))

        @pl.when(jnp.logical_and(inner, i < nq + kept))
        def _():
            back_copy(src, 0, i - nq).start()

        @pl.when(jnp.logical_and(outer, i >= nq + kept))
        def _():
            up_copy(src, 0, i).start()

    @pl.when(outer)
    def _():
        up_weights(w_src(parity, last_block, my_rows), 0).start()

    @pl.loop(0, 3)
    def _(r):
        along_z(hello_sem.at[0, r], hello_sem.at[1, r])

        @pl.when(up)
        def _():
            pl.semaphore_wait(hello_sem.at[0, r], 1)

        @pl.when(down)
        def _():
            pl.semaphore_wait(hello_sem.at[1, r], 1)

    for i, device in enumerate((pair_dev, freq_dev, core_dev)):
        greet(pair_hello.at[i], device)
        pl.semaphore_wait(pair_hello.at[i], 1)

    acc[...] = jnp.zeros_like(acc)

    @pl.loop(0, 2 * nq)
    def _(q):
        own_copy(q).wait()

    @pl.loop(0, n)
    def _(j):
        w_own_copy(j).wait()

    def product(w, gi, gj, s):
        lanes = slice(s * LANES, (s + 1) * LANES)
        both = jnp.concatenate([gj[0, :, lanes], gj[1, :, lanes]], axis=1)
        ab = jnp.dot(w[...].reshape(2 * h, h), both, preferred_element_type=jnp.float32)
        a, b = ab[:h], ab[h:]
        t = gi[0, :, lanes].astype(jnp.float32) * (a[:, :LANES] - b[:, LANES:])
        t = t + gi[1, :, lanes].astype(jnp.float32) * (a[:, LANES:] + b[:, :LANES])
        return jnp.sum(t.reshape(h // 8, 8, LANES), axis=0)

    def contribute(w, gi, gj, q, weight):
        for s in range(sub):
            acc[q * sub + s] += product(w, gi, gj, s) * weight

    own_pair_block = block_of(z, 1)

    def own_work(q):
        contribute(w_own.at[me], g_own.at[q], g_own.at[q], q, 1.0)

    def cross_work(q):
        contribute(w_own.at[own_pair_block], g_own.at[q], g_pair.at[q], q, 2.0)

    def pair_work(q):
        contribute(w_pair.at[own_pair_block], g_pair.at[q], g_pair.at[q], q, 1.0)

    def far_work(slot, w, g):
        q = r_base + lax.rem(slot, nq)
        contribute(w.at[far_block(slot // nq)], g.at[q], far.at[slot], q, 2.0)

    def near_work(p, q, w, g):
        contribute(w.at[block_of(near_z, p)], g.at[q], near.at[p, q], q, 2.0)

    def edge_work(c):
        q = r_base + c

        @pl.loop(0, 2)
        def _(p):
            contribute(w_edge.at[p], near.at[p, q], far.at[3 * nq + c], q, 2.0)

    def wait_far(t):
        ref = far.at[t]
        remote(ref, ref, down_send.at[t], far_recv.at[t], in_dev).wait_recv()

    def wait_near(p, i):
        slot = p * 2 * nq + i
        ref = near.at[p, pair_q(i)]
        remote(ref, ref, in_send.at[slot], near_recv.at[slot], in_dev).wait_recv()

    def wait_w_pair():
        @pl.loop(0, n)
        def _(j):
            w_pair_copy(j).wait_recv()

        sibling_copy(my_rows).start()

    def share_part():
        part[rank] = jnp.sum(acc[...], axis=1) / stations

        @pl.loop(0, total // 2 - 1)
        def _(k):
            part_copy(total // 2 - 1 - k, rank).start()

    def at_rank(target):
        return {"stn": target // n_freq, "freq": lax.rem(target, n_freq)}

    def flipped(k):
        bit, flip = total // 2, jnp.int32(0)
        while bit:
            mine = lax.rem(rank // bit, 2)
            turn = lax.rem(k // bit, 2)
            flip = flip + bit * (mine + turn - 2 * mine * turn)
            bit //= 2
        return flip

    def part_copy(k, source):
        ref = part.at[source]
        return remote(ref, ref, part_send.at[k - 1], part_recv.at[k - 1], at_rank(flipped(k)))

    my_group = (hi * 2 + parity) * n_freq + fq
    late_rows = late * sub

    sends = [(k, other) for k in FAR_FIRST for other in range(2) if k or other]

    def extra_copy(k, other):
        def turned(v, bit):
            return 1 - v if k & bit else v

        target_z = 2 * turned(hi, 8) + turned(lax.rem(z, 2), 4)
        target = {
            "stn": 2 * target_z + turned(parity, 2), "freq": turned(fq, 1),
            "pts": 1 - core if other else core,
        }
        return remote(
            extras.at[0, my_group], extras.at[other, my_group],
            extra_send.at[other, k], extra_recv.at[other], target,
        )

    def finish():
        first = (r_base + nq - late) * sub
        q, slot = r_base + nq - 1, steps - 1
        j = far_block(3)
        for c in range(late_rows - sub):
            row = jnp.sum(acc[first + c], axis=0, keepdims=True) / stations
            extras[0, my_group, c] = row
        wait_far(slot)
        for s in range(sub):
            gj = far.at[slot]
            t = product(w_own.at[j], g_own.at[q], gj, s)
            t = t + product(w_pair.at[j], g_pair.at[q], gj, s)
            for p in range(2):
                t = t + product(w_edge.at[p], near.at[p, q], gj, s)
            t = acc[q * sub + s] + 2.0 * t
            row = jnp.sum(t, axis=0, keepdims=True) / stations
            extras[0, my_group, late_rows - sub + s] = row
        for k, other in sends:
            extra_copy(k, other).start()

    near_second = 2 * nq - kept + 1
    near_third = 3 * nq - kept + 2
    near_end = 4 * nq - 2 * kept + 2

    def near_at(t):
        second = t >= near_second
        third = t >= near_third
        i = jnp.where(t < nq, t, t + kept)
        i = jnp.where(second, t - near_second, i)
        i = jnp.where(third, t - near_third + nq + kept, i)
        present = jnp.logical_and(t != near_second - 1, t != near_third - 1)
        return jnp.logical_and(present, t < near_end), second.astype(jnp.int32), i

    @pl.when(inner)
    def _():
        @pl.loop(0, steps - 1)
        def _(t):
            has_near, p, i = near_at(t)
            has_pair = jnp.logical_and(t >= nq, t < 3 * nq)
            turn = t - nq
            wait_far(t)

            @pl.when(t < 3 * nq + kept)
            def _():
                down_copy(t).start()

            @pl.when(has_near)
            def _():
                wait_near(p, i)

                @pl.when(i < nq)
                def _():
                    mid_copy(near.at[p, pair_q(i)], (2 * p + 1) * nq + i).start()

            @pl.when(t == nq)
            def _():
                wait_w_pair()

            @pl.when(has_pair)
            def _():
                pair_copy(turn).wait_recv()

                @pl.when(turn < nq)
                def _():
                    mid_copy(g_pair.at[pair_q(turn)], 2 * nq + turn).start()

                @pl.when(jnp.logical_and(turn >= nq, turn < nq + kept))
                def _():
                    back_copy(g_pair.at[pair_q(turn)], 1, turn - nq).start()

            @pl.when(t == nq + 2)
            def _():
                sibling_copy(sib_rows).wait_recv()

            @pl.when(t == 3 * nq + kept - 1)
            def _():
                for r in range(2):
                    up_weights(w_edge.at[r, :, my_rows, :], r).wait_recv()
                edge_sibling_copy(my_rows).start()

            @pl.when(t == 3 * nq + kept)
            def _():
                edge_sibling_copy(sib_rows).wait_recv()

            far_work(t, w_own, g_own)

            @pl.when(t < 2 * nq)
            def _():
                own_work(t)

            @pl.when(has_near)
            def _():
                q = pair_q(i)
                near_work(p, q, w_own, g_own)

                @pl.when(p == 1)
                def _():
                    near_work(p, q, w_pair, g_pair)

            @pl.when(has_pair)
            def _():
                cross_work(pair_q(turn))

            lag = t - nq - 2

            @pl.when(jnp.logical_and(lag >= 0, lag < 2 * nq))
            def _():
                pair_work(pair_q(lag))

                @pl.when(lag < nq)
                def _():
                    near_work(0, pair_q(lag), w_pair, g_pair)

            @pl.when(jnp.logical_and(t >= 2 * nq, t < 3 * nq))
            def _():
                @pl.loop(0, 3)
                def _(e):
                    far_work(e * nq + t - 2 * nq, w_pair, g_pair)

                @pl.when(t >= 2 * nq + kept)
                def _():
                    near_work(0, r_base + t - 2 * nq, w_pair, g_pair)

            @pl.when(t >= 3 * nq)
            def _():
                far_work(t, w_pair, g_pair)

            @pl.when(t >= 3 * nq + kept)
            def _():
                edge_work(t - 3 * nq)

            @pl.when(t == steps - late - 1)
            def _():
                share_part()

                @pl.loop((nq - late) * sub, nq * sub)
                def _(c):
                    acc[r_base * sub + c] = jnp.zeros((8, LANES), jnp.float32)

        finish()

    @pl.when(outer)
    def _():
        @pl.loop(0, 3 * nq + kept)
        def _(t):
            turn = t - nq + 2
            has_pair = jnp.logical_and(turn >= 0, turn < 2 * nq)
            back = t - 2 * nq - 4

            @pl.when(turn == 0)
            def _():
                wait_w_pair()

            @pl.when(has_pair)
            def _():
                pair_copy(turn).wait_recv()

                @pl.when(jnp.logical_or(turn < nq, turn >= nq + kept))
                def _():
                    up_copy(g_pair.at[pair_q(turn)], 1, turn).start()

                @pl.when(turn == nq - 1)
                def _():
                    up_weights(w_pair.at[last_block, :, my_rows, :], 1).start()

            @pl.when(t == nq)
            def _():
                sibling_copy(sib_rows).wait_recv()

            @pl.when(t < kept)
            def _():
                wait_near(0, nq + t)

            @pl.when(jnp.logical_and(back >= 0, back < kept))
            def _():
                wait_near(1, nq + back)

            wait_far(t)
            far_work(t, w_own, g_own)

            @pl.when(t < 2 * nq)
            def _():
                own_work(t)

            @pl.when(t < kept)
            def _():
                near_work(0, r_base + t, w_own, g_own)

            @pl.when(jnp.logical_and(back >= 0, back < kept))
            def _():
                q = r_base + back
                near_work(0, q, w_pair, g_pair)
                near_work(1, q, w_own, g_own)
                near_work(1, q, w_pair, g_pair)

            @pl.when(has_pair)
            def _():
                cross_work(pair_q(turn))

            @pl.when(jnp.logical_and(t >= nq, t < 3 * nq))
            def _():
                pair_work(pair_q(t - nq))

            @pl.when(jnp.logical_and(t >= 2 * nq, t < 3 * nq))
            def _():
                @pl.loop(0, 3)
                def _(e):
                    far_work(e * nq + t - 2 * nq, w_pair, g_pair)

            @pl.when(t >= 3 * nq)
            def _():
                far_work(t, w_pair, g_pair)

        share_part()

    @pl.loop(1, total // 2)
    def _(k):
        part_copy(k, flipped(k)).wait_recv()

    base = hi * (total // 2)
    mine = part[base]
    for d in range(1, total // 2):
        mine = mine + part[base + d]
    side[hi] = mine

    def side_copy(which):
        ref = side.at[which]
        return remote(ref, ref, side_sem.at[0], side_sem.at[1], across_dev)

    side_copy(hi).start()
    side_copy(1 - hi).wait_recv()
    sums[0] = side[0] + side[1]
    base_copy = remote(sums.at[0], sums.at[1], base_sem.at[0], base_sem.at[1], core_dev)
    base_copy.start()

    @pl.loop(0, 2 * nq)
    def _(i):
        pair_copy(i).wait_send()

    @pl.loop(0, n)
    def _(j):
        w_pair_copy(j).wait_send()

    sibling_copy(my_rows).wait_send()

    @pl.loop(1, total // 2)
    def _(k):
        part_copy(k, rank).wait_send()

    @pl.when(inner)
    def _():
        @pl.loop(0, steps)
        def _(t):
            mid_copy(far.at[t], t).wait_send()

            @pl.when(t < 3 * nq + kept)
            def _():
                down_copy(t).wait_send()

        @pl.loop(0, 2 * kept)
        def _(i):
            back_copy(g_own.at[0], i // kept, lax.rem(i, kept)).wait_send()

        for k, other in sends:
            extra_copy(k, other).wait_send()

        edge_sibling_copy(my_rows).wait_send()

    @pl.when(outer)
    def _():
        @pl.loop(0, 4 * nq)
        def _(s):
            i = lax.rem(s, 2 * nq)

            @pl.when(jnp.logical_or(i < nq, i >= nq + kept))
            def _():
                up_copy(g_own.at[0], s // (2 * nq), i).wait_send()

        for r in range(2):
            up_weights(w_edge.at[r, :, my_rows, :], r).wait_send()

    side_copy(hi).wait_send()

    def wait_extras(which, groups):
        ref = extras.at[which, pl.ds(0, groups)]
        remote(ref, ref, extra_send.at[0, 0], extra_recv.at[which], core_dev).wait_recv()

    @pl.when(inner)
    def _():
        wait_extras(0, 4 * n_freq - 1)

    @pl.when(outer)
    def _():
        wait_extras(0, 4 * n_freq)

    wait_extras(1, 4 * n_freq)
    base_copy.wait()

    for which in range(2):
        for low in range(2):
            for c in range(late_rows):
                row = extras[which, low * 2 * n_freq, c]
                for g in range(1, 2 * n_freq):
                    row = row + extras[which, low * 2 * n_freq + g, c]
                at = ((1 - low) * nq + nq - late) * sub + c
                sums[which, at:at + 1, :] += row

    raw = sums[0]
    largest = jnp.max(jnp.maximum(jnp.abs(raw), jnp.abs(sums[1])), keepdims=True)
    out[...] = raw / (largest + 1e-6)


def line_body(n_freq, chunk, nq, blocked, greens, weights):
    _, _, h, points = greens.shape
    n = 8
    kept, late = nq // 4, 3
    stations = n * h
    dma = pltpu.SemaphoreType.DMA
    regular = pltpu.SemaphoreType.REGULAR
    bf16, f32 = jnp.bfloat16, jnp.float32
    rows = points // LANES
    late_rows = late * (chunk // LANES)
    total = n * n_freq
    out = pl.pallas_call(
        functools.partial(line_kernel, n_freq, h, stations, chunk, nq, kept, late, blocked),
        out_shape=pltpu.VMEM((rows, LANES), f32),
        in_specs=[pl.BlockSpec(memory_space=pl.ANY)] * 2,
        out_specs=pl.BlockSpec(memory_space=pltpu.VMEM),
        scratch_shapes=[
            pltpu.VMEM((2 * nq, 2, h, chunk), bf16),
            pltpu.VMEM((2 * nq, 2, h, chunk), bf16),
            pltpu.VMEM((2, 2 * nq, 2, h, chunk), bf16),
            pltpu.VMEM((4 * nq, 2, h, chunk), bf16),
            pltpu.VMEM((n, 2, h, h), bf16),
            pltpu.VMEM((n, 2, h, h), bf16),
            pltpu.VMEM((2, 2, h, h), bf16),
            pltpu.VMEM((rows, 8, LANES), f32),
            pltpu.VMEM((total, rows, LANES), f32),
            pltpu.VMEM((2, rows, LANES), f32),
            pltpu.VMEM((2, rows, LANES), f32),
            pltpu.VMEM((2, 4 * n_freq, late_rows, 1, LANES), f32),
            dma((2 * nq,)), dma((n,)), dma((2 * nq,)), dma((2 * nq,)), dma((n,)), dma((n,)), dma((2,)),
            dma((2,)), dma((2,)), dma((2,)),
            dma((4 * nq,)), dma((4 * nq,)), dma((4 * nq,)), dma((4 * nq,)), dma((2 * kept,)),
            dma((total // 2 - 1,)), dma((total // 2 - 1,)), dma((2,)),
            dma((2, total)), dma((2,)), dma((2,)),
            regular((2, 3)), regular((3,)),
        ],
        compiler_params=pltpu.CompilerParams(
            collective_id=0, has_side_effects=True, vmem_limit_bytes=60 * 1024 * 1024
        ),
    )(greens, weights)
    return out.reshape(points)


def passed_along(x, axis, by):
    size = lax.axis_size(axis)
    return lax.ppermute(x, axis, [(i, (i + by) % size) for i in range(size)])


def mixing_of(weights):
    negated = -weights[1]
    return jnp.stack([jnp.stack([weights[0], negated]), jnp.stack([weights[1], weights[0]])])


def body(greens, noise_weights):
    station_rows = greens.shape[2]
    stations = noise_weights.shape[3]
    device_index = lax.axis_index("stn")
    cycle_length = lax.axis_size("stn")
    mixing = mixing_of(noise_weights)

    def block_product(columns_start, arriving):
        block_rows = arriving.shape[2]
        weights_block = lax.dynamic_slice_in_dim(mixing, columns_start, block_rows, 4)
        return jnp.einsum(
            "ocfin,cfnx->ofix", weights_block, arriving, preferred_element_type=jnp.float32
        )

    half_way = cycle_length // 2
    diagonal = block_product(device_index * station_rows, greens)

    def advance(offset, loop_state):
        running, current = loop_state
        current = passed_along(current, "stn", -1)
        source = (device_index + offset) % cycle_length
        weight = jnp.where(offset == half_way, 1.0, 2.0).astype(jnp.float32)
        running = running + weight * block_product(source * station_rows, current)
        return (running, current)

    summed, current = lax.fori_loop(1, half_way + 1, advance, (diagonal, greens))
    green_real = greens[0].astype(jnp.float32)
    green_imag = greens[1].astype(jnp.float32)
    partial_kernel = (
        jnp.sum(green_real * summed[0] + green_imag * summed[1], axis=(0, 1)) / stations
    )
    raw_kernel = lax.psum(partial_kernel, "stn")
    raw_kernel = lax.psum(raw_kernel, "freq")
    largest = lax.pmax(jnp.max(jnp.abs(raw_kernel)), "pts")
    return raw_kernel / (largest + 1e-06)


def solution(mesh):
    n, cores, n_freq = mesh.shape["stn"], mesh.shape["pts"], mesh.shape["freq"]

    def either(greens, noise_weights):
        _, freqs, rows, points = greens.shape
        fits = n % 4 == 0 and cores == 2 and freqs == 2 and n_freq == 2 and rows % 32 == 0 and points % (2 * LANES) == 0
        if fits:
            return kernel_body(n, n_freq, greens, noise_weights)
        return body(greens, noise_weights)

    in_specs = (P(None, "freq", "stn", "pts"), P(None, "freq", "stn", None))
    return jax.shard_map(either, mesh=mesh, in_specs=in_specs, out_specs=P("pts"), check_vma=False)
```

```python
import functools

import jax
import jax.numpy as jnp
from jax import lax
from jax.experimental import pallas as pl
from jax.experimental.pallas import tpu as pltpu
from jax.sharding import PartitionSpec as P

MESH = pl.DeviceIdType.MESH
LANES = 128


def remote(src, dst, send_sem, recv_sem, target):
    return pltpu.make_async_remote_copy(
        src_ref=src, dst_ref=dst, send_sem=send_sem, recv_sem=recv_sem,
        device_id=target, device_id_type=MESH,
    )


def ring_kernel(
    n, n_freq, h, stations, chunk, nq, blocked,
    greens, weights, out,
    g_own, g_pair, near, far, w_own, w_pair, acc, red, max_out, max_in,
    own_sem, w_own_sem, pair_send, pair_recv, wp_send, wp_recv, sib_sem,
    in_send, in_recv, out_send, far_recv, red_send, red_recv, max_sem, hello_sem, pair_hello,
):
    m = n // 2
    side_len = m // 2
    sub = chunk // LANES
    half_rows = h // 2
    me = lax.axis_index("stn")
    core = lax.axis_index("pts")
    fq = lax.axis_index("freq")
    parity = lax.rem(me, 2)
    z = me // 2
    hi = (z >= side_len).astype(jnp.int32)
    edge = jnp.where(hi == 1, m - 1 - z, z)
    inward = jnp.where(hi == 1, -2, 2)
    inner = edge == side_len - 1
    s_base = hi * nq
    r_base = (1 - hi) * nq
    pair_dev = {"stn": me + 1 - 2 * parity}
    in_dev = {"stn": me + inward}
    out_dev = {"stn": me - inward}
    n_far = side_len * 2 * nq
    n_near = edge * 4 * nq
    n_near_max = (side_len - 1) * 4 * nq
    steps = max(n_far, n_near_max, 3 * nq + 2)
    spread = side_len == 2
    catch_up = 2 * nq + 1 if spread else max((steps * 25) // 32, 3 * nq + 1)
    left = steps - catch_up
    per_step = -(-steps // (steps - catch_up))

    def columns(q):
        return pl.ds(pl.multiple_of(q * chunk, LANES), chunk)

    def w_src(freq, j, rows):
        if blocked:
            return weights.at[:, freq, j, rows, :]
        return weights.at[:, freq, rows, pl.ds(pl.multiple_of(j * h, LANES), h)]

    def global_block(e, opposite):
        low = jnp.where(opposite, 1 - hi, hi) == 0
        return jnp.where(low, e, m - 1 - e)

    def near_slot(receiver_edge, p, half, b, c):
        return ((p * 2 + half) * receiver_edge + (receiver_edge - 1 - b)) * nq + c

    def far_slot(p, b, c):
        return (p * side_len + (side_len - 1 - b)) * nq + c

    def send_inward(src, p, half, b, c):
        q = jnp.where(half == 0, s_base, r_base) + c

        if side_len > 1:
            @pl.when(jnp.logical_not(inner))
            def _():
                slot = near_slot(edge + 1, p, half, b, c)
                remote(src, near.at[b, p, q], in_send.at[slot], in_recv.at[slot], in_dev).start()

        @pl.when(jnp.logical_and(inner, half == 0))
        def _():
            slot = far_slot(p, b, c)
            remote(src, far.at[b, p, c], in_send.at[slot], far_recv.at[slot], in_dev).start()

    freq_dev = {"freq": n_freq - 1 - fq}
    barrier = pltpu.get_barrier_semaphore()
    up, down = z < m - 1, z > 0
    greeted = [pair_dev, {"pts": 1 - core}, freq_dev]

    def greet(sem, device):
        pl.semaphore_signal(sem, inc=1, device_id=device, device_id_type=MESH)

    def along_z(sem_down, sem_up):
        @pl.when(up)
        def _():
            greet(sem_up, {"stn": me + 2})

        @pl.when(down)
        def _():
            greet(sem_down, {"stn": me - 2})

    for device in greeted:
        greet(barrier, device)
    along_z(barrier, barrier)
    pl.semaphore_wait(barrier, len(greeted) + up.astype(jnp.int32) + down.astype(jnp.int32))

    def hello():
        @pl.loop(0, m - 1)
        def _(r):
            along_z(hello_sem.at[0, r], hello_sem.at[1, r])

            @pl.when(up)
            def _():
                pl.semaphore_wait(hello_sem.at[0, r], 1)

            @pl.when(down)
            def _():
                pl.semaphore_wait(hello_sem.at[1, r], 1)

        for i, device in enumerate((pair_dev, freq_dev)):
            greet(pair_hello.at[i], device)
            pl.semaphore_wait(pair_hello.at[i], 1)

    every_row = pl.ds(0, h)
    pair_rows = pl.ds(pl.multiple_of(core * half_rows, 8), half_rows)

    def pair_q(i):
        return jnp.where(i < nq, s_base + i, r_base + i - nq)

    def pair_copy(i):
        q = pair_q(i)
        return remote(
            greens.at[:, 1 - parity, :, columns(q)], g_pair.at[q],
            pair_send.at[i], pair_recv.at[i], pair_dev,
        )

    def w_pair_copy(j):
        return remote(
            w_src(1 - parity, j, pair_rows), w_pair.at[j, :, pair_rows, :],
            wp_send.at[j], wp_recv.at[j], pair_dev,
        )

    def sibling_copy(rows):
        return remote(
            w_pair.at[:, :, rows, :], w_pair.at[:, :, rows, :],
            sib_sem.at[0], sib_sem.at[1], {"pts": 1 - core},
        )

    def own_copy(q):
        return pltpu.make_async_copy(
            greens.at[:, parity, :, columns(q)], g_own.at[q], own_sem.at[q]
        )

    def w_own_copy(j):
        return pltpu.make_async_copy(w_src(parity, j, every_row), w_own.at[j], w_own_sem.at[j])

    @pl.loop(0, 2 * nq)
    def _(i):
        @pl.when(i < nq)
        def _():
            pair_copy(i).start()

        half = i // nq
        c = lax.rem(i, nq)
        send_inward(greens.at[:, parity, :, columns(pair_q(i))], 0, half, edge, c)
        own_copy(i).start()

    @pl.loop(0, n)
    def _(j):
        w_pair_copy(j).start()
        w_own_copy(j).start()

    @pl.loop(nq, 2 * nq)
    def _(i):
        pair_copy(i).start()

    hello()

    acc[...] = jnp.zeros_like(acc)

    @pl.loop(0, 2 * nq)
    def _(q):
        own_copy(q).wait()

    @pl.loop(0, n)
    def _(j):
        w_own_copy(j).wait()

    def contribute(w, gi, gj, q, weight):
        for s in range(sub):
            part = slice(s * LANES, (s + 1) * LANES)
            both = jnp.concatenate([gj[0, :, part], gj[1, :, part]], axis=1)
            ab = jnp.dot(w[...].reshape(2 * h, h), both, preferred_element_type=jnp.float32)
            a, b = ab[:h], ab[h:]
            t = gi[0, :, part].astype(jnp.float32) * (a[:, :LANES] - b[:, LANES:])
            t = t + gi[1, :, part].astype(jnp.float32) * (a[:, LANES:] + b[:, :LANES])
            t = jnp.sum(t.reshape(h // 8, 8, LANES), axis=0)
            acc[q * sub + s] += t * weight

    def far_at(t):
        p = t // (side_len * nq)
        rest = lax.rem(t, side_len * nq)
        return p, side_len - 1 - rest // nq, lax.rem(rest, nq)

    def near_at(t):
        width = jnp.maximum(edge, 1) * nq
        p = t // (2 * width)
        half = lax.rem(t // width, 2)
        rest = lax.rem(t, width)
        return p, half, jnp.maximum(edge, 1) - 1 - rest // nq, lax.rem(rest, nq)

    def part_of(p):
        return jnp.where(p == 0, parity, 1 - parity)

    def far_work(t, w, g):
        p, b, c = far_at(t)
        q = r_base + c
        j = global_block(b, True) * 2 + part_of(p)
        contribute(w.at[j], g.at[q], far.at[b, p, c], q, 2.0)

    def near_work(t, w, g):
        p, half, b, c = near_at(t)
        q = jnp.where(half == 0, s_base, r_base) + c
        j = global_block(b, False) * 2 + part_of(p)
        contribute(w.at[j], g.at[q], near.at[b, p, q], q, 2.0)

    def far_wait(t):
        p, b, c = far_at(t)
        ref = far.at[b, p, c]
        remote(ref, ref, out_send.at[t], far_recv.at[t], in_dev).wait_recv()

        @pl.when(edge > 0)
        def _():
            remote(ref, ref, out_send.at[t], far_recv.at[t], out_dev).start()

    def near_wait(t):
        p, half, b, c = near_at(t)
        q = jnp.where(half == 0, s_base, r_base) + c
        ref = near.at[b, p, q]
        remote(ref, ref, in_send.at[t], in_recv.at[t], out_dev).wait_recv()
        send_inward(ref, p, half, b, c)

    def newest(u):
        far_work(u, w_pair, g_pair)

        @pl.when(u < n_near)
        def _():
            near_work(u, w_pair, g_pair)

    @pl.loop(0, steps)
    def _(t):
        has_pair = jnp.logical_and(jnp.logical_and(t >= nq, t <= 3 * nq), t != 2 * nq)
        turn = t - nq - (t > 2 * nq).astype(jnp.int32)

        @pl.when(has_pair)
        def _():
            i = turn
            pair_copy(i).wait_recv()
            send_inward(g_pair.at[pair_q(i)], 1, i // nq, edge, lax.rem(i, nq))

        @pl.when(t < n_far)
        def _():
            far_wait(t)

        if side_len > 1:
            @pl.when(t < n_near)
            def _():
                near_wait(t)

        @pl.when(t == catch_up - 1)
        def _():
            @pl.loop(0, n)
            def _(j):
                w_pair_copy(j).wait_recv()

            sibling_copy(pair_rows).start()

        @pl.when(t < 2 * nq)
        def _():
            contribute(w_own.at[2 * z + parity], g_own.at[t], g_own.at[t], t, 1.0)

        @pl.when(has_pair)
        def _():
            q = pair_q(turn)
            contribute(w_own.at[2 * z + 1 - parity], g_own.at[q], g_pair.at[q], q, 2.0)

        @pl.when(t < n_far)
        def _():
            far_work(t, w_own, g_own)

        if side_len > 1:
            @pl.when(t < n_near)
            def _():
                near_work(t, w_own, g_own)

        @pl.when(t == catch_up)
        def _():
            sibling_copy(pl.ds(pl.multiple_of((1 - core) * half_rows, 8), half_rows)).wait_recv()

        @pl.when(t >= catch_up)
        def _():
            first = (t - catch_up) * per_step
            last = jnp.minimum(first + per_step, steps)
            if spread:
                first = ((t - catch_up) * 2 * nq) // left
                last = ((t - catch_up + 1) * 2 * nq) // left

            @pl.loop(first, last)
            def _(u):
                @pl.when(u < 2 * nq)
                def _():
                    q = pair_q(u)
                    contribute(w_pair.at[2 * z + 1 - parity], g_pair.at[q], g_pair.at[q], q, 1.0)

                if spread:
                    far_work(lax.rem(u, side_len) * nq + u // side_len, w_pair, g_pair)
                else:
                    @pl.when(u < n_far)
                    def _():
                        far_work(u, w_pair, g_pair)

                if side_len > 1:
                    @pl.when(u < n_near)
                    def _():
                        near_work(u, w_pair, g_pair)

            if spread:
                newest(t - 1)

    if spread:
        newest(steps - 1)

    total = n * n_freq
    rank = me * n_freq + fq
    red[rank] = jnp.sum(acc[...], axis=1) / stations

    def share_copy(k, source):
        target = lax.rem(rank + k, total)
        return remote(
            red.at[source], red.at[source], red_send.at[k - 1], red_recv.at[k - 1],
            {"stn": target // n_freq, "freq": lax.rem(target, n_freq)},
        )

    @pl.loop(1, total)
    def _(k):
        share_copy(k, rank).start()

    @pl.loop(1, total)
    def _(k):
        share_copy(k, lax.rem(rank - k + total, total)).wait_recv()

    raw = red[0]
    for d in range(1, total):
        raw = raw + red[d]
    max_out[...] = jnp.broadcast_to(jnp.max(jnp.abs(raw)), max_out.shape)
    max_copy = remote(max_out, max_in, max_sem.at[0], max_sem.at[1], {"pts": 1 - core})
    max_copy.start()

    @pl.loop(1, total)
    def _(k):
        share_copy(k, rank).wait_send()

    @pl.loop(0, 2 * nq)
    def _(i):
        pair_copy(i).wait_send()

    @pl.loop(0, n)
    def _(j):
        w_pair_copy(j).wait_send()

    sibling_copy(pair_rows).wait_send()
    ref = far.at[0, 0, 0]

    @pl.loop(0, jnp.where(inner, n_far, (edge + 1) * 4 * nq))
    def _(t):
        remote(ref, ref, in_send.at[t], far_recv.at[0], in_dev).wait_send()

    @pl.when(edge > 0)
    def _():
        @pl.loop(0, n_far)
        def _(t):
            remote(ref, ref, out_send.at[t], far_recv.at[0], out_dev).wait_send()

    max_copy.wait()
    largest = jnp.maximum(max_out[0:1, 0:1], max_in[0:1, 0:1])
    out[...] = raw / (largest + 1e-6)


def kernel_body(n, n_freq, greens, weights):
    _, _, h, points = greens.shape
    stations = weights.shape[3]
    half = points // 2
    chunk = LANES
    while chunk * 2 * h <= 32768 and half % (chunk * 2) == 0:
        chunk *= 2
    nq = half // chunk
    side_len = n // 4
    n_far = side_len * 2 * nq
    n_near = max(side_len - 1, 1) * 4 * nq
    blocked = h % LANES != 0
    if blocked:
        weights = weights.reshape(2, weights.shape[1], h, n, h).swapaxes(2, 3)
    if side_len == 2 and nq >= 4:
        return line_body(n_freq, chunk, nq, blocked, greens, weights)
    dma = pltpu.SemaphoreType.DMA
    bf16, f32 = jnp.bfloat16, jnp.float32
    rows = points // LANES
    out = pl.pallas_call(
        functools.partial(ring_kernel, n, n_freq, h, stations, chunk, nq, blocked),
        out_shape=jax.ShapeDtypeStruct((rows, LANES), f32),
        in_specs=[pl.BlockSpec(memory_space=pl.ANY)] * 2,
        out_specs=pl.BlockSpec(memory_space=pltpu.VMEM),
        scratch_shapes=[
            pltpu.VMEM((2 * nq, 2, h, chunk), bf16),
            pltpu.VMEM((2 * nq, 2, h, chunk), bf16),
            pltpu.VMEM((max(side_len - 1, 1), 2, 2 * nq, 2, h, chunk), bf16),
            pltpu.VMEM((side_len, 2, nq, 2, h, chunk), bf16),
            pltpu.VMEM((n, 2, h, h), bf16),
            pltpu.VMEM((n, 2, h, h), bf16),
            pltpu.VMEM((rows, 8, LANES), f32),
            pltpu.VMEM((n * n_freq, rows, LANES), f32),
            pltpu.VMEM((8, LANES), f32),
            pltpu.VMEM((8, LANES), f32),
            dma((2 * nq,)), dma((n,)), dma((2 * nq,)), dma((2 * nq,)), dma((n,)), dma((n,)), dma((2,)),
            dma((max(n_near, n_far),)), dma((n_near,)), dma((n_far,)), dma((n_far,)),
            dma((n * n_freq - 1,)), dma((n * n_freq - 1,)), dma((2,)),
            pltpu.SemaphoreType.REGULAR((2, n // 2 - 1)), pltpu.SemaphoreType.REGULAR((2,)),
        ],
        compiler_params=pltpu.CompilerParams(
            collective_id=0, has_side_effects=True, vmem_limit_bytes=60 * 1024 * 1024
        ),
    )(greens, weights)
    return out.reshape(points)


FAR_FIRST = (11, 9, 10, 8, 15, 7, 13, 14, 5, 6, 12, 4, 3, 1, 2, 0)


def line_kernel(
    n_freq, h, stations, chunk, nq, kept, late, blocked,
    greens, weights, out,
    g_own, g_pair, near, far, w_own, w_pair, w_edge, folded, acc, part, side, sums, extras,
    own_sem, w_own_sem, pair_send, pair_recv, wp_send, wp_recv, sib_sem, we_send, we_recv, we_sib,
    in_send, near_recv, far_recv, down_send, back_send, part_send, part_recv, side_sem,
    extra_send, extra_recv, base_sem, fold_sem, hello_sem, pair_hello,
):
    n = 8
    sub = chunk // LANES
    half_rows = h // 2
    steps = 4 * nq
    me = lax.axis_index("stn")
    core = lax.axis_index("pts")
    fq = lax.axis_index("freq")
    parity = lax.rem(me, 2)
    z = me // 2
    hi = z // 2
    inner = jnp.logical_or(z == 1, z == 2)
    outer = jnp.logical_not(inner)
    s_base = hi * nq
    r_base = (1 - hi) * nq
    rank = me * n_freq + fq
    total = n * n_freq
    inward = jnp.where(hi == 1, -2, 2)
    pair_dev = {"stn": me + 1 - 2 * parity}
    in_dev = {"stn": me + inward}
    out_dev = {"stn": me - inward}
    core_dev = {"pts": 1 - core}
    freq_dev = {"freq": n_freq - 1 - fq}
    across_dev = {"stn": 2 * (3 - z) + parity}
    other_inner = 2 - hi
    other_edge = 3 - 3 * hi
    near_z = jnp.where(inner, z - inward // 2, z + inward // 2)

    def columns(q):
        return pl.ds(pl.multiple_of(q * chunk, LANES), chunk)

    def w_src(freq, j, rows):
        if blocked:
            return weights.at[:, freq, j, rows, :]
        return weights.at[:, freq, rows, pl.ds(pl.multiple_of(j * h, LANES), h)]

    def block_of(where, p):
        return 2 * where + jnp.where(p == 0, parity, 1 - parity)

    def far_block(e):
        return block_of(jnp.where(lax.rem(e, 2) == 0, other_inner, other_edge), e // 2)

    every_row = pl.ds(0, h)
    my_rows = pl.ds(pl.multiple_of(core * half_rows, 8), half_rows)
    sib_rows = pl.ds(pl.multiple_of((1 - core) * half_rows, 8), half_rows)

    def pair_q(i):
        return jnp.where(i < nq, s_base + i, r_base + i - nq)

    def g_src(q):
        return greens.at[:, parity, :, columns(q)]

    def own_copy(q):
        return pltpu.make_async_copy(g_src(q), g_own.at[q], own_sem.at[q])

    def w_own_copy(j):
        return pltpu.make_async_copy(w_src(parity, j, every_row), w_own.at[j], w_own_sem.at[j])

    def pair_copy(i):
        q = pair_q(i)
        return remote(
            greens.at[:, 1 - parity, :, columns(q)], g_pair.at[q],
            pair_send.at[i], pair_recv.at[i], pair_dev,
        )

    def w_pair_copy(j):
        return remote(
            w_src(1 - parity, j, my_rows), w_pair.at[j, :, my_rows, :],
            wp_send.at[j], wp_recv.at[j], pair_dev,
        )

    def sibling_copy(rows):
        part_of_w = w_pair.at[:, :, rows, :]
        return remote(part_of_w, part_of_w, sib_sem.at[0], sib_sem.at[1], core_dev)

    def edge_sibling_copy(rows):
        part_of_w = w_edge.at[:, :, :, rows, :]
        return remote(part_of_w, part_of_w, we_sib.at[0], we_sib.at[1], core_dev)

    def up_copy(src, p, i):
        slot = p * 2 * nq + i
        return remote(src, near.at[p, pair_q(i)], in_send.at[slot], near_recv.at[slot], in_dev)

    def up_weights(src, b, p):
        i = 2 * b + p
        return remote(src, w_edge.at[b, p, :, my_rows, :], we_send.at[i], we_recv.at[i], in_dev)

    def mid_copy(src, slot):
        last = slot == steps - 1
        land = jnp.where(jnp.logical_and(last, core == 0), steps, slot)
        target = {"stn": me + inward, "pts": jnp.where(last, 1, core)}
        return remote(src, far.at[land], in_send.at[slot], far_recv.at[land], target)

    def down_copy(slot):
        return remote(far.at[slot], far.at[slot], down_send.at[slot], far_recv.at[slot], out_dev)

    def back_copy(src, p, c):
        return remote(
            src, near.at[p, (1 - hi) * nq + c], back_send.at[p * kept + c],
            near_recv.at[p * 2 * nq + nq + c], out_dev,
        )

    barrier = pltpu.get_barrier_semaphore()
    up, down = z < 3, z > 0
    greeted = [pair_dev, core_dev, freq_dev]

    def greet(sem, device):
        pl.semaphore_signal(sem, inc=1, device_id=device, device_id_type=MESH)

    def along_z(sem_down, sem_up):
        @pl.when(up)
        def _():
            greet(sem_up, {"stn": me + 2})

        @pl.when(down)
        def _():
            greet(sem_down, {"stn": me - 2})

    along_z(barrier, barrier)
    for device in greeted:
        greet(barrier, device)
    pl.semaphore_wait(barrier, len(greeted) + up.astype(jnp.int32) + down.astype(jnp.int32))

    @pl.loop(0, nq)
    def _(i):
        src = g_src(pair_q(i))

        @pl.when(inner)
        def _():
            mid_copy(src, i).start()

        @pl.when(outer)
        def _():
            up_copy(src, 0, i).start()

    @pl.loop(0, n)
    def _(j):
        w_pair_copy(j).start()
        w_own_copy(j).start()

    @pl.loop(0, 2 * nq)
    def _(i):
        own_copy(pair_q(i)).start()
        pair_copy(i).start()

    @pl.loop(nq, 2 * nq)
    def _(i):
        src = g_src(pair_q(i))

        @pl.when(jnp.logical_and(inner, i < nq + kept))
        def _():
            back_copy(src, 0, i - nq).start()

        @pl.when(jnp.logical_and(outer, i >= nq + kept))
        def _():
            up_copy(src, 0, i).start()

    @pl.when(outer)
    def _():
        for b in range(2):
            up_weights(w_src(parity, far_block(2 + b), my_rows), b, 0).start()

    @pl.loop(0, 3)
    def _(r):
        along_z(hello_sem.at[0, r], hello_sem.at[1, r])

        @pl.when(up)
        def _():
            pl.semaphore_wait(hello_sem.at[0, r], 1)

        @pl.when(down)
        def _():
            pl.semaphore_wait(hello_sem.at[1, r], 1)

    for i, device in enumerate((pair_dev, freq_dev, core_dev)):
        greet(pair_hello.at[i], device)
        pl.semaphore_wait(pair_hello.at[i], 1)

    acc[...] = jnp.zeros_like(acc)

    @pl.loop(0, 2 * nq)
    def _(q):
        own_copy(q).wait()

    @pl.loop(0, n)
    def _(j):
        w_own_copy(j).wait()

    def product(w, gi, gj, s):
        lanes = slice(s * LANES, (s + 1) * LANES)
        both = jnp.concatenate([gj[0, :, lanes], gj[1, :, lanes]], axis=1)
        ab = jnp.dot(w[...].reshape(2 * h, h), both, preferred_element_type=jnp.float32)
        a, b = ab[:h], ab[h:]
        t = gi[0, :, lanes].astype(jnp.float32) * (a[:, :LANES] - b[:, LANES:])
        t = t + gi[1, :, lanes].astype(jnp.float32) * (a[:, LANES:] + b[:, :LANES])
        return jnp.sum(t.reshape(h // 8, 8, LANES), axis=0)

    def contribute(w, gi, gj, q, weight):
        for s in range(sub):
            acc[q * sub + s] += product(w, gi, gj, s) * weight

    own_pair_block = block_of(z, 1)

    def own_work(q):
        contribute(w_own.at[me], g_own.at[q], g_own.at[q], q, 1.0)

    def cross_work(q):
        contribute(w_own.at[own_pair_block], g_own.at[q], g_pair.at[q], q, 2.0)

    def pair_work(q):
        contribute(w_pair.at[own_pair_block], g_pair.at[q], g_pair.at[q], q, 1.0)

    def far_work(slot, w, g):
        q = r_base + lax.rem(slot, nq)
        contribute(w.at[far_block(slot // nq)], g.at[q], far.at[slot], q, 2.0)

    def near_work(p, q, w, g):
        contribute(w.at[block_of(near_z, p)], g.at[q], near.at[p, q], q, 2.0)

    def edge_work(b, c):
        q = r_base + c

        @pl.loop(0, 2)
        def _(p):
            contribute(w_edge.at[b, p], near.at[p, q], far.at[(2 + b) * nq + c], q, 2.0)

    def transposed(w, g):
        return lax.dot_general(w, g, (((0,), (0,)), ((), ())), preferred_element_type=jnp.float32)

    def fold(w, gi, s):
        lanes = slice(s * LANES, (s + 1) * LANES)
        both = jnp.concatenate([gi[0, :, lanes], gi[1, :, lanes]], axis=1)
        a, b = transposed(w[0], both), transposed(w[1], both)
        return a[:, :LANES] + b[:, LANES:], a[:, LANES:] - b[:, :LANES]

    def fold_last():
        q, j = r_base + nq - 1, far_block(3)
        for s in range(sub):
            lanes = slice(s * LANES, (s + 1) * LANES)
            re, im = fold(w_own.at[j], g_own.at[q], s)
            folded[core, 0, :, lanes] = re
            folded[core, 1, :, lanes] = im
            for w, g in ((w_pair.at[j], g_pair.at[q]), (w_edge.at[1, 0], near.at[0, q]), (w_edge.at[1, 1], near.at[1, q])):
                re, im = fold(w, g, s)
                folded[core, 0, :, lanes] += re
                folded[core, 1, :, lanes] += im

        @pl.when(core == 0)
        def _():
            fold_copy().start()

    def fold_copy():
        return remote(folded.at[0], folded.at[0], fold_sem.at[0], fold_sem.at[1], core_dev)

    def unfold(which, slot, s):
        lanes = slice(s * LANES, (s + 1) * LANES)
        t = far[slot, 0, :, lanes].astype(jnp.float32) * folded[which, 0, :, lanes]
        t = t + far[slot, 1, :, lanes].astype(jnp.float32) * folded[which, 1, :, lanes]
        return 2.0 * jnp.sum(t.reshape(h // 8, 8, LANES), axis=0)

    def passed_down(t):
        return jnp.logical_or(t < 2 * nq, lax.rem(t, nq) < kept)

    def wait_far(t):
        ref = far.at[t]
        remote(ref, ref, in_send.at[0], far_recv.at[t], in_dev).wait_recv()

    def wait_near(p, i):
        slot = p * 2 * nq + i
        ref = near.at[p, pair_q(i)]
        remote(ref, ref, in_send.at[slot], near_recv.at[slot], in_dev).wait_recv()

    def wait_w_pair():
        @pl.loop(0, n)
        def _(j):
            w_pair_copy(j).wait_recv()

        sibling_copy(my_rows).start()

    def share_part():
        part[rank] = jnp.sum(acc[...], axis=1) / stations

        @pl.loop(0, total // 2 - 1)
        def _(k):
            part_copy(total // 2 - 1 - k, rank).start()

    def at_rank(target):
        return {"stn": target // n_freq, "freq": lax.rem(target, n_freq)}

    def flipped(k):
        bit, flip = total // 2, jnp.int32(0)
        while bit:
            mine = lax.rem(rank // bit, 2)
            turn = lax.rem(k // bit, 2)
            flip = flip + bit * (mine + turn - 2 * mine * turn)
            bit //= 2
        return flip

    def part_copy(k, source):
        ref = part.at[source]
        return remote(ref, ref, part_send.at[k - 1], part_recv.at[k - 1], at_rank(flipped(k)))

    my_group = (hi * 2 + parity) * n_freq + fq
    late_rows = late * sub

    sends = [(k, other) for k in FAR_FIRST for other in range(2) if k or other]

    def extra_copy(k, other):
        def turned(v, bit):
            return 1 - v if k & bit else v

        target_z = 2 * turned(hi, 8) + turned(lax.rem(z, 2), 4)
        target = {
            "stn": 2 * target_z + turned(parity, 2), "freq": turned(fq, 1),
            "pts": 1 - core if other else core,
        }
        return remote(
            extras.at[core, my_group], extras.at[core, my_group],
            extra_send.at[other, k], extra_recv.at[core], target,
        )

    def late_row(t):
        return jnp.sum(t, axis=0, keepdims=True) / stations

    def finish():
        first = (r_base + nq - late) * sub
        for c in range(late_rows):
            extras[core, my_group, c] = late_row(acc[first + c])
        for s in range(sub):
            extras[core, my_group, late_rows + s] = jnp.zeros((1, LANES), jnp.float32)

        @pl.when(core == 1)
        def _():
            fold_copy().wait_recv()
            wait_far(steps)
            wait_far(steps - 1)
            for s in range(sub):
                c = late_rows - sub + s
                extras[1, my_group, c] = late_row(acc[first + c] + unfold(1, steps - 1, s))
                extras[1, my_group, late_rows + s] = late_row(unfold(0, steps, s))

        for k, other in sends:
            extra_copy(k, other).start()

    near_second = 2 * nq - kept + 4
    near_third = near_second + nq
    near_end = near_third + nq - kept

    def near_at(t):
        second = t >= near_second
        i = jnp.where(t < nq, t, t + kept)
        i = jnp.where(second, t - near_second, i)
        i = jnp.where(t >= near_third, t - near_third + nq + kept, i)
        present = jnp.logical_or(t < 2 * nq - kept, jnp.logical_and(second, t < near_end))
        return present, second.astype(jnp.int32), i

    @pl.when(inner)
    def _():
        @pl.loop(0, steps - 1)
        def _(t):
            has_near, p, i = near_at(t)
            has_pair = jnp.logical_and(t >= nq, t < 3 * nq)
            turn = t - nq
            wait_far(t)

            @pl.when(passed_down(t))
            def _():
                down_copy(t).start()

            @pl.when(has_near)
            def _():
                wait_near(p, i)

                @pl.when(i < nq)
                def _():
                    mid_copy(near.at[p, pair_q(i)], (2 * p + 1) * nq + i).start()

            @pl.when(t == nq)
            def _():
                wait_w_pair()

            @pl.when(has_pair)
            def _():
                pair_copy(turn).wait_recv()

                @pl.when(turn < nq)
                def _():
                    mid_copy(g_pair.at[pair_q(turn)], 2 * nq + turn).start()

                @pl.when(jnp.logical_and(turn >= nq, turn < nq + kept))
                def _():
                    back_copy(g_pair.at[pair_q(turn)], 1, turn - nq).start()

            @pl.when(t == nq + 2)
            def _():
                sibling_copy(sib_rows).wait_recv()

            @pl.when(t == near_second)
            def _():
                for r in range(4):
                    part_of_w = w_edge.at[r // 2, r % 2, :, my_rows, :]
                    up_weights(part_of_w, r // 2, r % 2).wait_recv()
                edge_sibling_copy(my_rows).start()

            @pl.when(t == near_second + 2)
            def _():
                edge_sibling_copy(sib_rows).wait_recv()

            far_work(t, w_own, g_own)

            @pl.when(t < 2 * nq)
            def _():
                own_work(t)

            @pl.when(has_near)
            def _():
                q = pair_q(i)
                near_work(p, q, w_own, g_own)

                @pl.when(p == 1)
                def _():
                    near_work(p, q, w_pair, g_pair)

                    @pl.when(i >= nq)
                    def _():
                        edge_work(0, i - nq)

            @pl.when(has_pair)
            def _():
                cross_work(pair_q(turn))

            lag = t - nq - 2

            @pl.when(jnp.logical_and(lag >= 0, lag < 2 * nq))
            def _():
                pair_work(pair_q(lag))

                @pl.when(lag < nq)
                def _():
                    near_work(0, pair_q(lag), w_pair, g_pair)

            @pl.when(jnp.logical_and(t >= 2 * nq, t < 3 * nq))
            def _():
                @pl.loop(0, 3)
                def _(e):
                    far_work(e * nq + t - 2 * nq, w_pair, g_pair)

                @pl.when(t >= 2 * nq + kept)
                def _():
                    near_work(0, r_base + t - 2 * nq, w_pair, g_pair)

            @pl.when(t >= 3 * nq)
            def _():
                far_work(t, w_pair, g_pair)

            @pl.when(t >= 3 * nq + kept)
            def _():
                edge_work(1, t - 3 * nq)

            @pl.when(t == steps - late - 1)
            def _():
                share_part()

                @pl.loop((nq - late) * sub, nq * sub)
                def _(c):
                    acc[r_base * sub + c] = jnp.zeros((8, LANES), jnp.float32)

            @pl.when(t == near_end - 1)
            def _():
                fold_last()

        finish()

    @pl.when(outer)
    def _():
        @pl.loop(0, 3 * nq)
        def _(t):
            turn = t - nq + 2
            has_pair = jnp.logical_and(turn >= 0, turn < 2 * nq)
            back = t - 2 * nq - 4
            has_back = jnp.logical_and(back >= 0, back < kept)
            slot = jnp.where(t < 2 * nq + kept, t, t + nq - kept)
            has_far = t < 2 * nq + 2 * kept

            @pl.when(turn == 0)
            def _():
                wait_w_pair()
                for b in range(2):
                    up_weights(w_pair.at[far_block(2 + b), :, my_rows, :], b, 1).start()

            @pl.when(has_pair)
            def _():
                pair_copy(turn).wait_recv()

                @pl.when(jnp.logical_or(turn < nq, turn >= nq + kept))
                def _():
                    up_copy(g_pair.at[pair_q(turn)], 1, turn).start()

            @pl.when(t == nq)
            def _():
                sibling_copy(sib_rows).wait_recv()

            @pl.when(t < kept)
            def _():
                wait_near(0, nq + t)

            @pl.when(has_back)
            def _():
                wait_near(1, nq + back)

            @pl.when(has_far)
            def _():
                wait_far(slot)
                far_work(slot, w_own, g_own)

            @pl.when(jnp.logical_and(has_far, t >= 2 * nq))
            def _():
                far_work(slot, w_pair, g_pair)

            @pl.when(t < 2 * nq)
            def _():
                own_work(t)

            @pl.when(t < kept)
            def _():
                near_work(0, r_base + t, w_own, g_own)

            @pl.when(has_back)
            def _():
                q = r_base + back
                near_work(0, q, w_pair, g_pair)
                near_work(1, q, w_own, g_own)
                near_work(1, q, w_pair, g_pair)

            @pl.when(has_pair)
            def _():
                cross_work(pair_q(turn))

            @pl.when(t >= nq)
            def _():
                pair_work(pair_q(t - nq))

            @pl.when(t >= 2 * nq)
            def _():
                @pl.loop(0, 2)
                def _(e):
                    far_work(e * nq + t - 2 * nq, w_pair, g_pair)

        share_part()

    @pl.loop(1, total // 2)
    def _(k):
        part_copy(k, flipped(k)).wait_recv()

    base = hi * (total // 2)
    mine = part[base]
    for d in range(1, total // 2):
        mine = mine + part[base + d]
    side[hi] = mine

    def side_copy(which):
        ref = side.at[which]
        return remote(ref, ref, side_sem.at[0], side_sem.at[1], across_dev)

    side_copy(hi).start()
    side_copy(1 - hi).wait_recv()
    sums[core] = side[0] + side[1]
    base_copy = remote(sums.at[core], sums.at[core], base_sem.at[0], base_sem.at[1], core_dev)
    base_copy.start()

    @pl.loop(0, 2 * nq)
    def _(i):
        pair_copy(i).wait_send()

    @pl.loop(0, n)
    def _(j):
        w_pair_copy(j).wait_send()

    sibling_copy(my_rows).wait_send()

    @pl.loop(1, total // 2)
    def _(k):
        part_copy(k, rank).wait_send()

    @pl.when(inner)
    def _():
        @pl.loop(0, steps)
        def _(t):
            mid_copy(far.at[0], t).wait_send()

            @pl.when(passed_down(t))
            def _():
                down_copy(t).wait_send()

        @pl.loop(0, 2 * kept)
        def _(i):
            back_copy(g_own.at[0], i // kept, lax.rem(i, kept)).wait_send()

        for k, other in sends:
            extra_copy(k, other).wait_send()

        edge_sibling_copy(my_rows).wait_send()

        @pl.when(core == 0)
        def _():
            fold_copy().wait_send()

    @pl.when(outer)
    def _():
        @pl.loop(0, 4 * nq)
        def _(s):
            i = lax.rem(s, 2 * nq)

            @pl.when(jnp.logical_or(i < nq, i >= nq + kept))
            def _():
                up_copy(g_own.at[0], s // (2 * nq), i).wait_send()

        for r in range(4):
            part_of_w = w_edge.at[r // 2, r % 2, :, my_rows, :]
            up_weights(part_of_w, r // 2, r % 2).wait_send()

    side_copy(hi).wait_send()

    def wait_extras(which, groups):
        ref = extras.at[which, pl.ds(0, groups)]
        remote(ref, ref, extra_send.at[0, 0], extra_recv.at[which], core_dev).wait_recv()

    @pl.when(inner)
    def _():
        wait_extras(core, 4 * n_freq - 1)
        wait_extras(1 - core, 4 * n_freq)

    @pl.when(outer)
    def _():
        wait_extras(0, 4 * n_freq)
        wait_extras(1, 4 * n_freq)

    base_copy.wait_send()
    sum_ref = sums.at[1 - core]
    remote(sum_ref, sum_ref, base_sem.at[0], base_sem.at[1], core_dev).wait_recv()

    def late_sum(which, low, c):
        row = extras[which, low * 2 * n_freq, c]
        for g in range(1, 2 * n_freq):
            row = row + extras[which, low * 2 * n_freq + g, c]
        return row

    for which in range(2):
        for low in range(2):
            for c in range(late_rows):
                row = late_sum(which, low, c)
                if which == 0 and c >= late_rows - sub:
                    row = row + late_sum(1, low, c + sub)
                at = ((1 - low) * nq + nq - late) * sub + c
                sums[which, at:at + 1, :] += row

    largest = jnp.max(jnp.maximum(jnp.abs(sums[0]), jnp.abs(sums[1])), keepdims=True)
    out[...] = sums[core] / (largest + 1e-6)


def line_body(n_freq, chunk, nq, blocked, greens, weights):
    _, _, h, points = greens.shape
    n = 8
    kept, late = 3 * nq // 8, 3
    stations = n * h
    dma = pltpu.SemaphoreType.DMA
    regular = pltpu.SemaphoreType.REGULAR
    bf16, f32 = jnp.bfloat16, jnp.float32
    rows = points // LANES
    late_rows = late * (chunk // LANES)
    total = n * n_freq
    out = pl.pallas_call(
        functools.partial(line_kernel, n_freq, h, stations, chunk, nq, kept, late, blocked),
        out_shape=pltpu.VMEM((rows, LANES), f32),
        in_specs=[pl.BlockSpec(memory_space=pl.ANY)] * 2,
        out_specs=pl.BlockSpec(memory_space=pltpu.VMEM),
        scratch_shapes=[
            pltpu.VMEM((2 * nq, 2, h, chunk), bf16),
            pltpu.VMEM((2 * nq, 2, h, chunk), bf16),
            pltpu.VMEM((2, 2 * nq, 2, h, chunk), bf16),
            pltpu.VMEM((4 * nq + 1, 2, h, chunk), bf16),
            pltpu.VMEM((n, 2, h, h), bf16),
            pltpu.VMEM((n, 2, h, h), bf16),
            pltpu.VMEM((2, 2, 2, h, h), bf16),
            pltpu.VMEM((2, 2, h, chunk), f32),
            pltpu.VMEM((rows, 8, LANES), f32),
            pltpu.VMEM((total, rows, LANES), f32),
            pltpu.VMEM((2, rows, LANES), f32),
            pltpu.VMEM((2, rows, LANES), f32),
            pltpu.VMEM((2, 4 * n_freq, late_rows + chunk // LANES, 1, LANES), f32),
            dma((2 * nq,)), dma((n,)), dma((2 * nq,)), dma((2 * nq,)), dma((n,)), dma((n,)), dma((2,)),
            dma((4,)), dma((4,)), dma((2,)),
            dma((4 * nq,)), dma((4 * nq,)), dma((4 * nq + 1,)), dma((4 * nq,)), dma((2 * kept,)),
            dma((total // 2 - 1,)), dma((total // 2 - 1,)), dma((2,)),
            dma((2, total)), dma((2,)), dma((2,)), dma((2,)),
            regular((2, 3)), regular((3,)),
        ],
        compiler_params=pltpu.CompilerParams(
            collective_id=0, has_side_effects=True, vmem_limit_bytes=60 * 1024 * 1024
        ),
    )(greens, weights)
    return out.reshape(points)


def passed_along(x, axis, by):
    size = lax.axis_size(axis)
    return lax.ppermute(x, axis, [(i, (i + by) % size) for i in range(size)])


def mixing_of(weights):
    negated = -weights[1]
    return jnp.stack([jnp.stack([weights[0], negated]), jnp.stack([weights[1], weights[0]])])


def body(greens, noise_weights):
    station_rows = greens.shape[2]
    stations = noise_weights.shape[3]
    device_index = lax.axis_index("stn")
    cycle_length = lax.axis_size("stn")
    mixing = mixing_of(noise_weights)

    def block_product(columns_start, arriving):
        block_rows = arriving.shape[2]
        weights_block = lax.dynamic_slice_in_dim(mixing, columns_start, block_rows, 4)
        return jnp.einsum(
            "ocfin,cfnx->ofix", weights_block, arriving, preferred_element_type=jnp.float32
        )

    half_way = cycle_length // 2
    diagonal = block_product(device_index * station_rows, greens)

    def advance(offset, loop_state):
        running, current = loop_state
        current = passed_along(current, "stn", -1)
        source = (device_index + offset) % cycle_length
        weight = jnp.where(offset == half_way, 1.0, 2.0).astype(jnp.float32)
        running = running + weight * block_product(source * station_rows, current)
        return (running, current)

    summed, current = lax.fori_loop(1, half_way + 1, advance, (diagonal, greens))
    green_real = greens[0].astype(jnp.float32)
    green_imag = greens[1].astype(jnp.float32)
    partial_kernel = (
        jnp.sum(green_real * summed[0] + green_imag * summed[1], axis=(0, 1)) / stations
    )
    raw_kernel = lax.psum(partial_kernel, "stn")
    raw_kernel = lax.psum(raw_kernel, "freq")
    largest = lax.pmax(jnp.max(jnp.abs(raw_kernel)), "pts")
    return raw_kernel / (largest + 1e-06)


def solution(mesh):
    n, cores, n_freq = mesh.shape["stn"], mesh.shape["pts"], mesh.shape["freq"]

    def either(greens, noise_weights):
        _, freqs, rows, points = greens.shape
        fits = n % 4 == 0 and cores == 2 and freqs == 2 and n_freq == 2 and rows % 32 == 0 and points % (2 * LANES) == 0
        if fits:
            return kernel_body(n, n_freq, greens, noise_weights)
        return body(greens, noise_weights)

    in_specs = (P(None, "freq", "stn", "pts"), P(None, "freq", "stn", None))
    return jax.shard_map(either, mesh=mesh, in_specs=in_specs, out_specs=P("pts"), check_vma=False)
```

```python
import functools

import jax
import jax.numpy as jnp
from jax import lax
from jax.experimental import pallas as pl
from jax.experimental.pallas import tpu as pltpu
from jax.sharding import PartitionSpec as P

MESH = pl.DeviceIdType.MESH
LANES = 128


def remote(src, dst, send_sem, recv_sem, target):
    return pltpu.make_async_remote_copy(
        src_ref=src, dst_ref=dst, send_sem=send_sem, recv_sem=recv_sem,
        device_id=target, device_id_type=MESH,
    )


def ring_kernel(
    n, n_freq, h, stations, chunk, nq, blocked,
    greens, weights, out,
    g_own, g_pair, near, far, w_own, w_pair, acc, red, max_out, max_in,
    own_sem, w_own_sem, pair_send, pair_recv, wp_send, wp_recv, sib_sem,
    in_send, in_recv, out_send, far_recv, red_send, red_recv, max_sem, hello_sem, pair_hello,
):
    m = n // 2
    side_len = m // 2
    sub = chunk // LANES
    half_rows = h // 2
    me = lax.axis_index("stn")
    core = lax.axis_index("pts")
    fq = lax.axis_index("freq")
    parity = lax.rem(me, 2)
    z = me // 2
    hi = (z >= side_len).astype(jnp.int32)
    edge = jnp.where(hi == 1, m - 1 - z, z)
    inward = jnp.where(hi == 1, -2, 2)
    inner = edge == side_len - 1
    s_base = hi * nq
    r_base = (1 - hi) * nq
    pair_dev = {"stn": me + 1 - 2 * parity}
    in_dev = {"stn": me + inward}
    out_dev = {"stn": me - inward}
    n_far = side_len * 2 * nq
    n_near = edge * 4 * nq
    n_near_max = (side_len - 1) * 4 * nq
    steps = max(n_far, n_near_max, 3 * nq + 2)
    spread = side_len == 2
    catch_up = 2 * nq + 1 if spread else max((steps * 25) // 32, 3 * nq + 1)
    left = steps - catch_up
    per_step = -(-steps // (steps - catch_up))

    def columns(q):
        return pl.ds(pl.multiple_of(q * chunk, LANES), chunk)

    def w_src(freq, j, rows):
        if blocked:
            return weights.at[:, freq, j, rows, :]
        return weights.at[:, freq, rows, pl.ds(pl.multiple_of(j * h, LANES), h)]

    def global_block(e, opposite):
        low = jnp.where(opposite, 1 - hi, hi) == 0
        return jnp.where(low, e, m - 1 - e)

    def near_slot(receiver_edge, p, half, b, c):
        return ((p * 2 + half) * receiver_edge + (receiver_edge - 1 - b)) * nq + c

    def far_slot(p, b, c):
        return (p * side_len + (side_len - 1 - b)) * nq + c

    def send_inward(src, p, half, b, c):
        q = jnp.where(half == 0, s_base, r_base) + c

        if side_len > 1:
            @pl.when(jnp.logical_not(inner))
            def _():
                slot = near_slot(edge + 1, p, half, b, c)
                remote(src, near.at[b, p, q], in_send.at[slot], in_recv.at[slot], in_dev).start()

        @pl.when(jnp.logical_and(inner, half == 0))
        def _():
            slot = far_slot(p, b, c)
            remote(src, far.at[b, p, c], in_send.at[slot], far_recv.at[slot], in_dev).start()

    freq_dev = {"freq": n_freq - 1 - fq}
    barrier = pltpu.get_barrier_semaphore()
    up, down = z < m - 1, z > 0
    greeted = [pair_dev, {"pts": 1 - core}, freq_dev]

    def greet(sem, device):
        pl.semaphore_signal(sem, inc=1, device_id=device, device_id_type=MESH)

    def along_z(sem_down, sem_up):
        @pl.when(up)
        def _():
            greet(sem_up, {"stn": me + 2})

        @pl.when(down)
        def _():
            greet(sem_down, {"stn": me - 2})

    for device in greeted:
        greet(barrier, device)
    along_z(barrier, barrier)
    pl.semaphore_wait(barrier, len(greeted) + up.astype(jnp.int32) + down.astype(jnp.int32))

    def hello():
        @pl.loop(0, m - 1)
        def _(r):
            along_z(hello_sem.at[0, r], hello_sem.at[1, r])

            @pl.when(up)
            def _():
                pl.semaphore_wait(hello_sem.at[0, r], 1)

            @pl.when(down)
            def _():
                pl.semaphore_wait(hello_sem.at[1, r], 1)

        for i, device in enumerate((pair_dev, freq_dev)):
            greet(pair_hello.at[i], device)
            pl.semaphore_wait(pair_hello.at[i], 1)

    every_row = pl.ds(0, h)
    pair_rows = pl.ds(pl.multiple_of(core * half_rows, 8), half_rows)

    def pair_q(i):
        return jnp.where(i < nq, s_base + i, r_base + i - nq)

    def pair_copy(i):
        q = pair_q(i)
        return remote(
            greens.at[:, 1 - parity, :, columns(q)], g_pair.at[q],
            pair_send.at[i], pair_recv.at[i], pair_dev,
        )

    def w_pair_copy(j):
        return remote(
            w_src(1 - parity, j, pair_rows), w_pair.at[j, :, pair_rows, :],
            wp_send.at[j], wp_recv.at[j], pair_dev,
        )

    def sibling_copy(rows):
        return remote(
            w_pair.at[:, :, rows, :], w_pair.at[:, :, rows, :],
            sib_sem.at[0], sib_sem.at[1], {"pts": 1 - core},
        )

    def own_copy(q):
        return pltpu.make_async_copy(
            greens.at[:, parity, :, columns(q)], g_own.at[q], own_sem.at[q]
        )

    def w_own_copy(j):
        return pltpu.make_async_copy(w_src(parity, j, every_row), w_own.at[j], w_own_sem.at[j])

    @pl.loop(0, 2 * nq)
    def _(i):
        @pl.when(i < nq)
        def _():
            pair_copy(i).start()

        half = i // nq
        c = lax.rem(i, nq)
        send_inward(greens.at[:, parity, :, columns(pair_q(i))], 0, half, edge, c)
        own_copy(i).start()

    @pl.loop(0, n)
    def _(j):
        w_pair_copy(j).start()
        w_own_copy(j).start()

    @pl.loop(nq, 2 * nq)
    def _(i):
        pair_copy(i).start()

    hello()

    acc[...] = jnp.zeros_like(acc)

    @pl.loop(0, 2 * nq)
    def _(q):
        own_copy(q).wait()

    @pl.loop(0, n)
    def _(j):
        w_own_copy(j).wait()

    def contribute(w, gi, gj, q, weight):
        for s in range(sub):
            part = slice(s * LANES, (s + 1) * LANES)
            both = jnp.concatenate([gj[0, :, part], gj[1, :, part]], axis=1)
            ab = jnp.dot(w[...].reshape(2 * h, h), both, preferred_element_type=jnp.float32)
            a, b = ab[:h], ab[h:]
            t = gi[0, :, part].astype(jnp.float32) * (a[:, :LANES] - b[:, LANES:])
            t = t + gi[1, :, part].astype(jnp.float32) * (a[:, LANES:] + b[:, :LANES])
            t = jnp.sum(t.reshape(h // 8, 8, LANES), axis=0)
            acc[q * sub + s] += t * weight

    def far_at(t):
        p = t // (side_len * nq)
        rest = lax.rem(t, side_len * nq)
        return p, side_len - 1 - rest // nq, lax.rem(rest, nq)

    def near_at(t):
        width = jnp.maximum(edge, 1) * nq
        p = t // (2 * width)
        half = lax.rem(t // width, 2)
        rest = lax.rem(t, width)
        return p, half, jnp.maximum(edge, 1) - 1 - rest // nq, lax.rem(rest, nq)

    def part_of(p):
        return jnp.where(p == 0, parity, 1 - parity)

    def far_work(t, w, g):
        p, b, c = far_at(t)
        q = r_base + c
        j = global_block(b, True) * 2 + part_of(p)
        contribute(w.at[j], g.at[q], far.at[b, p, c], q, 2.0)

    def near_work(t, w, g):
        p, half, b, c = near_at(t)
        q = jnp.where(half == 0, s_base, r_base) + c
        j = global_block(b, False) * 2 + part_of(p)
        contribute(w.at[j], g.at[q], near.at[b, p, q], q, 2.0)

    def far_wait(t):
        p, b, c = far_at(t)
        ref = far.at[b, p, c]
        remote(ref, ref, out_send.at[t], far_recv.at[t], in_dev).wait_recv()

        @pl.when(edge > 0)
        def _():
            remote(ref, ref, out_send.at[t], far_recv.at[t], out_dev).start()

    def near_wait(t):
        p, half, b, c = near_at(t)
        q = jnp.where(half == 0, s_base, r_base) + c
        ref = near.at[b, p, q]
        remote(ref, ref, in_send.at[t], in_recv.at[t], out_dev).wait_recv()
        send_inward(ref, p, half, b, c)

    def newest(u):
        far_work(u, w_pair, g_pair)

        @pl.when(u < n_near)
        def _():
            near_work(u, w_pair, g_pair)

    @pl.loop(0, steps)
    def _(t):
        has_pair = jnp.logical_and(jnp.logical_and(t >= nq, t <= 3 * nq), t != 2 * nq)
        turn = t - nq - (t > 2 * nq).astype(jnp.int32)

        @pl.when(has_pair)
        def _():
            i = turn
            pair_copy(i).wait_recv()
            send_inward(g_pair.at[pair_q(i)], 1, i // nq, edge, lax.rem(i, nq))

        @pl.when(t < n_far)
        def _():
            far_wait(t)

        if side_len > 1:
            @pl.when(t < n_near)
            def _():
                near_wait(t)

        @pl.when(t == catch_up - 1)
        def _():
            @pl.loop(0, n)
            def _(j):
                w_pair_copy(j).wait_recv()

            sibling_copy(pair_rows).start()

        @pl.when(t < 2 * nq)
        def _():
            contribute(w_own.at[2 * z + parity], g_own.at[t], g_own.at[t], t, 1.0)

        @pl.when(has_pair)
        def _():
            q = pair_q(turn)
            contribute(w_own.at[2 * z + 1 - parity], g_own.at[q], g_pair.at[q], q, 2.0)

        @pl.when(t < n_far)
        def _():
            far_work(t, w_own, g_own)

        if side_len > 1:
            @pl.when(t < n_near)
            def _():
                near_work(t, w_own, g_own)

        @pl.when(t == catch_up)
        def _():
            sibling_copy(pl.ds(pl.multiple_of((1 - core) * half_rows, 8), half_rows)).wait_recv()

        @pl.when(t >= catch_up)
        def _():
            first = (t - catch_up) * per_step
            last = jnp.minimum(first + per_step, steps)
            if spread:
                first = ((t - catch_up) * 2 * nq) // left
                last = ((t - catch_up + 1) * 2 * nq) // left

            @pl.loop(first, last)
            def _(u):
                @pl.when(u < 2 * nq)
                def _():
                    q = pair_q(u)
                    contribute(w_pair.at[2 * z + 1 - parity], g_pair.at[q], g_pair.at[q], q, 1.0)

                if spread:
                    far_work(lax.rem(u, side_len) * nq + u // side_len, w_pair, g_pair)
                else:
                    @pl.when(u < n_far)
                    def _():
                        far_work(u, w_pair, g_pair)

                if side_len > 1:
                    @pl.when(u < n_near)
                    def _():
                        near_work(u, w_pair, g_pair)

            if spread:
                newest(t - 1)

    if spread:
        newest(steps - 1)

    total = n * n_freq
    rank = me * n_freq + fq
    red[rank] = jnp.sum(acc[...], axis=1) / stations

    def share_copy(k, source):
        target = lax.rem(rank + k, total)
        return remote(
            red.at[source], red.at[source], red_send.at[k - 1], red_recv.at[k - 1],
            {"stn": target // n_freq, "freq": lax.rem(target, n_freq)},
        )

    @pl.loop(1, total)
    def _(k):
        share_copy(k, rank).start()

    @pl.loop(1, total)
    def _(k):
        share_copy(k, lax.rem(rank - k + total, total)).wait_recv()

    raw = red[0]
    for d in range(1, total):
        raw = raw + red[d]
    max_out[...] = jnp.broadcast_to(jnp.max(jnp.abs(raw)), max_out.shape)
    max_copy = remote(max_out, max_in, max_sem.at[0], max_sem.at[1], {"pts": 1 - core})
    max_copy.start()

    @pl.loop(1, total)
    def _(k):
        share_copy(k, rank).wait_send()

    @pl.loop(0, 2 * nq)
    def _(i):
        pair_copy(i).wait_send()

    @pl.loop(0, n)
    def _(j):
        w_pair_copy(j).wait_send()

    sibling_copy(pair_rows).wait_send()
    ref = far.at[0, 0, 0]

    @pl.loop(0, jnp.where(inner, n_far, (edge + 1) * 4 * nq))
    def _(t):
        remote(ref, ref, in_send.at[t], far_recv.at[0], in_dev).wait_send()

    @pl.when(edge > 0)
    def _():
        @pl.loop(0, n_far)
        def _(t):
            remote(ref, ref, out_send.at[t], far_recv.at[0], out_dev).wait_send()

    max_copy.wait()
    largest = jnp.maximum(max_out[0:1, 0:1], max_in[0:1, 0:1])
    out[...] = raw / (largest + 1e-6)


def kernel_body(n, n_freq, greens, weights):
    _, _, h, points = greens.shape
    stations = weights.shape[3]
    half = points // 2
    chunk = LANES
    while chunk * 2 * h <= 32768 and half % (chunk * 2) == 0:
        chunk *= 2
    nq = half // chunk
    side_len = n // 4
    n_far = side_len * 2 * nq
    n_near = max(side_len - 1, 1) * 4 * nq
    blocked = h % LANES != 0
    if blocked:
        weights = weights.reshape(2, weights.shape[1], h, n, h).swapaxes(2, 3)
    if side_len == 2 and nq >= 4:
        return line_body(n_freq, chunk, nq, blocked, greens, weights)
    dma = pltpu.SemaphoreType.DMA
    bf16, f32 = jnp.bfloat16, jnp.float32
    rows = points // LANES
    out = pl.pallas_call(
        functools.partial(ring_kernel, n, n_freq, h, stations, chunk, nq, blocked),
        out_shape=jax.ShapeDtypeStruct((rows, LANES), f32),
        in_specs=[pl.BlockSpec(memory_space=pl.ANY)] * 2,
        out_specs=pl.BlockSpec(memory_space=pltpu.VMEM),
        scratch_shapes=[
            pltpu.VMEM((2 * nq, 2, h, chunk), bf16),
            pltpu.VMEM((2 * nq, 2, h, chunk), bf16),
            pltpu.VMEM((max(side_len - 1, 1), 2, 2 * nq, 2, h, chunk), bf16),
            pltpu.VMEM((side_len, 2, nq, 2, h, chunk), bf16),
            pltpu.VMEM((n, 2, h, h), bf16),
            pltpu.VMEM((n, 2, h, h), bf16),
            pltpu.VMEM((rows, 8, LANES), f32),
            pltpu.VMEM((n * n_freq, rows, LANES), f32),
            pltpu.VMEM((8, LANES), f32),
            pltpu.VMEM((8, LANES), f32),
            dma((2 * nq,)), dma((n,)), dma((2 * nq,)), dma((2 * nq,)), dma((n,)), dma((n,)), dma((2,)),
            dma((max(n_near, n_far),)), dma((n_near,)), dma((n_far,)), dma((n_far,)),
            dma((n * n_freq - 1,)), dma((n * n_freq - 1,)), dma((2,)),
            pltpu.SemaphoreType.REGULAR((2, n // 2 - 1)), pltpu.SemaphoreType.REGULAR((2,)),
        ],
        compiler_params=pltpu.CompilerParams(
            collective_id=0, has_side_effects=True, vmem_limit_bytes=60 * 1024 * 1024
        ),
    )(greens, weights)
    return out.reshape(points)


FAR_FIRST = (11, 9, 10, 8, 15, 7, 13, 14, 5, 6, 12, 4, 3, 1, 2, 0)


def line_kernel(
    n_freq, h, stations, chunk, nq, kept, late, blocked,
    greens, weights, out,
    g_own, g_pair, near, far, w_own, w_pair, w_edge, folded, acc, part, side, sums, extras,
    own_sem, w_own_sem, pair_send, pair_recv, wp_send, wp_recv, sib_sem, we_send, we_recv, we_sib,
    in_send, near_recv, far_recv, down_send, back_send, part_send, part_recv, side_sem,
    extra_send, extra_recv, base_sem, fold_sem, reply_sem, hello_sem, pair_hello,
):
    n = 8
    sub = chunk // LANES
    half_rows = h // 2
    steps = 4 * nq
    me = lax.axis_index("stn")
    core = lax.axis_index("pts")
    fq = lax.axis_index("freq")
    parity = lax.rem(me, 2)
    z = me // 2
    hi = z // 2
    inner = jnp.logical_or(z == 1, z == 2)
    outer = jnp.logical_not(inner)
    s_base = hi * nq
    r_base = (1 - hi) * nq
    rank = me * n_freq + fq
    total = n * n_freq
    inward = jnp.where(hi == 1, -2, 2)
    pair_dev = {"stn": me + 1 - 2 * parity}
    in_dev = {"stn": me + inward}
    out_dev = {"stn": me - inward}
    core_dev = {"pts": 1 - core}
    freq_dev = {"freq": n_freq - 1 - fq}
    across_dev = {"stn": 2 * (3 - z) + parity}
    other_inner = 2 - hi
    other_edge = 3 - 3 * hi
    near_z = jnp.where(inner, z - inward // 2, z + inward // 2)

    def columns(q):
        return pl.ds(pl.multiple_of(q * chunk, LANES), chunk)

    def w_src(freq, j, rows):
        if blocked:
            return weights.at[:, freq, j, rows, :]
        return weights.at[:, freq, rows, pl.ds(pl.multiple_of(j * h, LANES), h)]

    def block_of(where, p):
        return 2 * where + jnp.where(p == 0, parity, 1 - parity)

    def far_block(e):
        return block_of(jnp.where(lax.rem(e, 2) == 0, other_inner, other_edge), e // 2)

    def position(e, c):
        late_c = c >= jnp.where(e < 2, nq - 1, kept)
        pair_half = jnp.where(e == 2, 2 * nq, 2 * nq + kept) + c
        pair_late = jnp.where(e == 2, 2 * nq + kept, 3 * nq) + c
        early = jnp.where(late_c, 2 * nq - 2 + e, e * (nq - 1) + c)
        return jnp.where(e < 2, early, jnp.where(late_c, pair_late, pair_half))

    def block_at(t):
        e = (t >= nq - 1).astype(jnp.int32)
        c = t - e * (nq - 1)
        corner = t >= 2 * nq - 2
        e = jnp.where(corner, t - (2 * nq - 2), e)
        c = jnp.where(corner, nq - 1, c)
        pairs = t - 2 * nq
        third = jnp.logical_and(pairs >= kept, pairs < 2 * kept)
        third = jnp.logical_or(third, pairs >= nq + kept)
        pair_c = jnp.where(pairs < kept, pairs, jnp.where(pairs < nq + kept, pairs - kept, pairs - nq))
        e = jnp.where(pairs >= 0, 2 + third.astype(jnp.int32), e)
        c = jnp.where(pairs >= 0, pair_c, c)
        return e, c

    every_row = pl.ds(0, h)
    my_rows = pl.ds(pl.multiple_of(core * half_rows, 8), half_rows)
    sib_rows = pl.ds(pl.multiple_of((1 - core) * half_rows, 8), half_rows)

    def pair_q(i):
        return jnp.where(i < nq, s_base + i, r_base + i - nq)

    def g_src(q):
        return greens.at[:, parity, :, columns(q)]

    def own_copy(q):
        return pltpu.make_async_copy(g_src(q), g_own.at[q], own_sem.at[q])

    def w_own_copy(j):
        return pltpu.make_async_copy(w_src(parity, j, every_row), w_own.at[j], w_own_sem.at[j])

    def pair_copy(i):
        q = pair_q(i)
        return remote(
            greens.at[:, 1 - parity, :, columns(q)], g_pair.at[q],
            pair_send.at[i], pair_recv.at[i], pair_dev,
        )

    def w_pair_copy(j):
        return remote(
            w_src(1 - parity, j, my_rows), w_pair.at[j, :, my_rows, :],
            wp_send.at[j], wp_recv.at[j], pair_dev,
        )

    def sibling_copy(rows):
        part_of_w = w_pair.at[:, :, rows, :]
        return remote(part_of_w, part_of_w, sib_sem.at[0], sib_sem.at[1], core_dev)

    def edge_sibling_copy(rows):
        part_of_w = w_edge.at[:, :, :, rows, :]
        return remote(part_of_w, part_of_w, we_sib.at[0], we_sib.at[1], core_dev)

    def up_copy(src, p, i):
        slot = p * 2 * nq + i
        return remote(src, near.at[p, pair_q(i)], in_send.at[slot], near_recv.at[slot], in_dev)

    def up_weights(src, b, p):
        i = 2 * b + p
        return remote(src, w_edge.at[b, p, :, my_rows, :], we_send.at[i], we_recv.at[i], in_dev)

    def mid_copy(src, slot):
        last = slot == steps - 1
        land = jnp.where(jnp.logical_and(last, core == 0), steps, slot)
        target = {"stn": me + inward, "pts": jnp.where(last, 1, core)}
        return remote(src, far.at[land], in_send.at[slot], far_recv.at[land], target)

    corner = 2 * nq - 2

    def down_copy(slot):
        return remote(far.at[slot], far.at[slot], down_send.at[slot], far_recv.at[slot], out_dev)

    def back_copy(src, p, c):
        return remote(
            src, near.at[p, (1 - hi) * nq + c], back_send.at[p * kept + c],
            near_recv.at[p * 2 * nq + nq + c], out_dev,
        )

    barrier = pltpu.get_barrier_semaphore()
    up, down = z < 3, z > 0
    greeted = [pair_dev, core_dev, freq_dev]

    def greet(sem, device):
        pl.semaphore_signal(sem, inc=1, device_id=device, device_id_type=MESH)

    def along_z(sem_down, sem_up):
        @pl.when(up)
        def _():
            greet(sem_up, {"stn": me + 2})

        @pl.when(down)
        def _():
            greet(sem_down, {"stn": me - 2})

    @pl.when(inner)
    def _():
        greet(barrier, in_dev)
        greet(barrier, out_dev)

    for device in greeted:
        greet(barrier, device)
    pl.semaphore_wait(barrier, len(greeted) + 1)

    @pl.when(outer)
    def _():
        greet(reply_sem.at[0], in_dev)

    @pl.loop(0, nq)
    def _(i):
        src = g_src(pair_q(i))

        @pl.when(jnp.logical_and(inner, i < nq - 1))
        def _():
            mid_copy(src, i).start()

        @pl.when(outer)
        def _():
            up_copy(src, 0, i).start()

    corner_src = g_src(pair_q(nq - 1))

    @pl.loop(0, n)
    def _(j):
        w_pair_copy(j).start()
        w_own_copy(j).start()

    @pl.loop(0, 2 * nq)
    def _(i):
        own_copy(pair_q(i)).start()
        pair_copy(i).start()

    @pl.when(inner)
    def _():
        pl.semaphore_wait(reply_sem.at[0], 1)

        @pl.loop(0, kept)
        def _(c):
            back_copy(g_src(pair_q(nq + c)), 0, c).start()

    @pl.when(outer)
    def _():
        for b in range(2):
            up_weights(w_src(parity, far_block(2 + b), my_rows), b, 0).start()

    @pl.loop(0, 3)
    def _(r):
        along_z(hello_sem.at[0, r], hello_sem.at[1, r])

        @pl.when(up)
        def _():
            pl.semaphore_wait(hello_sem.at[0, r], 1)

        @pl.when(down)
        def _():
            pl.semaphore_wait(hello_sem.at[1, r], 1)

    for i, device in enumerate((pair_dev, freq_dev, core_dev)):
        greet(pair_hello.at[i], device)
        pl.semaphore_wait(pair_hello.at[i], 1)

    acc[...] = jnp.zeros_like(acc)

    @pl.loop(0, 2 * nq)
    def _(q):
        own_copy(q).wait()

    @pl.loop(0, n)
    def _(j):
        w_own_copy(j).wait()

    def product(w, gi, gj, s):
        lanes = slice(s * LANES, (s + 1) * LANES)
        both = jnp.concatenate([gj[0, :, lanes], gj[1, :, lanes]], axis=1)
        ab = jnp.dot(w[...].reshape(2 * h, h), both, preferred_element_type=jnp.float32)
        a, b = ab[:h], ab[h:]
        t = gi[0, :, lanes].astype(jnp.float32) * (a[:, :LANES] - b[:, LANES:])
        t = t + gi[1, :, lanes].astype(jnp.float32) * (a[:, LANES:] + b[:, :LANES])
        return jnp.sum(t.reshape(h // 8, 8, LANES), axis=0)

    def contribute(w, gi, gj, q, weight):
        for s in range(sub):
            acc[q * sub + s] += product(w, gi, gj, s) * weight

    own_pair_block = block_of(z, 1)

    def own_work(q):
        contribute(w_own.at[me], g_own.at[q], g_own.at[q], q, 1.0)

    def cross_work(q):
        contribute(w_own.at[own_pair_block], g_own.at[q], g_pair.at[q], q, 2.0)

    def pair_work(q):
        contribute(w_pair.at[own_pair_block], g_pair.at[q], g_pair.at[q], q, 1.0)

    def far_work(e, c, w, g):
        q = r_base + c
        contribute(w.at[far_block(e)], g.at[q], far.at[position(e, c)], q, 2.0)

    def near_work(p, q, w, g):
        contribute(w.at[block_of(near_z, p)], g.at[q], near.at[p, q], q, 2.0)

    def edge_work(b, c):
        q = r_base + c

        @pl.loop(0, 2)
        def _(p):
            contribute(w_edge.at[b, p], near.at[p, q], far.at[position(2 + b, c)], q, 2.0)

    def transposed(w, g):
        return lax.dot_general(w, g, (((0,), (0,)), ((), ())), preferred_element_type=jnp.float32)

    def fold(w, gi, s):
        lanes = slice(s * LANES, (s + 1) * LANES)
        both = jnp.concatenate([gi[0, :, lanes], gi[1, :, lanes]], axis=1)
        a, b = transposed(w[0], both), transposed(w[1], both)
        return a[:, :LANES] + b[:, LANES:], a[:, LANES:] - b[:, :LANES]

    def fold_last():
        q, j = r_base + nq - 1, far_block(3)
        for s in range(sub):
            lanes = slice(s * LANES, (s + 1) * LANES)
            re, im = fold(w_own.at[j], g_own.at[q], s)
            folded[core, 0, :, lanes] = re
            folded[core, 1, :, lanes] = im
            for w, g in ((w_pair.at[j], g_pair.at[q]), (w_edge.at[1, 0], near.at[0, q]), (w_edge.at[1, 1], near.at[1, q])):
                re, im = fold(w, g, s)
                folded[core, 0, :, lanes] += re
                folded[core, 1, :, lanes] += im

        @pl.when(core == 0)
        def _():
            fold_copy().start()

    def fold_copy():
        return remote(folded.at[0], folded.at[0], fold_sem.at[0], fold_sem.at[1], core_dev)

    def unfold(which, slot, s):
        lanes = slice(s * LANES, (s + 1) * LANES)
        t = far[slot, 0, :, lanes].astype(jnp.float32) * folded[which, 0, :, lanes]
        t = t + far[slot, 1, :, lanes].astype(jnp.float32) * folded[which, 1, :, lanes]
        return 2.0 * jnp.sum(t.reshape(h // 8, 8, LANES), axis=0)

    def passed_down(t):
        return t < 2 * nq + 2 * kept

    def wait_far(t):
        ref = far.at[t]
        remote(ref, ref, in_send.at[0], far_recv.at[t], in_dev).wait_recv()

    def wait_near(p, i):
        slot = p * 2 * nq + i
        ref = near.at[p, pair_q(i)]
        remote(ref, ref, in_send.at[slot], near_recv.at[slot], in_dev).wait_recv()

    def wait_w_pair():
        @pl.loop(0, n)
        def _(j):
            w_pair_copy(j).wait_recv()

        sibling_copy(my_rows).start()

    def share_part():
        part[rank] = jnp.sum(acc[...], axis=1) / stations

        @pl.loop(0, total // 2 - 1)
        def _(k):
            part_copy(total // 2 - 1 - k, rank).start()

    def at_rank(target):
        return {"stn": target // n_freq, "freq": lax.rem(target, n_freq)}

    def flipped(k):
        bit, flip = total // 2, jnp.int32(0)
        while bit:
            mine = lax.rem(rank // bit, 2)
            turn = lax.rem(k // bit, 2)
            flip = flip + bit * (mine + turn - 2 * mine * turn)
            bit //= 2
        return flip

    def part_copy(k, source):
        ref = part.at[source]
        return remote(ref, ref, part_send.at[k - 1], part_recv.at[k - 1], at_rank(flipped(k)))

    my_group = (hi * 2 + parity) * n_freq + fq
    late_rows = late * sub

    sends = [(k, other) for k in FAR_FIRST for other in range(2) if k or other]

    def extra_copy(k, other):
        def turned(v, bit):
            return 1 - v if k & bit else v

        target_z = 2 * turned(hi, 8) + turned(lax.rem(z, 2), 4)
        target = {
            "stn": 2 * target_z + turned(parity, 2), "freq": turned(fq, 1),
            "pts": 1 - core if other else core,
        }
        return remote(
            extras.at[core, my_group], extras.at[core, my_group],
            extra_send.at[other, k], extra_recv.at[core], target,
        )

    def late_row(t):
        return jnp.sum(t, axis=0, keepdims=True) / stations

    def finish():
        first = (r_base + nq - late) * sub
        for c in range(late_rows):
            extras[core, my_group, c] = late_row(acc[first + c])
        for s in range(sub):
            extras[core, my_group, late_rows + s] = jnp.zeros((1, LANES), jnp.float32)

        @pl.when(core == 1)
        def _():
            fold_copy().wait_recv()
            wait_far(steps)
            wait_far(steps - 1)
            for s in range(sub):
                c = late_rows - sub + s
                extras[1, my_group, c] = late_row(acc[first + c] + unfold(1, steps - 1, s))
                extras[1, my_group, late_rows + s] = late_row(unfold(0, steps, s))

        for k, other in sends:
            extra_copy(k, other).start()

    near_second = nq + 4
    near_third = near_second + nq
    near_fourth = near_third + nq - kept
    near_end = near_fourth + nq - kept

    def near_at(t):
        i = jnp.where(t >= near_second, t - near_second, t)
        i = jnp.where(t >= near_third, t - near_third + nq + kept, i)
        i = jnp.where(t >= near_fourth, t - near_fourth + nq + kept, i)
        second = jnp.logical_and(t >= near_second, t < near_third)
        p = jnp.logical_or(second, t >= near_fourth).astype(jnp.int32)
        present = jnp.logical_or(t < nq, jnp.logical_and(t >= near_second, t < near_end))
        return present, p, i

    @pl.when(inner)
    def _():
        @pl.loop(0, steps - 1)
        def _(t):
            has_near, p, i = near_at(t)
            has_pair = jnp.logical_and(t >= nq, t < 3 * nq)
            turn = t - nq
            wait_far(t)

            @pl.when(passed_down(t))
            def _():
                down_copy(t).start()

            @pl.when(has_near)
            def _():
                wait_near(p, i)

            @pl.when(t < nq)
            def _():
                mid_copy(near.at[0, pair_q(t)], position(1, t)).start()

            @pl.when(t == nq - 2)
            def _():
                mid_copy(corner_src, corner).start()

            @pl.when(t == nq)
            def _():
                wait_w_pair()

            @pl.when(has_pair)
            def _():
                pair_copy(turn).wait_recv()

                @pl.when(turn < kept)
                def _():
                    mid_copy(g_pair.at[pair_q(turn)], 2 * nq + turn).start()

                @pl.when(jnp.logical_and(turn >= nq, turn < nq + kept))
                def _():
                    back_copy(g_pair.at[pair_q(turn)], 1, turn - nq).start()

            third = t - near_second
            fourth = third - (nq - kept)

            @pl.when(jnp.logical_and(third >= 0, third < kept))
            def _():
                mid_copy(near.at[1, pair_q(third)], 2 * nq + kept + third).start()

            send_third = jnp.logical_and(third >= kept, third < nq)

            @pl.when(send_third)
            def _():
                mid_copy(g_pair.at[pair_q(third)], 2 * nq + kept + third).start()

            @pl.when(jnp.logical_and(fourth >= kept, fourth < nq))
            def _():
                mid_copy(near.at[1, pair_q(fourth)], 3 * nq + fourth).start()

            @pl.when(t == nq + 2)
            def _():
                sibling_copy(sib_rows).wait_recv()

            @pl.when(t == near_second)
            def _():
                for r in range(4):
                    part_of_w = w_edge.at[r // 2, r % 2, :, my_rows, :]
                    up_weights(part_of_w, r // 2, r % 2).wait_recv()
                edge_sibling_copy(my_rows).start()

            @pl.when(t == near_second + 2)
            def _():
                edge_sibling_copy(sib_rows).wait_recv()

            e, c = block_at(t)
            far_work(e, c, w_own, g_own)

            @pl.when(t < 2 * nq)
            def _():
                own_work(t)

            @pl.when(has_near)
            def _():
                q = pair_q(i)
                near_work(p, q, w_own, g_own)

                @pl.when(t >= nq)
                def _():
                    near_work(p, q, w_pair, g_pair)

                @pl.when(t >= near_fourth)
                def _():
                    edge_work(0, i - nq)

            @pl.when(has_pair)
            def _():
                cross_work(pair_q(turn))

            lag = t - nq - 2

            @pl.when(jnp.logical_and(lag >= 0, lag < 2 * nq))
            def _():
                pair_work(pair_q(lag))

                @pl.when(lag < nq)
                def _():
                    near_work(0, pair_q(lag), w_pair, g_pair)

            @pl.when(t >= 2 * nq)
            def _():
                far_work(e, c, w_pair, g_pair)

                @pl.when(t < 3 * nq)
                def _():
                    @pl.loop(0, 2)
                    def _(first):
                        far_work(first, t - 2 * nq, w_pair, g_pair)

            @pl.when(t >= 3 * nq + kept)
            def _():
                edge_work(1, t - 3 * nq)

            @pl.when(t == steps - late - 1)
            def _():
                share_part()

                @pl.loop((nq - late) * sub, nq * sub)
                def _(c):
                    acc[r_base * sub + c] = jnp.zeros((8, LANES), jnp.float32)

            @pl.when(t == near_end - 1)
            def _():
                fold_last()

        finish()

    @pl.when(outer)
    def _():
        @pl.loop(0, 3 * nq)
        def _(t):
            turn = t - nq + 2
            has_pair = jnp.logical_and(turn >= 0, turn < 2 * nq)
            back = t - 2 * nq - 4
            has_back = jnp.logical_and(back >= 0, back < kept)
            e, c = block_at(t)
            has_far = t < 2 * nq + 2 * kept

            @pl.when(turn == 0)
            def _():
                wait_w_pair()
                for b in range(2):
                    up_weights(w_pair.at[far_block(2 + b), :, my_rows, :], b, 1).start()

            @pl.when(has_pair)
            def _():
                pair_copy(turn).wait_recv()

                @pl.when(jnp.logical_or(turn < nq, turn >= nq + kept))
                def _():
                    up_copy(g_pair.at[pair_q(turn)], 1, turn).start()

                @pl.when(turn == nq - 1)
                def _():
                    @pl.loop(nq + kept, 2 * nq)
                    def _(i):
                        up_copy(g_src(pair_q(i)), 0, i).start()

            @pl.when(t == nq)
            def _():
                sibling_copy(sib_rows).wait_recv()

            @pl.when(t < kept)
            def _():
                wait_near(0, nq + t)

            @pl.when(has_back)
            def _():
                wait_near(1, nq + back)

            @pl.when(has_far)
            def _():
                wait_far(t)
                far_work(e, c, w_own, g_own)

            @pl.when(jnp.logical_and(has_far, t >= 2 * nq))
            def _():
                far_work(e, c, w_pair, g_pair)

            @pl.when(t < 2 * nq)
            def _():
                own_work(t)

            @pl.when(t < kept)
            def _():
                near_work(0, r_base + t, w_own, g_own)

            @pl.when(has_back)
            def _():
                q = r_base + back
                near_work(0, q, w_pair, g_pair)
                near_work(1, q, w_own, g_own)
                near_work(1, q, w_pair, g_pair)

            @pl.when(has_pair)
            def _():
                cross_work(pair_q(turn))

            @pl.when(t >= nq)
            def _():
                pair_work(pair_q(t - nq))

            @pl.when(t >= 2 * nq)
            def _():
                @pl.loop(0, 2)
                def _(first):
                    far_work(first, t - 2 * nq, w_pair, g_pair)

        share_part()

    @pl.loop(1, total // 2)
    def _(k):
        part_copy(k, flipped(k)).wait_recv()

    base = hi * (total // 2)
    mine = part[base]
    for d in range(1, total // 2):
        mine = mine + part[base + d]
    side[hi] = mine

    def side_copy(which):
        ref = side.at[which]
        return remote(ref, ref, side_sem.at[0], side_sem.at[1], across_dev)

    side_copy(hi).start()
    side_copy(1 - hi).wait_recv()
    sums[core] = side[0] + side[1]
    base_copy = remote(sums.at[core], sums.at[core], base_sem.at[0], base_sem.at[1], core_dev)
    base_copy.start()

    @pl.loop(0, 2 * nq)
    def _(i):
        pair_copy(i).wait_send()

    @pl.loop(0, n)
    def _(j):
        w_pair_copy(j).wait_send()

    sibling_copy(my_rows).wait_send()

    @pl.loop(1, total // 2)
    def _(k):
        part_copy(k, rank).wait_send()

    @pl.when(inner)
    def _():
        @pl.loop(0, steps)
        def _(t):
            mid_copy(far.at[0], t).wait_send()

            @pl.when(passed_down(t))
            def _():
                down_copy(t).wait_send()

        @pl.loop(0, 2 * kept)
        def _(i):
            back_copy(g_own.at[0], i // kept, lax.rem(i, kept)).wait_send()

        for k, other in sends:
            extra_copy(k, other).wait_send()

        edge_sibling_copy(my_rows).wait_send()

        @pl.when(core == 0)
        def _():
            fold_copy().wait_send()

    @pl.when(outer)
    def _():
        @pl.loop(0, 4 * nq)
        def _(s):
            i = lax.rem(s, 2 * nq)

            @pl.when(jnp.logical_or(i < nq, i >= nq + kept))
            def _():
                up_copy(g_own.at[0], s // (2 * nq), i).wait_send()

        for r in range(4):
            part_of_w = w_edge.at[r // 2, r % 2, :, my_rows, :]
            up_weights(part_of_w, r // 2, r % 2).wait_send()

    side_copy(hi).wait_send()

    def wait_extras(which, groups):
        ref = extras.at[which, pl.ds(0, groups)]
        remote(ref, ref, extra_send.at[0, 0], extra_recv.at[which], core_dev).wait_recv()

    @pl.when(inner)
    def _():
        wait_extras(core, 4 * n_freq - 1)
        wait_extras(1 - core, 4 * n_freq)

    @pl.when(outer)
    def _():
        wait_extras(0, 4 * n_freq)
        wait_extras(1, 4 * n_freq)

    base_copy.wait_send()
    sum_ref = sums.at[1 - core]
    remote(sum_ref, sum_ref, base_sem.at[0], base_sem.at[1], core_dev).wait_recv()

    def late_sum(which, low, c):
        row = extras[which, low * 2 * n_freq, c]
        for g in range(1, 2 * n_freq):
            row = row + extras[which, low * 2 * n_freq + g, c]
        return row

    for which in range(2):
        for low in range(2):
            for c in range(late_rows):
                row = late_sum(which, low, c)
                if which == 0 and c >= late_rows - sub:
                    row = row + late_sum(1, low, c + sub)
                at = ((1 - low) * nq + nq - late) * sub + c
                sums[which, at:at + 1, :] += row

    largest = jnp.max(jnp.maximum(jnp.abs(sums[0]), jnp.abs(sums[1])), keepdims=True)
    out[...] = sums[core] / (largest + 1e-6)


def line_body(n_freq, chunk, nq, blocked, greens, weights):
    _, _, h, points = greens.shape
    n = 8
    kept, late = 3 * nq // 8, 4
    stations = n * h
    dma = pltpu.SemaphoreType.DMA
    regular = pltpu.SemaphoreType.REGULAR
    bf16, f32 = jnp.bfloat16, jnp.float32
    rows = points // LANES
    late_rows = late * (chunk // LANES)
    total = n * n_freq
    out = pl.pallas_call(
        functools.partial(line_kernel, n_freq, h, stations, chunk, nq, kept, late, blocked),
        out_shape=pltpu.VMEM((rows, LANES), f32),
        in_specs=[pl.BlockSpec(memory_space=pl.ANY)] * 2,
        out_specs=pl.BlockSpec(memory_space=pltpu.VMEM),
        scratch_shapes=[
            pltpu.VMEM((2 * nq, 2, h, chunk), bf16),
            pltpu.VMEM((2 * nq, 2, h, chunk), bf16),
            pltpu.VMEM((2, 2 * nq, 2, h, chunk), bf16),
            pltpu.VMEM((4 * nq + 1, 2, h, chunk), bf16),
            pltpu.VMEM((n, 2, h, h), bf16),
            pltpu.VMEM((n, 2, h, h), bf16),
            pltpu.VMEM((2, 2, 2, h, h), bf16),
            pltpu.VMEM((2, 2, h, chunk), f32),
            pltpu.VMEM((rows, 8, LANES), f32),
            pltpu.VMEM((total, rows, LANES), f32),
            pltpu.VMEM((2, rows, LANES), f32),
            pltpu.VMEM((2, rows, LANES), f32),
            pltpu.VMEM((2, 4 * n_freq, late_rows + chunk // LANES, 1, LANES), f32),
            dma((2 * nq,)), dma((n,)), dma((2 * nq,)), dma((2 * nq,)), dma((n,)), dma((n,)), dma((2,)),
            dma((4,)), dma((4,)), dma((2,)),
            dma((4 * nq,)), dma((4 * nq,)), dma((4 * nq + 1,)), dma((4 * nq,)), dma((2 * kept,)),
            dma((total // 2 - 1,)), dma((total // 2 - 1,)), dma((2,)),
            dma((2, total)), dma((2,)), dma((2,)), dma((2,)),
            regular((1,)), regular((2, 3)), regular((3,)),
        ],
        compiler_params=pltpu.CompilerParams(
            collective_id=0, has_side_effects=True, vmem_limit_bytes=60 * 1024 * 1024
        ),
    )(greens, weights)
    return out.reshape(points)


def passed_along(x, axis, by):
    size = lax.axis_size(axis)
    return lax.ppermute(x, axis, [(i, (i + by) % size) for i in range(size)])


def mixing_of(weights):
    negated = -weights[1]
    return jnp.stack([jnp.stack([weights[0], negated]), jnp.stack([weights[1], weights[0]])])


def body(greens, noise_weights):
    station_rows = greens.shape[2]
    stations = noise_weights.shape[3]
    device_index = lax.axis_index("stn")
    cycle_length = lax.axis_size("stn")
    mixing = mixing_of(noise_weights)

    def block_product(columns_start, arriving):
        block_rows = arriving.shape[2]
        weights_block = lax.dynamic_slice_in_dim(mixing, columns_start, block_rows, 4)
        return jnp.einsum(
            "ocfin,cfnx->ofix", weights_block, arriving, preferred_element_type=jnp.float32
        )

    half_way = cycle_length // 2
    diagonal = block_product(device_index * station_rows, greens)

    def advance(offset, loop_state):
        running, current = loop_state
        current = passed_along(current, "stn", -1)
        source = (device_index + offset) % cycle_length
        weight = jnp.where(offset == half_way, 1.0, 2.0).astype(jnp.float32)
        running = running + weight * block_product(source * station_rows, current)
        return (running, current)

    summed, current = lax.fori_loop(1, half_way + 1, advance, (diagonal, greens))
    green_real = greens[0].astype(jnp.float32)
    green_imag = greens[1].astype(jnp.float32)
    partial_kernel = (
        jnp.sum(green_real * summed[0] + green_imag * summed[1], axis=(0, 1)) / stations
    )
    raw_kernel = lax.psum(partial_kernel, "stn")
    raw_kernel = lax.psum(raw_kernel, "freq")
    largest = lax.pmax(jnp.max(jnp.abs(raw_kernel)), "pts")
    return raw_kernel / (largest + 1e-06)


def solution(mesh):
    n, cores, n_freq = mesh.shape["stn"], mesh.shape["pts"], mesh.shape["freq"]

    def either(greens, noise_weights):
        _, freqs, rows, points = greens.shape
        fits = n % 4 == 0 and cores == 2 and freqs == 2 and n_freq == 2 and rows % 32 == 0 and points % (2 * LANES) == 0
        if fits:
            return kernel_body(n, n_freq, greens, noise_weights)
        return body(greens, noise_weights)

    in_specs = (P(None, "freq", "stn", "pts"), P(None, "freq", "stn", None))
    return jax.shard_map(either, mesh=mesh, in_specs=in_specs, out_specs=P("pts"), check_vma=False)
```

```python
import functools

import jax
import jax.numpy as jnp
from jax import lax
from jax.experimental import pallas as pl
from jax.experimental.pallas import tpu as pltpu
from jax.sharding import PartitionSpec as P

MESH = pl.DeviceIdType.MESH
LANES = 128


def remote(src, dst, send_sem, recv_sem, target):
    return pltpu.make_async_remote_copy(
        src_ref=src, dst_ref=dst, send_sem=send_sem, recv_sem=recv_sem,
        device_id=target, device_id_type=MESH,
    )


def ring_kernel(
    n, n_freq, h, stations, chunk, nq, blocked,
    greens, weights, out,
    g_own, g_pair, near, far, w_own, w_pair, acc, red, max_out, max_in,
    own_sem, w_own_sem, pair_send, pair_recv, wp_send, wp_recv, sib_sem,
    in_send, in_recv, out_send, far_recv, red_send, red_recv, max_sem, hello_sem, pair_hello,
):
    m = n // 2
    side_len = m // 2
    sub = chunk // LANES
    half_rows = h // 2
    me = lax.axis_index("stn")
    core = lax.axis_index("pts")
    fq = lax.axis_index("freq")
    parity = lax.rem(me, 2)
    z = me // 2
    hi = (z >= side_len).astype(jnp.int32)
    edge = jnp.where(hi == 1, m - 1 - z, z)
    inward = jnp.where(hi == 1, -2, 2)
    inner = edge == side_len - 1
    s_base = hi * nq
    r_base = (1 - hi) * nq
    pair_dev = {"stn": me + 1 - 2 * parity}
    in_dev = {"stn": me + inward}
    out_dev = {"stn": me - inward}
    n_far = side_len * 2 * nq
    n_near = edge * 4 * nq
    n_near_max = (side_len - 1) * 4 * nq
    steps = max(n_far, n_near_max, 3 * nq + 2)
    spread = side_len == 2
    catch_up = 2 * nq + 1 if spread else max((steps * 25) // 32, 3 * nq + 1)
    left = steps - catch_up
    per_step = -(-steps // (steps - catch_up))

    def columns(q):
        return pl.ds(pl.multiple_of(q * chunk, LANES), chunk)

    def w_src(freq, j, rows):
        if blocked:
            return weights.at[:, freq, j, rows, :]
        return weights.at[:, freq, rows, pl.ds(pl.multiple_of(j * h, LANES), h)]

    def global_block(e, opposite):
        low = jnp.where(opposite, 1 - hi, hi) == 0
        return jnp.where(low, e, m - 1 - e)

    def near_slot(receiver_edge, p, half, b, c):
        return ((p * 2 + half) * receiver_edge + (receiver_edge - 1 - b)) * nq + c

    def far_slot(p, b, c):
        return (p * side_len + (side_len - 1 - b)) * nq + c

    def send_inward(src, p, half, b, c):
        q = jnp.where(half == 0, s_base, r_base) + c

        if side_len > 1:
            @pl.when(jnp.logical_not(inner))
            def _():
                slot = near_slot(edge + 1, p, half, b, c)
                remote(src, near.at[b, p, q], in_send.at[slot], in_recv.at[slot], in_dev).start()

        @pl.when(jnp.logical_and(inner, half == 0))
        def _():
            slot = far_slot(p, b, c)
            remote(src, far.at[b, p, c], in_send.at[slot], far_recv.at[slot], in_dev).start()

    freq_dev = {"freq": n_freq - 1 - fq}
    barrier = pltpu.get_barrier_semaphore()
    up, down = z < m - 1, z > 0
    greeted = [pair_dev, {"pts": 1 - core}, freq_dev]

    def greet(sem, device):
        pl.semaphore_signal(sem, inc=1, device_id=device, device_id_type=MESH)

    def along_z(sem_down, sem_up):
        @pl.when(up)
        def _():
            greet(sem_up, {"stn": me + 2})

        @pl.when(down)
        def _():
            greet(sem_down, {"stn": me - 2})

    for device in greeted:
        greet(barrier, device)
    along_z(barrier, barrier)
    pl.semaphore_wait(barrier, len(greeted) + up.astype(jnp.int32) + down.astype(jnp.int32))

    def hello():
        @pl.loop(0, m - 1)
        def _(r):
            along_z(hello_sem.at[0, r], hello_sem.at[1, r])

            @pl.when(up)
            def _():
                pl.semaphore_wait(hello_sem.at[0, r], 1)

            @pl.when(down)
            def _():
                pl.semaphore_wait(hello_sem.at[1, r], 1)

        for i, device in enumerate((pair_dev, freq_dev)):
            greet(pair_hello.at[i], device)
            pl.semaphore_wait(pair_hello.at[i], 1)

    every_row = pl.ds(0, h)
    pair_rows = pl.ds(pl.multiple_of(core * half_rows, 8), half_rows)

    def pair_q(i):
        return jnp.where(i < nq, s_base + i, r_base + i - nq)

    def pair_copy(i):
        q = pair_q(i)
        return remote(
            greens.at[:, 1 - parity, :, columns(q)], g_pair.at[q],
            pair_send.at[i], pair_recv.at[i], pair_dev,
        )

    def w_pair_copy(j):
        return remote(
            w_src(1 - parity, j, pair_rows), w_pair.at[j, :, pair_rows, :],
            wp_send.at[j], wp_recv.at[j], pair_dev,
        )

    def sibling_copy(rows):
        return remote(
            w_pair.at[:, :, rows, :], w_pair.at[:, :, rows, :],
            sib_sem.at[0], sib_sem.at[1], {"pts": 1 - core},
        )

    def own_copy(q):
        return pltpu.make_async_copy(
            greens.at[:, parity, :, columns(q)], g_own.at[q], own_sem.at[q]
        )

    def w_own_copy(j):
        return pltpu.make_async_copy(w_src(parity, j, every_row), w_own.at[j], w_own_sem.at[j])

    @pl.loop(0, 2 * nq)
    def _(i):
        @pl.when(i < nq)
        def _():
            pair_copy(i).start()

        half = i // nq
        c = lax.rem(i, nq)
        send_inward(greens.at[:, parity, :, columns(pair_q(i))], 0, half, edge, c)
        own_copy(i).start()

    @pl.loop(0, n)
    def _(j):
        w_pair_copy(j).start()
        w_own_copy(j).start()

    @pl.loop(nq, 2 * nq)
    def _(i):
        pair_copy(i).start()

    hello()

    acc[...] = jnp.zeros_like(acc)

    @pl.loop(0, 2 * nq)
    def _(q):
        own_copy(q).wait()

    @pl.loop(0, n)
    def _(j):
        w_own_copy(j).wait()

    def contribute(w, gi, gj, q, weight):
        for s in range(sub):
            part = slice(s * LANES, (s + 1) * LANES)
            both = jnp.concatenate([gj[0, :, part], gj[1, :, part]], axis=1)
            ab = jnp.dot(w[...].reshape(2 * h, h), both, preferred_element_type=jnp.float32)
            a, b = ab[:h], ab[h:]
            t = gi[0, :, part].astype(jnp.float32) * (a[:, :LANES] - b[:, LANES:])
            t = t + gi[1, :, part].astype(jnp.float32) * (a[:, LANES:] + b[:, :LANES])
            t = jnp.sum(t.reshape(h // 8, 8, LANES), axis=0)
            acc[q * sub + s] += t * weight

    def far_at(t):
        p = t // (side_len * nq)
        rest = lax.rem(t, side_len * nq)
        return p, side_len - 1 - rest // nq, lax.rem(rest, nq)

    def near_at(t):
        width = jnp.maximum(edge, 1) * nq
        p = t // (2 * width)
        half = lax.rem(t // width, 2)
        rest = lax.rem(t, width)
        return p, half, jnp.maximum(edge, 1) - 1 - rest // nq, lax.rem(rest, nq)

    def part_of(p):
        return jnp.where(p == 0, parity, 1 - parity)

    def far_work(t, w, g):
        p, b, c = far_at(t)
        q = r_base + c
        j = global_block(b, True) * 2 + part_of(p)
        contribute(w.at[j], g.at[q], far.at[b, p, c], q, 2.0)

    def near_work(t, w, g):
        p, half, b, c = near_at(t)
        q = jnp.where(half == 0, s_base, r_base) + c
        j = global_block(b, False) * 2 + part_of(p)
        contribute(w.at[j], g.at[q], near.at[b, p, q], q, 2.0)

    def far_wait(t):
        p, b, c = far_at(t)
        ref = far.at[b, p, c]
        remote(ref, ref, out_send.at[t], far_recv.at[t], in_dev).wait_recv()

        @pl.when(edge > 0)
        def _():
            remote(ref, ref, out_send.at[t], far_recv.at[t], out_dev).start()

    def near_wait(t):
        p, half, b, c = near_at(t)
        q = jnp.where(half == 0, s_base, r_base) + c
        ref = near.at[b, p, q]
        remote(ref, ref, in_send.at[t], in_recv.at[t], out_dev).wait_recv()
        send_inward(ref, p, half, b, c)

    def newest(u):
        far_work(u, w_pair, g_pair)

        @pl.when(u < n_near)
        def _():
            near_work(u, w_pair, g_pair)

    @pl.loop(0, steps)
    def _(t):
        has_pair = jnp.logical_and(jnp.logical_and(t >= nq, t <= 3 * nq), t != 2 * nq)
        turn = t - nq - (t > 2 * nq).astype(jnp.int32)

        @pl.when(has_pair)
        def _():
            i = turn
            pair_copy(i).wait_recv()
            send_inward(g_pair.at[pair_q(i)], 1, i // nq, edge, lax.rem(i, nq))

        @pl.when(t < n_far)
        def _():
            far_wait(t)

        if side_len > 1:
            @pl.when(t < n_near)
            def _():
                near_wait(t)

        @pl.when(t == catch_up - 1)
        def _():
            @pl.loop(0, n)
            def _(j):
                w_pair_copy(j).wait_recv()

            sibling_copy(pair_rows).start()

        @pl.when(t < 2 * nq)
        def _():
            contribute(w_own.at[2 * z + parity], g_own.at[t], g_own.at[t], t, 1.0)

        @pl.when(has_pair)
        def _():
            q = pair_q(turn)
            contribute(w_own.at[2 * z + 1 - parity], g_own.at[q], g_pair.at[q], q, 2.0)

        @pl.when(t < n_far)
        def _():
            far_work(t, w_own, g_own)

        if side_len > 1:
            @pl.when(t < n_near)
            def _():
                near_work(t, w_own, g_own)

        @pl.when(t == catch_up)
        def _():
            sibling_copy(pl.ds(pl.multiple_of((1 - core) * half_rows, 8), half_rows)).wait_recv()

        @pl.when(t >= catch_up)
        def _():
            first = (t - catch_up) * per_step
            last = jnp.minimum(first + per_step, steps)
            if spread:
                first = ((t - catch_up) * 2 * nq) // left
                last = ((t - catch_up + 1) * 2 * nq) // left

            @pl.loop(first, last)
            def _(u):
                @pl.when(u < 2 * nq)
                def _():
                    q = pair_q(u)
                    contribute(w_pair.at[2 * z + 1 - parity], g_pair.at[q], g_pair.at[q], q, 1.0)

                if spread:
                    far_work(lax.rem(u, side_len) * nq + u // side_len, w_pair, g_pair)
                else:
                    @pl.when(u < n_far)
                    def _():
                        far_work(u, w_pair, g_pair)

                if side_len > 1:
                    @pl.when(u < n_near)
                    def _():
                        near_work(u, w_pair, g_pair)

            if spread:
                newest(t - 1)

    if spread:
        newest(steps - 1)

    total = n * n_freq
    rank = me * n_freq + fq
    red[rank] = jnp.sum(acc[...], axis=1) / stations

    def share_copy(k, source):
        target = lax.rem(rank + k, total)
        return remote(
            red.at[source], red.at[source], red_send.at[k - 1], red_recv.at[k - 1],
            {"stn": target // n_freq, "freq": lax.rem(target, n_freq)},
        )

    @pl.loop(1, total)
    def _(k):
        share_copy(k, rank).start()

    @pl.loop(1, total)
    def _(k):
        share_copy(k, lax.rem(rank - k + total, total)).wait_recv()

    raw = red[0]
    for d in range(1, total):
        raw = raw + red[d]
    max_out[...] = jnp.broadcast_to(jnp.max(jnp.abs(raw)), max_out.shape)
    max_copy = remote(max_out, max_in, max_sem.at[0], max_sem.at[1], {"pts": 1 - core})
    max_copy.start()

    @pl.loop(1, total)
    def _(k):
        share_copy(k, rank).wait_send()

    @pl.loop(0, 2 * nq)
    def _(i):
        pair_copy(i).wait_send()

    @pl.loop(0, n)
    def _(j):
        w_pair_copy(j).wait_send()

    sibling_copy(pair_rows).wait_send()
    ref = far.at[0, 0, 0]

    @pl.loop(0, jnp.where(inner, n_far, (edge + 1) * 4 * nq))
    def _(t):
        remote(ref, ref, in_send.at[t], far_recv.at[0], in_dev).wait_send()

    @pl.when(edge > 0)
    def _():
        @pl.loop(0, n_far)
        def _(t):
            remote(ref, ref, out_send.at[t], far_recv.at[0], out_dev).wait_send()

    max_copy.wait()
    largest = jnp.maximum(max_out[0:1, 0:1], max_in[0:1, 0:1])
    out[...] = raw / (largest + 1e-6)


def kernel_body(n, n_freq, greens, weights):
    _, _, h, points = greens.shape
    stations = weights.shape[3]
    half = points // 2
    chunk = LANES
    while chunk * 2 * h <= 32768 and half % (chunk * 2) == 0:
        chunk *= 2
    nq = half // chunk
    side_len = n // 4
    n_far = side_len * 2 * nq
    n_near = max(side_len - 1, 1) * 4 * nq
    blocked = h % LANES != 0
    if blocked:
        weights = weights.reshape(2, weights.shape[1], h, n, h).swapaxes(2, 3)
    if side_len == 2 and nq >= 4:
        return line_body(n_freq, chunk, nq, blocked, greens, weights)
    dma = pltpu.SemaphoreType.DMA
    bf16, f32 = jnp.bfloat16, jnp.float32
    rows = points // LANES
    out = pl.pallas_call(
        functools.partial(ring_kernel, n, n_freq, h, stations, chunk, nq, blocked),
        out_shape=jax.ShapeDtypeStruct((rows, LANES), f32),
        in_specs=[pl.BlockSpec(memory_space=pl.ANY)] * 2,
        out_specs=pl.BlockSpec(memory_space=pltpu.VMEM),
        scratch_shapes=[
            pltpu.VMEM((2 * nq, 2, h, chunk), bf16),
            pltpu.VMEM((2 * nq, 2, h, chunk), bf16),
            pltpu.VMEM((max(side_len - 1, 1), 2, 2 * nq, 2, h, chunk), bf16),
            pltpu.VMEM((side_len, 2, nq, 2, h, chunk), bf16),
            pltpu.VMEM((n, 2, h, h), bf16),
            pltpu.VMEM((n, 2, h, h), bf16),
            pltpu.VMEM((rows, 8, LANES), f32),
            pltpu.VMEM((n * n_freq, rows, LANES), f32),
            pltpu.VMEM((8, LANES), f32),
            pltpu.VMEM((8, LANES), f32),
            dma((2 * nq,)), dma((n,)), dma((2 * nq,)), dma((2 * nq,)), dma((n,)), dma((n,)), dma((2,)),
            dma((max(n_near, n_far),)), dma((n_near,)), dma((n_far,)), dma((n_far,)),
            dma((n * n_freq - 1,)), dma((n * n_freq - 1,)), dma((2,)),
            pltpu.SemaphoreType.REGULAR((2, n // 2 - 1)), pltpu.SemaphoreType.REGULAR((2,)),
        ],
        compiler_params=pltpu.CompilerParams(
            collective_id=0, has_side_effects=True, vmem_limit_bytes=60 * 1024 * 1024
        ),
    )(greens, weights)
    return out.reshape(points)


FAR_FIRST = (11, 9, 10, 8, 15, 7, 13, 14, 5, 6, 12, 4, 3, 1, 2, 0)


def line_kernel(
    n_freq, h, stations, chunk, nq, kept, late, blocked,
    greens, weights, out,
    g_own, g_pair, near, far, w_own, w_pair, w_edge, folded, lent, acc, part, side, sums, extras,
    own_sem, w_own_sem, pair_send, pair_recv, wp_send, wp_recv, sib_sem, we_send, we_recv, we_sib,
    in_send, near_recv, far_recv, down_send, back_send, part_send, part_recv, side_sem,
    extra_send, extra_recv, base_sem, fold_sem, lend_sem, reply_sem, hello_sem, pair_hello,
):
    n = 8
    sub = chunk // LANES
    half_rows = h // 2
    steps = 4 * nq
    me = lax.axis_index("stn")
    core = lax.axis_index("pts")
    fq = lax.axis_index("freq")
    parity = lax.rem(me, 2)
    z = me // 2
    hi = z // 2
    inner = jnp.logical_or(z == 1, z == 2)
    outer = jnp.logical_not(inner)
    s_base = hi * nq
    r_base = (1 - hi) * nq
    rank = me * n_freq + fq
    total = n * n_freq
    inward = jnp.where(hi == 1, -2, 2)
    pair_dev = {"stn": me + 1 - 2 * parity}
    in_dev = {"stn": me + inward}
    out_dev = {"stn": me - inward}
    core_dev = {"pts": 1 - core}
    freq_dev = {"freq": n_freq - 1 - fq}
    across_dev = {"stn": 2 * (3 - z) + parity}
    other_inner = 2 - hi
    other_edge = 3 - 3 * hi
    near_z = jnp.where(inner, z - inward // 2, z + inward // 2)

    def columns(q):
        return pl.ds(pl.multiple_of(q * chunk, LANES), chunk)

    def w_src(freq, j, rows):
        if blocked:
            return weights.at[:, freq, j, rows, :]
        return weights.at[:, freq, rows, pl.ds(pl.multiple_of(j * h, LANES), h)]

    def block_of(where, p):
        return 2 * where + jnp.where(p == 0, parity, 1 - parity)

    def far_block(e):
        return block_of(jnp.where(lax.rem(e, 2) == 0, other_inner, other_edge), e // 2)

    def position(e, c):
        late_c = c >= jnp.where(e < 2, nq - 1, kept)
        pair_half = jnp.where(e == 2, 2 * nq, 2 * nq + kept) + c
        pair_late = jnp.where(e == 2, 2 * nq + kept, 3 * nq) + c
        early = jnp.where(late_c, 2 * nq - 2 + e, e * (nq - 1) + c)
        return jnp.where(e < 2, early, jnp.where(late_c, pair_late, pair_half))

    def block_at(t):
        e = (t >= nq - 1).astype(jnp.int32)
        c = t - e * (nq - 1)
        corner = t >= 2 * nq - 2
        e = jnp.where(corner, t - (2 * nq - 2), e)
        c = jnp.where(corner, nq - 1, c)
        pairs = t - 2 * nq
        third = jnp.logical_and(pairs >= kept, pairs < 2 * kept)
        third = jnp.logical_or(third, pairs >= nq + kept)
        pair_c = jnp.where(pairs < kept, pairs, jnp.where(pairs < nq + kept, pairs - kept, pairs - nq))
        e = jnp.where(pairs >= 0, 2 + third.astype(jnp.int32), e)
        c = jnp.where(pairs >= 0, pair_c, c)
        return e, c

    every_row = pl.ds(0, h)
    my_rows = pl.ds(pl.multiple_of(core * half_rows, 8), half_rows)
    sib_rows = pl.ds(pl.multiple_of((1 - core) * half_rows, 8), half_rows)

    def pair_q(i):
        return jnp.where(i < nq, s_base + i, r_base + i - nq)

    def g_src(q):
        return greens.at[:, parity, :, columns(q)]

    def own_copy(q):
        return pltpu.make_async_copy(g_src(q), g_own.at[q], own_sem.at[0])

    def w_own_copy(j):
        return pltpu.make_async_copy(w_src(parity, j, every_row), w_own.at[j], w_own_sem.at[0])

    def pair_copy(i):
        q = pair_q(i)
        return remote(
            greens.at[:, 1 - parity, :, columns(q)], g_pair.at[q],
            pair_send.at[0], pair_recv.at[i], pair_dev,
        )

    def w_pair_copy(j):
        return remote(
            w_src(1 - parity, j, my_rows), w_pair.at[j, :, my_rows, :],
            wp_send.at[0], wp_recv.at[0], pair_dev,
        )

    def sibling_copy(rows):
        part_of_w = w_pair.at[:, :, rows, :]
        return remote(part_of_w, part_of_w, sib_sem.at[0], sib_sem.at[1], core_dev)

    def edge_sibling_copy(rows):
        part_of_w = w_edge.at[:, :, :, rows, :]
        return remote(part_of_w, part_of_w, we_sib.at[0], we_sib.at[1], core_dev)

    def near_slot(p, i):
        return p * (2 * nq - kept) + jnp.where(i < nq, i, i - kept)

    def whole(ref, send_sem, recv_sem):
        return remote(ref, ref, send_sem.at[0], recv_sem.at[0], pair_dev)

    def up_copy(src, p, i):
        return remote(src, near.at[p, pair_q(i)], in_send.at[0], near_recv.at[near_slot(p, i)], in_dev)

    def up_weights(src, b, p):
        return remote(src, w_edge.at[b, p, :, my_rows, :], we_send.at[0], we_recv.at[0], in_dev)

    def mid_copy(src, slot):
        return remote(src, far.at[slot], in_send.at[0], far_recv.at[slot], in_dev)

    def lend_copy():
        src = near.at[1, pair_q(nq - 1)]
        return remote(src, lent, lend_sem.at[0], lend_sem.at[1], core_dev)

    corner = 2 * nq - 2

    def down_copy(slot):
        return remote(far.at[slot], far.at[slot], down_send.at[0], far_recv.at[slot], out_dev)

    def back_copy(src, p, c):
        return remote(
            src, near.at[p, r_base + c], back_send.at[0], near_recv.at[near_slot(p, c)], out_dev,
        )

    barrier = pltpu.get_barrier_semaphore()
    up, down = z < 3, z > 0
    greeted = [pair_dev, core_dev, freq_dev]

    def greet(sem, device):
        pl.semaphore_signal(sem, inc=1, device_id=device, device_id_type=MESH)

    def along_z(sem_down, sem_up):
        @pl.when(up)
        def _():
            greet(sem_up, {"stn": me + 2})

        @pl.when(down)
        def _():
            greet(sem_down, {"stn": me - 2})

    @pl.when(inner)
    def _():
        greet(barrier, in_dev)
        greet(barrier, out_dev)

    for device in greeted:
        greet(barrier, device)
    pl.semaphore_wait(barrier, len(greeted) + 1)

    @pl.when(outer)
    def _():
        greet(reply_sem.at[0], in_dev)

    @pl.loop(0, nq)
    def _(i):
        src = g_src(pair_q(i))

        @pl.when(jnp.logical_and(inner, i < nq - 1))
        def _():
            mid_copy(src, i).start()

        @pl.when(outer)
        def _():
            up_copy(src, 0, i).start()

    corner_src = g_src(pair_q(nq - 1))

    @pl.loop(0, n)
    def _(j):
        w_pair_copy(j).start()
        w_own_copy(j).start()

    @pl.loop(0, 2 * nq)
    def _(i):
        own_copy(pair_q(i)).start()
        pair_copy(i).start()

    @pl.when(inner)
    def _():
        pl.semaphore_wait(reply_sem.at[0], 1)

        @pl.loop(0, kept)
        def _(c):
            back_copy(g_src(pair_q(nq + c)), 0, c).start()

    @pl.when(outer)
    def _():
        for b in range(2):
            up_weights(w_src(parity, far_block(2 + b), my_rows), b, 0).start()

    @pl.loop(0, 3)
    def _(r):
        along_z(hello_sem.at[0, r], hello_sem.at[1, r])

        @pl.when(up)
        def _():
            pl.semaphore_wait(hello_sem.at[0, r], 1)

        @pl.when(down)
        def _():
            pl.semaphore_wait(hello_sem.at[1, r], 1)

    for i, device in enumerate((pair_dev, freq_dev, core_dev)):
        greet(pair_hello.at[i], device)
        pl.semaphore_wait(pair_hello.at[i], 1)

    acc[...] = jnp.zeros_like(acc)

    pltpu.make_async_copy(g_own, g_own, own_sem.at[0]).wait()
    pltpu.make_async_copy(w_own, w_own, w_own_sem.at[0]).wait()

    def product(w, gi, gj, s):
        lanes = slice(s * LANES, (s + 1) * LANES)
        both = jnp.concatenate([gj[0, :, lanes], gj[1, :, lanes]], axis=1)
        ab = jnp.dot(w[...].reshape(2 * h, h), both, preferred_element_type=jnp.float32)
        a, b = ab[:h], ab[h:]
        t = gi[0, :, lanes].astype(jnp.float32) * (a[:, :LANES] - b[:, LANES:])
        t = t + gi[1, :, lanes].astype(jnp.float32) * (a[:, LANES:] + b[:, :LANES])
        return jnp.sum(t.reshape(h // 8, 8, LANES), axis=0)

    def contribute(w, gi, gj, q, weight):
        for s in range(sub):
            acc[q * sub + s] += product(w, gi, gj, s) * weight

    own_pair_block = block_of(z, 1)

    def own_work(q):
        contribute(w_own.at[me], g_own.at[q], g_own.at[q], q, 1.0)

    def cross_work(q):
        contribute(w_own.at[own_pair_block], g_own.at[q], g_pair.at[q], q, 2.0)

    def pair_work(q):
        contribute(w_pair.at[own_pair_block], g_pair.at[q], g_pair.at[q], q, 1.0)

    def far_work(e, c, w, g):
        q = r_base + c
        contribute(w.at[far_block(e)], g.at[q], far.at[position(e, c)], q, 2.0)

    def near_work(p, q, w, g):
        contribute(w.at[block_of(near_z, p)], g.at[q], near.at[p, q], q, 2.0)

    def edge_work(b, c):
        q = r_base + c

        @pl.loop(0, 2)
        def _(p):
            contribute(w_edge.at[b, p], near.at[p, q], far.at[position(2 + b, c)], q, 2.0)

    def transposed(w, g):
        return lax.dot_general(w, g, (((0,), (0,)), ((), ())), preferred_element_type=jnp.float32)

    def fold(w, gi, s):
        lanes = slice(s * LANES, (s + 1) * LANES)
        both = jnp.concatenate([gi[0, :, lanes], gi[1, :, lanes]], axis=1)
        a, b = transposed(w[0], both), transposed(w[1], both)
        return a[:, :LANES] + b[:, LANES:], a[:, LANES:] - b[:, :LANES]

    def fold_last():
        q, j = r_base + nq - 1, far_block(3)
        for s in range(sub):
            lanes = slice(s * LANES, (s + 1) * LANES)
            re, im = fold(w_own.at[j], g_own.at[q], s)
            folded[core, 0, :, lanes] = re
            folded[core, 1, :, lanes] = im
            for w, g in ((w_pair.at[j], g_pair.at[q]), (w_edge.at[1, 0], near.at[0, q]), (w_edge.at[1, 1], near.at[1, q])):
                re, im = fold(w, g, s)
                folded[core, 0, :, lanes] += re
                folded[core, 1, :, lanes] += im

        @pl.when(core == 0)
        def _():
            fold_copy().start()

    def fold_copy():
        return remote(folded.at[0], folded.at[0], fold_sem.at[0], fold_sem.at[1], core_dev)

    def unfold(which, slot, s):
        lanes = slice(s * LANES, (s + 1) * LANES)
        t = far[slot, 0, :, lanes].astype(jnp.float32) * folded[which, 0, :, lanes]
        t = t + far[slot, 1, :, lanes].astype(jnp.float32) * folded[which, 1, :, lanes]
        return 2.0 * jnp.sum(t.reshape(h // 8, 8, LANES), axis=0)

    def passed_down(t):
        return t < 2 * nq + 2 * kept

    def wait_far(t):
        ref = far.at[t]
        remote(ref, ref, in_send.at[0], far_recv.at[t], in_dev).wait_recv()

    def wait_near(p, i):
        ref = near.at[p, pair_q(i)]
        remote(ref, ref, in_send.at[0], near_recv.at[near_slot(p, i)], in_dev).wait_recv()

    def wait_back(p, c):
        ref = near.at[p, r_base + c]
        remote(ref, ref, in_send.at[0], near_recv.at[near_slot(p, c)], in_dev).wait_recv()

    def wait_w_pair():
        whole(w_pair.at[:, :, my_rows, :], wp_send, wp_recv).wait_recv()
        sibling_copy(my_rows).start()

    def share_part():
        part[rank] = jnp.sum(acc[...], axis=1) / stations

        @pl.loop(0, total // 2 - 1)
        def _(k):
            part_copy(total // 2 - 1 - k, rank).start()

    def at_rank(target):
        return {"stn": target // n_freq, "freq": lax.rem(target, n_freq)}

    def flipped(k):
        bit, flip = total // 2, jnp.int32(0)
        while bit:
            mine = lax.rem(rank // bit, 2)
            turn = lax.rem(k // bit, 2)
            flip = flip + bit * (mine + turn - 2 * mine * turn)
            bit //= 2
        return flip

    def part_copy(k, source):
        ref = part.at[source]
        return remote(ref, ref, part_send.at[0], part_recv.at[0], at_rank(flipped(k)))

    my_group = (hi * 2 + parity) * n_freq + fq
    late_rows = late * sub

    sends = [(k, other) for k in FAR_FIRST for other in range(2) if k or other]

    def extra_copy(k, other):
        def turned(v, bit):
            return 1 - v if k & bit else v

        message = extras.at[core * 4 * n_freq + my_group]
        target_z = 2 * turned(hi, 8) + turned(lax.rem(z, 2), 4)
        target = {
            "stn": 2 * target_z + turned(parity, 2), "freq": turned(fq, 1),
            "pts": 1 - core if other else core,
        }
        return remote(
            message, message, extra_send.at[other], extra_recv.at[core], target,
        )

    def late_row(t):
        return jnp.sum(t, axis=0, keepdims=True) / stations

    def finish():
        first = (r_base + nq - late) * sub
        for c in range(late_rows):
            extras[core * 4 * n_freq + my_group, c] = late_row(acc[first + c])
        for s in range(sub):
            extras[core * 4 * n_freq + my_group, late_rows + s] = jnp.zeros((1, LANES), jnp.float32)

        @pl.when(core == 1)
        def _():
            fold_copy().wait_recv()
            wait_far(steps)
            wait_far(steps - 1)
            for s in range(sub):
                c = late_rows - sub + s
                extras[4 * n_freq + my_group, c] = late_row(acc[first + c] + unfold(1, steps - 1, s))
                extras[4 * n_freq + my_group, late_rows + s] = late_row(unfold(0, steps, s))

        for k, other in sends:
            extra_copy(k, other).start()

    near_second = nq + 4
    near_third = near_second + nq
    near_fourth = near_third + nq - kept
    near_end = near_fourth + nq - kept

    def near_at(t):
        i = jnp.where(t >= near_second, t - near_second, t)
        i = jnp.where(t >= near_third, t - near_third + nq + kept, i)
        i = jnp.where(t >= near_fourth, t - near_fourth + nq + kept, i)
        second = jnp.logical_and(t >= near_second, t < near_third)
        p = jnp.logical_or(second, t >= near_fourth).astype(jnp.int32)
        present = jnp.logical_or(t < nq, jnp.logical_and(t >= near_second, t < near_end))
        return present, p, i

    @pl.when(inner)
    def _():
        @pl.loop(0, steps - 1)
        def _(t):
            has_near, p, i = near_at(t)
            has_pair = jnp.logical_and(t >= nq, t < 3 * nq)
            turn = t - nq
            wait_far(t)

            @pl.when(passed_down(t))
            def _():
                down_copy(t).start()

            @pl.when(has_near)
            def _():
                wait_near(p, i)

            @pl.when(t < nq)
            def _():
                mid_copy(near.at[0, pair_q(t)], position(1, t)).start()

            @pl.when(t == nq - 2)
            def _():
                mid_copy(corner_src, corner).start()

            @pl.when(t == nq)
            def _():
                wait_w_pair()

            @pl.when(has_pair)
            def _():
                pair_copy(turn).wait_recv()

                @pl.when(turn < kept)
                def _():
                    mid_copy(g_pair.at[pair_q(turn)], 2 * nq + turn).start()

                @pl.when(jnp.logical_and(turn >= nq, turn < nq + kept))
                def _():
                    back_copy(g_pair.at[pair_q(turn)], 1, turn - nq).start()

            third = t - near_second
            fourth = third - (nq - kept)

            @pl.when(jnp.logical_and(third >= 0, third < kept))
            def _():
                mid_copy(near.at[1, pair_q(third)], 2 * nq + kept + third).start()

            send_third = jnp.logical_and(third >= kept, third < nq)

            @pl.when(send_third)
            def _():
                mid_copy(g_pair.at[pair_q(third)], 2 * nq + kept + third).start()

            @pl.when(jnp.logical_and(third == nq - 1, core == 0))
            def _():
                lend_copy().start()

            @pl.when(jnp.logical_and(fourth >= kept, fourth < nq - 1 + core))
            def _():
                mid_copy(near.at[1, pair_q(fourth)], 3 * nq + fourth).start()

            @pl.when(jnp.logical_and(fourth == nq - 1, core == 1))
            def _():
                lend_copy().wait_recv()
                mid_copy(lent, steps).start()

            @pl.when(t == nq + 2)
            def _():
                sibling_copy(sib_rows).wait_recv()

            @pl.when(t == near_second)
            def _():
                whole(w_edge.at[:, :, :, my_rows, :], we_send, we_recv).wait_recv()
                edge_sibling_copy(my_rows).start()

            @pl.when(t == near_second + 2)
            def _():
                edge_sibling_copy(sib_rows).wait_recv()

            e, c = block_at(t)
            far_work(e, c, w_own, g_own)

            @pl.when(t < 2 * nq)
            def _():
                own_work(t)

            @pl.when(has_near)
            def _():
                q = pair_q(i)
                near_work(p, q, w_own, g_own)

                @pl.when(t >= nq)
                def _():
                    near_work(p, q, w_pair, g_pair)

                @pl.when(t >= near_fourth)
                def _():
                    edge_work(0, i - nq)

            @pl.when(has_pair)
            def _():
                cross_work(pair_q(turn))

            lag = t - nq - 2

            @pl.when(jnp.logical_and(lag >= 0, lag < 2 * nq))
            def _():
                pair_work(pair_q(lag))

                @pl.when(lag < nq)
                def _():
                    near_work(0, pair_q(lag), w_pair, g_pair)

            @pl.when(t >= 2 * nq)
            def _():
                far_work(e, c, w_pair, g_pair)

                @pl.when(t < 3 * nq)
                def _():
                    @pl.loop(0, 2)
                    def _(first):
                        far_work(first, t - 2 * nq, w_pair, g_pair)

            @pl.when(t >= 3 * nq + kept)
            def _():
                edge_work(1, t - 3 * nq)

            @pl.when(t == steps - late - 1)
            def _():
                share_part()

                @pl.loop((nq - late) * sub, nq * sub)
                def _(c):
                    acc[r_base * sub + c] = jnp.zeros((8, LANES), jnp.float32)

            @pl.when(t == near_end - 1)
            def _():
                fold_last()

        finish()

    @pl.when(outer)
    def _():
        @pl.loop(0, 3 * nq)
        def _(t):
            turn = t - nq + 2
            has_pair = jnp.logical_and(turn >= 0, turn < 2 * nq)
            back = t - 2 * nq - 4
            has_back = jnp.logical_and(back >= 0, back < kept)
            e, c = block_at(t)
            has_far = t < 2 * nq + 2 * kept

            @pl.when(turn == 0)
            def _():
                wait_w_pair()
                for b in range(2):
                    up_weights(w_pair.at[far_block(2 + b), :, my_rows, :], b, 1).start()

            @pl.when(has_pair)
            def _():
                pair_copy(turn).wait_recv()

                @pl.when(jnp.logical_or(turn < nq, turn >= nq + kept))
                def _():
                    up_copy(g_pair.at[pair_q(turn)], 1, turn).start()

                @pl.when(turn == nq - 1)
                def _():
                    @pl.loop(nq + kept, 2 * nq)
                    def _(i):
                        up_copy(g_src(pair_q(i)), 0, i).start()

            @pl.when(t == nq)
            def _():
                sibling_copy(sib_rows).wait_recv()

            @pl.when(t < kept)
            def _():
                wait_back(0, t)

            @pl.when(has_back)
            def _():
                wait_back(1, back)

            @pl.when(has_far)
            def _():
                wait_far(t)
                far_work(e, c, w_own, g_own)

            @pl.when(jnp.logical_and(has_far, t >= 2 * nq))
            def _():
                far_work(e, c, w_pair, g_pair)

            @pl.when(t < 2 * nq)
            def _():
                own_work(t)

            @pl.when(t < kept)
            def _():
                near_work(0, r_base + t, w_own, g_own)

            @pl.when(has_back)
            def _():
                q = r_base + back
                near_work(0, q, w_pair, g_pair)
                near_work(1, q, w_own, g_own)
                near_work(1, q, w_pair, g_pair)

            @pl.when(has_pair)
            def _():
                cross_work(pair_q(turn))

            @pl.when(t >= nq)
            def _():
                pair_work(pair_q(t - nq))

            @pl.when(t >= 2 * nq)
            def _():
                @pl.loop(0, 2)
                def _(first):
                    far_work(first, t - 2 * nq, w_pair, g_pair)

        share_part()

    parts = part.at[pl.ds(0, total // 2 - 1)]
    whole(parts, part_send, part_recv).wait_recv()

    base = hi * (total // 2)
    mine = part[base]
    for d in range(1, total // 2):
        mine = mine + part[base + d]
    side[hi] = mine

    def side_copy(which):
        ref = side.at[which]
        return remote(ref, ref, side_sem.at[0], side_sem.at[1], across_dev)

    side_copy(hi).start()
    side_copy(1 - hi).wait_recv()
    sums[core] = side[0] + side[1]
    base_copy = remote(sums.at[core], sums.at[core], base_sem.at[0], base_sem.at[1], core_dev)
    base_copy.start()

    whole(g_pair, pair_send, pair_recv).wait_send()
    whole(w_pair.at[:, :, my_rows, :], wp_send, wp_recv).wait_send()
    sibling_copy(my_rows).wait_send()
    whole(parts, part_send, part_recv).wait_send()

    def sent(count, send_sem):
        whole(far.at[pl.ds(0, count)], send_sem, far_recv).wait_send()

    @pl.when(inner)
    def _():
        sent(2 * nq + 2 * kept, down_send)
        sent(2 * kept, back_send)
        edge_sibling_copy(my_rows).wait_send()
        for other in range(2):
            ref = extras.at[pl.ds(0, total - 1 + other)]
            remote(ref, ref, extra_send.at[other], extra_recv.at[0], core_dev).wait_send()

        @pl.when(core == 0)
        def _():
            sent(steps - 1, in_send)
            fold_copy().wait_send()
            lend_copy().wait_send()

        @pl.when(core == 1)
        def _():
            sent(steps + 1, in_send)

    @pl.when(outer)
    def _():
        sent(steps - 2 * kept, in_send)
        whole(w_edge.at[:, :, :, my_rows, :], we_send, we_recv).wait_send()

    side_copy(hi).wait_send()

    def wait_extras(which, groups):
        ref = extras.at[pl.ds(which * 4 * n_freq, groups)]
        remote(ref, ref, extra_send.at[0], extra_recv.at[which], core_dev).wait_recv()

    @pl.when(inner)
    def _():
        wait_extras(core, 4 * n_freq - 1)
        wait_extras(1 - core, 4 * n_freq)

    @pl.when(outer)
    def _():
        wait_extras(0, 4 * n_freq)
        wait_extras(1, 4 * n_freq)

    base_copy.wait_send()
    sum_ref = sums.at[1 - core]
    remote(sum_ref, sum_ref, base_sem.at[0], base_sem.at[1], core_dev).wait_recv()

    def late_sum(which, low, c):
        first = (2 * which + low) * 2 * n_freq
        row = extras[first, c]
        for g in range(1, 2 * n_freq):
            row = row + extras[first + g, c]
        return row

    for which in range(2):
        for low in range(2):
            gathered = [late_sum(which, low, c) for c in range(late_rows)]
            if which == 0:
                for s in range(sub):
                    gathered[late_rows - sub + s] += late_sum(1, low, late_rows + s)
            at = ((1 - low) * nq + nq - late) * sub
            sums[which, at:at + late_rows, :] += jnp.concatenate(gathered, axis=0)

    largest = jnp.max(jnp.maximum(jnp.abs(sums[0]), jnp.abs(sums[1])), keepdims=True)
    out[...] = sums[core] / (largest + 1e-6)


def line_body(n_freq, chunk, nq, blocked, greens, weights):
    _, _, h, points = greens.shape
    n = 8
    kept, late = 3 * nq // 8, 4
    stations = n * h
    dma = pltpu.SemaphoreType.DMA
    one, two = dma((1,)), dma((2,))
    regular = pltpu.SemaphoreType.REGULAR
    bf16, f32 = jnp.bfloat16, jnp.float32
    rows = points // LANES
    late_rows = late * (chunk // LANES)
    total = n * n_freq
    out = pl.pallas_call(
        functools.partial(line_kernel, n_freq, h, stations, chunk, nq, kept, late, blocked),
        out_shape=pltpu.VMEM((rows, LANES), f32),
        in_specs=[pl.BlockSpec(memory_space=pl.ANY)] * 2,
        out_specs=pl.BlockSpec(memory_space=pltpu.VMEM),
        scratch_shapes=[
            pltpu.VMEM((2 * nq, 2, h, chunk), bf16),
            pltpu.VMEM((2 * nq, 2, h, chunk), bf16),
            pltpu.VMEM((2, 2 * nq, 2, h, chunk), bf16),
            pltpu.VMEM((4 * nq + 1, 2, h, chunk), bf16),
            pltpu.VMEM((n, 2, h, h), bf16),
            pltpu.VMEM((n, 2, h, h), bf16),
            pltpu.VMEM((2, 2, 2, h, h), bf16),
            pltpu.VMEM((2, 2, h, chunk), f32),
            pltpu.VMEM((2, h, chunk), bf16),
            pltpu.VMEM((rows, 8, LANES), f32),
            pltpu.VMEM((total, rows, LANES), f32),
            pltpu.VMEM((2, rows, LANES), f32),
            pltpu.VMEM((2, rows, LANES), f32),
            pltpu.VMEM((8 * n_freq, late_rows + chunk // LANES, 1, LANES), f32),
            one, one, one, dma((2 * nq,)), one, one, two,
            one, one, two,
            one, dma((4 * nq - 2 * kept,)), dma((4 * nq + 1,)), one, one,
            one, one, two,
            two, two, two, two, two,
            regular((1,)), regular((2, 3)), regular((3,)),
        ],
        compiler_params=pltpu.CompilerParams(
            collective_id=0, has_side_effects=True, vmem_limit_bytes=60 * 1024 * 1024
        ),
    )(greens, weights)
    return out.reshape(points)


def passed_along(x, axis, by):
    size = lax.axis_size(axis)
    return lax.ppermute(x, axis, [(i, (i + by) % size) for i in range(size)])


def mixing_of(weights):
    negated = -weights[1]
    return jnp.stack([jnp.stack([weights[0], negated]), jnp.stack([weights[1], weights[0]])])


def body(greens, noise_weights):
    station_rows = greens.shape[2]
    stations = noise_weights.shape[3]
    device_index = lax.axis_index("stn")
    cycle_length = lax.axis_size("stn")
    mixing = mixing_of(noise_weights)

    def block_product(columns_start, arriving):
        block_rows = arriving.shape[2]
        weights_block = lax.dynamic_slice_in_dim(mixing, columns_start, block_rows, 4)
        return jnp.einsum(
            "ocfin,cfnx->ofix", weights_block, arriving, preferred_element_type=jnp.float32
        )

    half_way = cycle_length // 2
    diagonal = block_product(device_index * station_rows, greens)

    def advance(offset, loop_state):
        running, current = loop_state
        current = passed_along(current, "stn", -1)
        source = (device_index + offset) % cycle_length
        weight = jnp.where(offset == half_way, 1.0, 2.0).astype(jnp.float32)
        running = running + weight * block_product(source * station_rows, current)
        return (running, current)

    summed, current = lax.fori_loop(1, half_way + 1, advance, (diagonal, greens))
    green_real = greens[0].astype(jnp.float32)
    green_imag = greens[1].astype(jnp.float32)
    partial_kernel = (
        jnp.sum(green_real * summed[0] + green_imag * summed[1], axis=(0, 1)) / stations
    )
    raw_kernel = lax.psum(partial_kernel, "stn")
    raw_kernel = lax.psum(raw_kernel, "freq")
    largest = lax.pmax(jnp.max(jnp.abs(raw_kernel)), "pts")
    return raw_kernel / (largest + 1e-06)


def solution(mesh):
    n, cores, n_freq = mesh.shape["stn"], mesh.shape["pts"], mesh.shape["freq"]

    def either(greens, noise_weights):
        _, freqs, rows, points = greens.shape
        fits = n % 4 == 0 and cores == 2 and freqs == 2 and n_freq == 2 and rows % 32 == 0 and points % (2 * LANES) == 0
        if fits:
            return kernel_body(n, n_freq, greens, noise_weights)
        return body(greens, noise_weights)

    in_specs = (P(None, "freq", "stn", "pts"), P(None, "freq", "stn", None))
    return jax.shard_map(either, mesh=mesh, in_specs=in_specs, out_specs=P("pts"), check_vma=False)
```

```python
import functools

import jax
import jax.numpy as jnp
from jax import lax
from jax.experimental import pallas as pl
from jax.experimental.pallas import tpu as pltpu
from jax.sharding import PartitionSpec as P

MESH = pl.DeviceIdType.MESH
LANES = 128


def remote(src, dst, send_sem, recv_sem, target):
    return pltpu.make_async_remote_copy(
        src_ref=src, dst_ref=dst, send_sem=send_sem, recv_sem=recv_sem,
        device_id=target, device_id_type=MESH,
    )


def ring_kernel(
    n, n_freq, h, stations, chunk, nq, blocked,
    greens, weights, out,
    g_own, g_pair, near, far, w_own, w_pair, acc, red, max_out, max_in,
    own_sem, w_own_sem, pair_send, pair_recv, wp_send, wp_recv, sib_sem,
    in_send, in_recv, out_send, far_recv, red_send, red_recv, max_sem, hello_sem, pair_hello,
):
    m = n // 2
    side_len = m // 2
    sub = chunk // LANES
    half_rows = h // 2
    me = lax.axis_index("stn")
    core = lax.axis_index("pts")
    fq = lax.axis_index("freq")
    parity = lax.rem(me, 2)
    z = me // 2
    hi = (z >= side_len).astype(jnp.int32)
    edge = jnp.where(hi == 1, m - 1 - z, z)
    inward = jnp.where(hi == 1, -2, 2)
    inner = edge == side_len - 1
    s_base = hi * nq
    r_base = (1 - hi) * nq
    pair_dev = {"stn": me + 1 - 2 * parity}
    in_dev = {"stn": me + inward}
    out_dev = {"stn": me - inward}
    n_far = side_len * 2 * nq
    n_near = edge * 4 * nq
    n_near_max = (side_len - 1) * 4 * nq
    steps = max(n_far, n_near_max, 3 * nq + 2)
    spread = side_len == 2
    catch_up = 2 * nq + 1 if spread else max((steps * 25) // 32, 3 * nq + 1)
    left = steps - catch_up
    per_step = -(-steps // (steps - catch_up))

    def columns(q):
        return pl.ds(pl.multiple_of(q * chunk, LANES), chunk)

    def w_src(freq, j, rows):
        if blocked:
            return weights.at[:, freq, j, rows, :]
        return weights.at[:, freq, rows, pl.ds(pl.multiple_of(j * h, LANES), h)]

    def global_block(e, opposite):
        low = jnp.where(opposite, 1 - hi, hi) == 0
        return jnp.where(low, e, m - 1 - e)

    def near_slot(receiver_edge, p, half, b, c):
        return ((p * 2 + half) * receiver_edge + (receiver_edge - 1 - b)) * nq + c

    def far_slot(p, b, c):
        return (p * side_len + (side_len - 1 - b)) * nq + c

    def send_inward(src, p, half, b, c):
        q = jnp.where(half == 0, s_base, r_base) + c

        if side_len > 1:
            @pl.when(jnp.logical_not(inner))
            def _():
                slot = near_slot(edge + 1, p, half, b, c)
                remote(src, near.at[b, p, q], in_send.at[slot], in_recv.at[slot], in_dev).start()

        @pl.when(jnp.logical_and(inner, half == 0))
        def _():
            slot = far_slot(p, b, c)
            remote(src, far.at[b, p, c], in_send.at[slot], far_recv.at[slot], in_dev).start()

    freq_dev = {"freq": n_freq - 1 - fq}
    barrier = pltpu.get_barrier_semaphore()
    up, down = z < m - 1, z > 0
    greeted = [pair_dev, {"pts": 1 - core}, freq_dev]

    def greet(sem, device):
        pl.semaphore_signal(sem, inc=1, device_id=device, device_id_type=MESH)

    def along_z(sem_down, sem_up):
        @pl.when(up)
        def _():
            greet(sem_up, {"stn": me + 2})

        @pl.when(down)
        def _():
            greet(sem_down, {"stn": me - 2})

    for device in greeted:
        greet(barrier, device)
    along_z(barrier, barrier)
    pl.semaphore_wait(barrier, len(greeted) + up.astype(jnp.int32) + down.astype(jnp.int32))

    def hello():
        @pl.loop(0, m - 1)
        def _(r):
            along_z(hello_sem.at[0, r], hello_sem.at[1, r])

            @pl.when(up)
            def _():
                pl.semaphore_wait(hello_sem.at[0, r], 1)

            @pl.when(down)
            def _():
                pl.semaphore_wait(hello_sem.at[1, r], 1)

        for i, device in enumerate((pair_dev, freq_dev)):
            greet(pair_hello.at[i], device)
            pl.semaphore_wait(pair_hello.at[i], 1)

    every_row = pl.ds(0, h)
    pair_rows = pl.ds(pl.multiple_of(core * half_rows, 8), half_rows)

    def pair_q(i):
        return jnp.where(i < nq, s_base + i, r_base + i - nq)

    def pair_copy(i):
        q = pair_q(i)
        return remote(
            greens.at[:, 1 - parity, :, columns(q)], g_pair.at[q],
            pair_send.at[i], pair_recv.at[i], pair_dev,
        )

    def w_pair_copy(j):
        return remote(
            w_src(1 - parity, j, pair_rows), w_pair.at[j, :, pair_rows, :],
            wp_send.at[j], wp_recv.at[j], pair_dev,
        )

    def sibling_copy(rows):
        return remote(
            w_pair.at[:, :, rows, :], w_pair.at[:, :, rows, :],
            sib_sem.at[0], sib_sem.at[1], {"pts": 1 - core},
        )

    def own_copy(q):
        return pltpu.make_async_copy(
            greens.at[:, parity, :, columns(q)], g_own.at[q], own_sem.at[q]
        )

    def w_own_copy(j):
        return pltpu.make_async_copy(w_src(parity, j, every_row), w_own.at[j], w_own_sem.at[j])

    @pl.loop(0, 2 * nq)
    def _(i):
        @pl.when(i < nq)
        def _():
            pair_copy(i).start()

        half = i // nq
        c = lax.rem(i, nq)
        send_inward(greens.at[:, parity, :, columns(pair_q(i))], 0, half, edge, c)
        own_copy(i).start()

    @pl.loop(0, n)
    def _(j):
        w_pair_copy(j).start()
        w_own_copy(j).start()

    @pl.loop(nq, 2 * nq)
    def _(i):
        pair_copy(i).start()

    hello()

    acc[...] = jnp.zeros_like(acc)

    @pl.loop(0, 2 * nq)
    def _(q):
        own_copy(q).wait()

    @pl.loop(0, n)
    def _(j):
        w_own_copy(j).wait()

    def contribute(w, gi, gj, q, weight):
        for s in range(sub):
            part = slice(s * LANES, (s + 1) * LANES)
            both = jnp.concatenate([gj[0, :, part], gj[1, :, part]], axis=1)
            ab = jnp.dot(w[...].reshape(2 * h, h), both, preferred_element_type=jnp.float32)
            a, b = ab[:h], ab[h:]
            t = gi[0, :, part].astype(jnp.float32) * (a[:, :LANES] - b[:, LANES:])
            t = t + gi[1, :, part].astype(jnp.float32) * (a[:, LANES:] + b[:, :LANES])
            t = jnp.sum(t.reshape(h // 8, 8, LANES), axis=0)
            acc[q * sub + s] += t * weight

    def far_at(t):
        p = t // (side_len * nq)
        rest = lax.rem(t, side_len * nq)
        return p, side_len - 1 - rest // nq, lax.rem(rest, nq)

    def near_at(t):
        width = jnp.maximum(edge, 1) * nq
        p = t // (2 * width)
        half = lax.rem(t // width, 2)
        rest = lax.rem(t, width)
        return p, half, jnp.maximum(edge, 1) - 1 - rest // nq, lax.rem(rest, nq)

    def part_of(p):
        return jnp.where(p == 0, parity, 1 - parity)

    def far_work(t, w, g):
        p, b, c = far_at(t)
        q = r_base + c
        j = global_block(b, True) * 2 + part_of(p)
        contribute(w.at[j], g.at[q], far.at[b, p, c], q, 2.0)

    def near_work(t, w, g):
        p, half, b, c = near_at(t)
        q = jnp.where(half == 0, s_base, r_base) + c
        j = global_block(b, False) * 2 + part_of(p)
        contribute(w.at[j], g.at[q], near.at[b, p, q], q, 2.0)

    def far_wait(t):
        p, b, c = far_at(t)
        ref = far.at[b, p, c]
        remote(ref, ref, out_send.at[t], far_recv.at[t], in_dev).wait_recv()

        @pl.when(edge > 0)
        def _():
            remote(ref, ref, out_send.at[t], far_recv.at[t], out_dev).start()

    def near_wait(t):
        p, half, b, c = near_at(t)
        q = jnp.where(half == 0, s_base, r_base) + c
        ref = near.at[b, p, q]
        remote(ref, ref, in_send.at[t], in_recv.at[t], out_dev).wait_recv()
        send_inward(ref, p, half, b, c)

    def newest(u):
        far_work(u, w_pair, g_pair)

        @pl.when(u < n_near)
        def _():
            near_work(u, w_pair, g_pair)

    @pl.loop(0, steps)
    def _(t):
        has_pair = jnp.logical_and(jnp.logical_and(t >= nq, t <= 3 * nq), t != 2 * nq)
        turn = t - nq - (t > 2 * nq).astype(jnp.int32)

        @pl.when(has_pair)
        def _():
            i = turn
            pair_copy(i).wait_recv()
            send_inward(g_pair.at[pair_q(i)], 1, i // nq, edge, lax.rem(i, nq))

        @pl.when(t < n_far)
        def _():
            far_wait(t)

        if side_len > 1:
            @pl.when(t < n_near)
            def _():
                near_wait(t)

        @pl.when(t == catch_up - 1)
        def _():
            @pl.loop(0, n)
            def _(j):
                w_pair_copy(j).wait_recv()

            sibling_copy(pair_rows).start()

        @pl.when(t < 2 * nq)
        def _():
            contribute(w_own.at[2 * z + parity], g_own.at[t], g_own.at[t], t, 1.0)

        @pl.when(has_pair)
        def _():
            q = pair_q(turn)
            contribute(w_own.at[2 * z + 1 - parity], g_own.at[q], g_pair.at[q], q, 2.0)

        @pl.when(t < n_far)
        def _():
            far_work(t, w_own, g_own)

        if side_len > 1:
            @pl.when(t < n_near)
            def _():
                near_work(t, w_own, g_own)

        @pl.when(t == catch_up)
        def _():
            sibling_copy(pl.ds(pl.multiple_of((1 - core) * half_rows, 8), half_rows)).wait_recv()

        @pl.when(t >= catch_up)
        def _():
            first = (t - catch_up) * per_step
            last = jnp.minimum(first + per_step, steps)
            if spread:
                first = ((t - catch_up) * 2 * nq) // left
                last = ((t - catch_up + 1) * 2 * nq) // left

            @pl.loop(first, last)
            def _(u):
                @pl.when(u < 2 * nq)
                def _():
                    q = pair_q(u)
                    contribute(w_pair.at[2 * z + 1 - parity], g_pair.at[q], g_pair.at[q], q, 1.0)

                if spread:
                    far_work(lax.rem(u, side_len) * nq + u // side_len, w_pair, g_pair)
                else:
                    @pl.when(u < n_far)
                    def _():
                        far_work(u, w_pair, g_pair)

                if side_len > 1:
                    @pl.when(u < n_near)
                    def _():
                        near_work(u, w_pair, g_pair)

            if spread:
                newest(t - 1)

    if spread:
        newest(steps - 1)

    total = n * n_freq
    rank = me * n_freq + fq
    red[rank] = jnp.sum(acc[...], axis=1) / stations

    def share_copy(k, source):
        target = lax.rem(rank + k, total)
        return remote(
            red.at[source], red.at[source], red_send.at[k - 1], red_recv.at[k - 1],
            {"stn": target // n_freq, "freq": lax.rem(target, n_freq)},
        )

    @pl.loop(1, total)
    def _(k):
        share_copy(k, rank).start()

    @pl.loop(1, total)
    def _(k):
        share_copy(k, lax.rem(rank - k + total, total)).wait_recv()

    raw = red[0]
    for d in range(1, total):
        raw = raw + red[d]
    max_out[...] = jnp.broadcast_to(jnp.max(jnp.abs(raw)), max_out.shape)
    max_copy = remote(max_out, max_in, max_sem.at[0], max_sem.at[1], {"pts": 1 - core})
    max_copy.start()

    @pl.loop(1, total)
    def _(k):
        share_copy(k, rank).wait_send()

    @pl.loop(0, 2 * nq)
    def _(i):
        pair_copy(i).wait_send()

    @pl.loop(0, n)
    def _(j):
        w_pair_copy(j).wait_send()

    sibling_copy(pair_rows).wait_send()
    ref = far.at[0, 0, 0]

    @pl.loop(0, jnp.where(inner, n_far, (edge + 1) * 4 * nq))
    def _(t):
        remote(ref, ref, in_send.at[t], far_recv.at[0], in_dev).wait_send()

    @pl.when(edge > 0)
    def _():
        @pl.loop(0, n_far)
        def _(t):
            remote(ref, ref, out_send.at[t], far_recv.at[0], out_dev).wait_send()

    max_copy.wait()
    largest = jnp.maximum(max_out[0:1, 0:1], max_in[0:1, 0:1])
    out[...] = raw / (largest + 1e-6)


def kernel_body(n, n_freq, greens, weights):
    _, _, h, points = greens.shape
    stations = weights.shape[3]
    half = points // 2
    chunk = LANES
    while chunk * 2 * h <= 32768 and half % (chunk * 2) == 0:
        chunk *= 2
    nq = half // chunk
    side_len = n // 4
    n_far = side_len * 2 * nq
    n_near = max(side_len - 1, 1) * 4 * nq
    blocked = h % LANES != 0
    if blocked:
        weights = weights.reshape(2, weights.shape[1], h, n, h).swapaxes(2, 3)
    if side_len == 2 and nq >= 8 and nq % 2 == 0:
        return line_body(n_freq, chunk, nq, blocked, greens, weights)
    dma = pltpu.SemaphoreType.DMA
    bf16, f32 = jnp.bfloat16, jnp.float32
    rows = points // LANES
    out = pl.pallas_call(
        functools.partial(ring_kernel, n, n_freq, h, stations, chunk, nq, blocked),
        out_shape=jax.ShapeDtypeStruct((rows, LANES), f32),
        in_specs=[pl.BlockSpec(memory_space=pl.ANY)] * 2,
        out_specs=pl.BlockSpec(memory_space=pltpu.VMEM),
        scratch_shapes=[
            pltpu.VMEM((2 * nq, 2, h, chunk), bf16),
            pltpu.VMEM((2 * nq, 2, h, chunk), bf16),
            pltpu.VMEM((max(side_len - 1, 1), 2, 2 * nq, 2, h, chunk), bf16),
            pltpu.VMEM((side_len, 2, nq, 2, h, chunk), bf16),
            pltpu.VMEM((n, 2, h, h), bf16),
            pltpu.VMEM((n, 2, h, h), bf16),
            pltpu.VMEM((rows, 8, LANES), f32),
            pltpu.VMEM((n * n_freq, rows, LANES), f32),
            pltpu.VMEM((8, LANES), f32),
            pltpu.VMEM((8, LANES), f32),
            dma((2 * nq,)), dma((n,)), dma((2 * nq,)), dma((2 * nq,)), dma((n,)), dma((n,)), dma((2,)),
            dma((max(n_near, n_far),)), dma((n_near,)), dma((n_far,)), dma((n_far,)),
            dma((n * n_freq - 1,)), dma((n * n_freq - 1,)), dma((2,)),
            pltpu.SemaphoreType.REGULAR((2, n // 2 - 1)), pltpu.SemaphoreType.REGULAR((2,)),
        ],
        compiler_params=pltpu.CompilerParams(
            collective_id=0, has_side_effects=True, vmem_limit_bytes=60 * 1024 * 1024
        ),
    )(greens, weights)
    return out.reshape(points)


FAR_FIRST = (11, 9, 10, 8, 15, 7, 13, 14, 5, 6, 12, 4, 3, 1, 2, 0)


def line_kernel(
    n_freq, h, stations, chunk, nq, kept, late, blocked,
    greens, weights, out,
    g_own, g_pair, near, far, w_own, w_pair, w_edge, folded, lent, acc, part, side, sums, extras,
    own_sem, w_own_sem, pair_send, pair_recv, wp_send, wp_recv, sib_sem, we_send, we_recv, we_sib,
    in_send, near_recv, far_recv, down_send, back_send, part_send, part_recv, side_sem,
    extra_send, extra_recv, base_sem, fold_sem, lend_sem, reply_sem, hello_sem, pair_hello,
):
    n = 8
    sub = chunk // LANES
    half_rows = h // 2
    steps = 4 * nq
    me = lax.axis_index("stn")
    core = lax.axis_index("pts")
    fq = lax.axis_index("freq")
    parity = lax.rem(me, 2)
    z = me // 2
    hi = z // 2
    inner = jnp.logical_or(z == 1, z == 2)
    outer = jnp.logical_not(inner)
    s_base = hi * nq
    r_base = (1 - hi) * nq
    rank = me * n_freq + fq
    total = n * n_freq
    inward = jnp.where(hi == 1, -2, 2)
    pair_dev = {"stn": me + 1 - 2 * parity}
    in_dev = {"stn": me + inward}
    out_dev = {"stn": me - inward}
    core_dev = {"pts": 1 - core}
    freq_dev = {"freq": n_freq - 1 - fq}
    across_dev = {"stn": 2 * (3 - z) + parity}
    other_inner = 2 - hi
    other_edge = 3 - 3 * hi
    near_z = jnp.where(inner, z - inward // 2, z + inward // 2)

    def columns(q):
        return pl.ds(pl.multiple_of(q * chunk, LANES), chunk)

    def w_src(freq, j, rows):
        if blocked:
            return weights.at[:, freq, j, rows, :]
        return weights.at[:, freq, rows, pl.ds(pl.multiple_of(j * h, LANES), h)]

    def block_of(where, p):
        return 2 * where + jnp.where(p == 0, parity, 1 - parity)

    def far_block(e):
        return block_of(jnp.where(lax.rem(e, 2) == 0, other_inner, other_edge), e // 2)

    def position(e, c):
        late_c = c >= jnp.where(e < 2, nq - 1, kept)
        pair_half = jnp.where(e == 2, 2 * nq, 2 * nq + kept) + c
        pair_late = jnp.where(e == 2, 2 * nq + kept, 3 * nq) + c
        early = jnp.where(late_c, 2 * nq - 2 + e, e * (nq - 1) + c)
        return jnp.where(e < 2, early, jnp.where(late_c, pair_late, pair_half))

    def block_at(t):
        e = (t >= nq - 1).astype(jnp.int32)
        c = t - e * (nq - 1)
        corner = t >= 2 * nq - 2
        e = jnp.where(corner, t - (2 * nq - 2), e)
        c = jnp.where(corner, nq - 1, c)
        pairs = t - 2 * nq
        third = jnp.logical_and(pairs >= kept, pairs < 2 * kept)
        third = jnp.logical_or(third, pairs >= nq + kept)
        pair_c = jnp.where(pairs < kept, pairs, jnp.where(pairs < nq + kept, pairs - kept, pairs - nq))
        e = jnp.where(pairs >= 0, 2 + third.astype(jnp.int32), e)
        c = jnp.where(pairs >= 0, pair_c, c)
        return e, c

    every_row = pl.ds(0, h)
    my_rows = pl.ds(pl.multiple_of(core * half_rows, 8), half_rows)
    sib_rows = pl.ds(pl.multiple_of((1 - core) * half_rows, 8), half_rows)

    def pair_q(i):
        return jnp.where(i < nq, s_base + i, r_base + i - nq)

    def g_src(q):
        return greens.at[:, parity, :, columns(q)]

    def own_copy(q):
        return pltpu.make_async_copy(g_src(q), g_own.at[q], own_sem.at[0])

    def w_own_copy(j):
        return pltpu.make_async_copy(w_src(parity, j, every_row), w_own.at[j], w_own_sem.at[0])

    def pair_copy(i):
        q = pair_q(i)
        return remote(
            greens.at[:, 1 - parity, :, columns(q)], g_pair.at[q],
            pair_send.at[0], pair_recv.at[i // 2], pair_dev,
        )

    def w_pair_copy(j):
        return remote(
            w_src(1 - parity, j, my_rows), w_pair.at[j, :, my_rows, :],
            wp_send.at[0], wp_recv.at[0], pair_dev,
        )

    def sibling_copy(rows):
        part_of_w = w_pair.at[:, :, rows, :]
        return remote(part_of_w, part_of_w, sib_sem.at[0], sib_sem.at[1], core_dev)

    def edge_sibling_copy(rows):
        part_of_w = w_edge.at[:, :, :, rows, :]
        return remote(part_of_w, part_of_w, we_sib.at[0], we_sib.at[1], core_dev)

    first_groups = nq // 2 + (nq - kept + 1) // 2
    back_group = first_groups + nq // 2 + nq - kept
    singles = 2 * nq + 2 * kept

    def near_slot(p, i):
        m = i - nq - kept
        return p * first_groups + jnp.where(i < nq, i // 2, nq // 2 + jnp.where(p == 0, m // 2, m))

    def far_slot(slot):
        return jnp.where(slot < singles, slot // 2, slot - singles // 2)

    def whole(ref, send_sem, recv_sem):
        return remote(ref, ref, send_sem.at[0], recv_sem.at[0], pair_dev)

    def up_copy(src, p, i):
        return remote(src, near.at[p, pair_q(i)], in_send.at[0], near_recv.at[near_slot(p, i)], in_dev)

    def up_weights(src, b, p):
        return remote(src, w_edge.at[b, p, :, my_rows, :], we_send.at[0], we_recv.at[0], in_dev)

    def mid_copy(src, slot):
        return remote(src, far.at[slot], in_send.at[0], far_recv.at[far_slot(slot)], in_dev)

    def lend_copy():
        src = near.at[1, pair_q(nq - 1)]
        return remote(src, lent, lend_sem.at[0], lend_sem.at[1], core_dev)

    corner = 2 * nq - 2

    def down_copy(slot):
        return remote(far.at[slot], far.at[slot], down_send.at[0], far_recv.at[far_slot(slot)], out_dev)

    def back_copy(src, p, c):
        return remote(
            src, near.at[p, r_base + c], back_send.at[0], near_recv.at[back_group + p], out_dev,
        )

    barrier = pltpu.get_barrier_semaphore()
    up, down = z < 3, z > 0
    greeted = [pair_dev, core_dev, freq_dev]

    def greet(sem, device):
        pl.semaphore_signal(sem, inc=1, device_id=device, device_id_type=MESH)

    def along_z(sem_down, sem_up):
        @pl.when(up)
        def _():
            greet(sem_up, {"stn": me + 2})

        @pl.when(down)
        def _():
            greet(sem_down, {"stn": me - 2})

    @pl.when(inner)
    def _():
        greet(barrier, in_dev)
        greet(barrier, out_dev)

    for device in greeted:
        greet(barrier, device)
    pl.semaphore_wait(barrier, len(greeted) + 1)

    @pl.when(outer)
    def _():
        greet(reply_sem.at[0], in_dev)

    @pl.loop(0, nq)
    def _(i):
        src = g_src(pair_q(i))

        @pl.when(jnp.logical_and(inner, i < nq - 1))
        def _():
            mid_copy(src, i).start()

        @pl.when(outer)
        def _():
            up_copy(src, 0, i).start()

    corner_src = g_src(pair_q(nq - 1))

    @pl.loop(0, n)
    def _(j):
        w_pair_copy(j).start()
        w_own_copy(j).start()

    @pl.loop(0, 2 * nq)
    def _(i):
        own_copy(pair_q(i)).start()
        pair_copy(i).start()

    @pl.when(inner)
    def _():
        pl.semaphore_wait(reply_sem.at[0], 1)

        @pl.loop(0, kept)
        def _(c):
            back_copy(g_src(pair_q(nq + c)), 0, c).start()

    @pl.when(outer)
    def _():
        for b in range(2):
            up_weights(w_src(parity, far_block(2 + b), my_rows), b, 0).start()

    @pl.loop(0, 2)
    def _(r):
        along_z(hello_sem.at[0], hello_sem.at[1])

        @pl.when(up)
        def _():
            pl.semaphore_wait(hello_sem.at[0], 1)

        @pl.when(down)
        def _():
            pl.semaphore_wait(hello_sem.at[1], 1)

    for i, device in enumerate((pair_dev, freq_dev, core_dev)):
        greet(pair_hello.at[i], device)
        pl.semaphore_wait(pair_hello.at[i], 1)

    acc[...] = jnp.zeros_like(acc)

    pltpu.make_async_copy(g_own, g_own, own_sem.at[0]).wait()
    pltpu.make_async_copy(w_own, w_own, w_own_sem.at[0]).wait()

    def product(w, gi, gj, s):
        lanes = slice(s * LANES, (s + 1) * LANES)
        both = jnp.concatenate([gj[0, :, lanes], gj[1, :, lanes]], axis=1)
        ab = jnp.dot(w[...].reshape(2 * h, h), both, preferred_element_type=jnp.float32)
        a, b = ab[:h], ab[h:]
        t = gi[0, :, lanes].astype(jnp.float32) * (a[:, :LANES] - b[:, LANES:])
        t = t + gi[1, :, lanes].astype(jnp.float32) * (a[:, LANES:] + b[:, :LANES])
        return jnp.sum(t.reshape(h // 8, 8, LANES), axis=0)

    def contribute(w, gi, gj, q, weight):
        for s in range(sub):
            acc[q * sub + s] += product(w, gi, gj, s) * weight

    own_pair_block = block_of(z, 1)

    def own_work(q):
        contribute(w_own.at[me], g_own.at[q], g_own.at[q], q, 1.0)

    def cross_work(q):
        contribute(w_own.at[own_pair_block], g_own.at[q], g_pair.at[q], q, 2.0)

    def pair_work(q):
        contribute(w_pair.at[own_pair_block], g_pair.at[q], g_pair.at[q], q, 1.0)

    def far_work(e, c, w, g):
        q = r_base + c
        contribute(w.at[far_block(e)], g.at[q], far.at[position(e, c)], q, 2.0)

    def near_work(p, q, w, g):
        contribute(w.at[block_of(near_z, p)], g.at[q], near.at[p, q], q, 2.0)

    def edge_work(b, c):
        q = r_base + c

        @pl.loop(0, 2)
        def _(p):
            contribute(w_edge.at[b, p], near.at[p, q], far.at[position(2 + b, c)], q, 2.0)

    def transposed(w, g):
        return lax.dot_general(w, g, (((0,), (0,)), ((), ())), preferred_element_type=jnp.float32)

    def fold(w, gi, s):
        lanes = slice(s * LANES, (s + 1) * LANES)
        both = jnp.concatenate([gi[0, :, lanes], gi[1, :, lanes]], axis=1)
        a, b = transposed(w[0], both), transposed(w[1], both)
        return a[:, :LANES] + b[:, LANES:], a[:, LANES:] - b[:, :LANES]

    def fold_last():
        q, j = r_base + nq - 1, far_block(3)
        for s in range(sub):
            lanes = slice(s * LANES, (s + 1) * LANES)
            re, im = fold(w_own.at[j], g_own.at[q], s)
            folded[core, 0, :, lanes] = re
            folded[core, 1, :, lanes] = im
            for w, g in ((w_pair.at[j], g_pair.at[q]), (w_edge.at[1, 0], near.at[0, q]), (w_edge.at[1, 1], near.at[1, q])):
                re, im = fold(w, g, s)
                folded[core, 0, :, lanes] += re
                folded[core, 1, :, lanes] += im

        @pl.when(core == 0)
        def _():
            fold_copy().start()

    def fold_copy():
        return remote(folded.at[0], folded.at[0], fold_sem.at[0], fold_sem.at[1], core_dev)

    def unfold(which, slot, s):
        lanes = slice(s * LANES, (s + 1) * LANES)
        t = far[slot, 0, :, lanes].astype(jnp.float32) * folded[which, 0, :, lanes]
        t = t + far[slot, 1, :, lanes].astype(jnp.float32) * folded[which, 1, :, lanes]
        return 2.0 * jnp.sum(t.reshape(h // 8, 8, LANES), axis=0)

    def passed_down(t):
        return t < 2 * nq + 2 * kept

    def wait_blocks(count, recv_sem):
        ref = far.at[pl.ds(0, count)]
        remote(ref, ref, in_send.at[0], recv_sem, in_dev).wait_recv()

    def wait_far(t):
        @pl.when(jnp.logical_and(t < singles, lax.rem(t, 2) == 0))
        def _():
            wait_blocks(2, far_recv.at[t // 2])

        @pl.when(t >= singles)
        def _():
            wait_blocks(1, far_recv.at[t - singles // 2])

    def wait_pair(i):
        @pl.when(lax.rem(i, 2) == 0)
        def _():
            wait_blocks(2, pair_recv.at[i // 2])

    def wait_near(p, i):
        m = jnp.where(i < nq, i, i - nq - kept)
        even = lax.rem(m, 2) == 0
        alone = jnp.logical_and(i >= nq, p == 1)
        two = even & jnp.logical_not(alone) & (i < 2 * nq - 1)
        lone = jnp.logical_or(alone, even & (i == 2 * nq - 1))

        @pl.when(two)
        def _():
            wait_blocks(2, near_recv.at[near_slot(p, i)])

        @pl.when(lone)
        def _():
            wait_blocks(1, near_recv.at[near_slot(p, i)])

    def wait_back(p):
        wait_blocks(kept, near_recv.at[back_group + p])

    def wait_w_pair():
        whole(w_pair.at[:, :, my_rows, :], wp_send, wp_recv).wait_recv()
        sibling_copy(my_rows).start()

    def share_part():
        part[rank] = jnp.sum(acc[...], axis=1) / stations

        @pl.loop(0, total // 2 - 1)
        def _(k):
            part_copy(total // 2 - 1 - k, rank).start()

    def at_rank(target):
        return {"stn": target // n_freq, "freq": lax.rem(target, n_freq)}

    def flipped(k):
        bit, flip = total // 2, jnp.int32(0)
        while bit:
            mine = lax.rem(rank // bit, 2)
            turn = lax.rem(k // bit, 2)
            flip = flip + bit * (mine + turn - 2 * mine * turn)
            bit //= 2
        return flip

    def part_copy(k, source):
        ref = part.at[source]
        return remote(ref, ref, part_send.at[0], part_recv.at[0], at_rank(flipped(k)))

    my_group = (hi * 2 + parity) * n_freq + fq
    late_rows = late * sub

    sends = [(k, other) for k in FAR_FIRST for other in range(2) if k or other]

    def extra_copy(k, other):
        def turned(v, bit):
            return 1 - v if k & bit else v

        message = extras.at[core * 4 * n_freq + my_group]
        target_z = 2 * turned(hi, 8) + turned(lax.rem(z, 2), 4)
        target = {
            "stn": 2 * target_z + turned(parity, 2), "freq": turned(fq, 1),
            "pts": 1 - core if other else core,
        }
        return remote(
            message, message, extra_send.at[other], extra_recv.at[core], target,
        )

    def late_row(t):
        return jnp.sum(t, axis=0, keepdims=True) / stations

    def finish():
        first = (r_base + nq - late) * sub
        for c in range(late_rows):
            extras[core * 4 * n_freq + my_group, c] = late_row(acc[first + c])
        for s in range(sub):
            extras[core * 4 * n_freq + my_group, late_rows + s] = jnp.zeros((1, LANES), jnp.float32)

        @pl.when(core == 1)
        def _():
            fold_copy().wait_recv()
            wait_blocks(1, far_recv.at[steps - singles // 2])
            wait_blocks(1, far_recv.at[steps - 1 - singles // 2])
            for s in range(sub):
                c = late_rows - sub + s
                extras[4 * n_freq + my_group, c] = late_row(acc[first + c] + unfold(1, steps - 1, s))
                extras[4 * n_freq + my_group, late_rows + s] = late_row(unfold(0, steps, s))

        for k, other in sends:
            extra_copy(k, other).start()

    near_second = nq + 4
    near_third = near_second + nq
    near_fourth = near_third + nq - kept
    near_end = near_fourth + nq - kept

    def near_at(t):
        i = jnp.where(t >= near_second, t - near_second, t)
        i = jnp.where(t >= near_third, t - near_third + nq + kept, i)
        i = jnp.where(t >= near_fourth, t - near_fourth + nq + kept, i)
        second = jnp.logical_and(t >= near_second, t < near_third)
        p = jnp.logical_or(second, t >= near_fourth).astype(jnp.int32)
        present = jnp.logical_or(t < nq, jnp.logical_and(t >= near_second, t < near_end))
        return present, p, i

    @pl.when(inner)
    def _():
        @pl.loop(0, steps - 1)
        def _(t):
            has_near, p, i = near_at(t)
            has_pair = jnp.logical_and(t >= nq, t < 3 * nq)
            turn = t - nq
            wait_far(t)

            @pl.when(passed_down(t))
            def _():
                down_copy(t).start()

            @pl.when(has_near)
            def _():
                wait_near(p, i)

            @pl.when(t < nq)
            def _():
                mid_copy(near.at[0, pair_q(t)], position(1, t)).start()

            @pl.when(t == nq - 2)
            def _():
                mid_copy(corner_src, corner).start()

            @pl.when(t == nq)
            def _():
                wait_w_pair()

            @pl.when(has_pair)
            def _():
                wait_pair(turn)

                @pl.when(turn < kept)
                def _():
                    mid_copy(g_pair.at[pair_q(turn)], 2 * nq + turn).start()

                @pl.when(jnp.logical_and(turn >= nq, turn < nq + kept))
                def _():
                    back_copy(g_pair.at[pair_q(turn)], 1, turn - nq).start()

            third = t - near_second
            fourth = third - (nq - kept)

            @pl.when(jnp.logical_and(third >= 0, third < kept))
            def _():
                mid_copy(near.at[1, pair_q(third)], 2 * nq + kept + third).start()

            send_third = jnp.logical_and(third >= kept, third < nq)

            @pl.when(send_third)
            def _():
                mid_copy(g_pair.at[pair_q(third)], 2 * nq + kept + third).start()

            @pl.when(jnp.logical_and(third == nq - 1, core == 0))
            def _():
                lend_copy().start()

            @pl.when(jnp.logical_and(fourth >= kept, fourth < nq - 1 + core))
            def _():
                mid_copy(near.at[1, pair_q(fourth)], 3 * nq + fourth).start()

            @pl.when(jnp.logical_and(fourth == nq - 1, core == 1))
            def _():
                lend_copy().wait_recv()
                mid_copy(lent, steps).start()

            @pl.when(t == nq + 2)
            def _():
                sibling_copy(sib_rows).wait_recv()

            @pl.when(t == near_second)
            def _():
                whole(w_edge.at[:, :, :, my_rows, :], we_send, we_recv).wait_recv()
                edge_sibling_copy(my_rows).start()

            @pl.when(t == near_second + 2)
            def _():
                edge_sibling_copy(sib_rows).wait_recv()

            e, c = block_at(t)
            far_work(e, c, w_own, g_own)

            @pl.when(t < 2 * nq)
            def _():
                own_work(t)

            @pl.when(has_near)
            def _():
                q = pair_q(i)
                near_work(p, q, w_own, g_own)

                @pl.when(t >= nq)
                def _():
                    near_work(p, q, w_pair, g_pair)

                @pl.when(t >= near_fourth)
                def _():
                    edge_work(0, i - nq)

            @pl.when(has_pair)
            def _():
                cross_work(pair_q(turn))

            lag = t - nq - 2

            @pl.when(jnp.logical_and(lag >= 0, lag < 2 * nq))
            def _():
                pair_work(pair_q(lag))

                @pl.when(lag < nq)
                def _():
                    near_work(0, pair_q(lag), w_pair, g_pair)

            @pl.when(t >= 2 * nq)
            def _():
                far_work(e, c, w_pair, g_pair)

                @pl.when(t < 3 * nq)
                def _():
                    @pl.loop(0, 2)
                    def _(first):
                        far_work(first, t - 2 * nq, w_pair, g_pair)

            @pl.when(t >= 3 * nq + kept)
            def _():
                edge_work(1, t - 3 * nq)

            @pl.when(t == steps - late - 1)
            def _():
                share_part()

                @pl.loop((nq - late) * sub, nq * sub)
                def _(c):
                    acc[r_base * sub + c] = jnp.zeros((8, LANES), jnp.float32)

            @pl.when(t == near_end - 1)
            def _():
                fold_last()

        finish()

    @pl.when(outer)
    def _():
        @pl.loop(0, 3 * nq)
        def _(t):
            turn = t - nq + 2
            has_pair = jnp.logical_and(turn >= 0, turn < 2 * nq)
            back = t - 2 * nq - 4
            has_back = jnp.logical_and(back >= 0, back < kept)
            e, c = block_at(t)
            has_far = t < 2 * nq + 2 * kept

            @pl.when(turn == 0)
            def _():
                wait_w_pair()
                for b in range(2):
                    up_weights(w_pair.at[far_block(2 + b), :, my_rows, :], b, 1).start()

            @pl.when(has_pair)
            def _():
                wait_pair(turn)

                @pl.when(jnp.logical_or(turn < nq, turn >= nq + kept))
                def _():
                    up_copy(g_pair.at[pair_q(turn)], 1, turn).start()

                @pl.when(turn == nq - 1)
                def _():
                    @pl.loop(nq + kept, 2 * nq)
                    def _(i):
                        up_copy(g_src(pair_q(i)), 0, i).start()

            @pl.when(t == nq)
            def _():
                sibling_copy(sib_rows).wait_recv()

            @pl.when(t == 0)
            def _():
                wait_back(0)

            @pl.when(back == 0)
            def _():
                wait_back(1)

            @pl.when(has_far)
            def _():
                wait_far(t)
                far_work(e, c, w_own, g_own)

            @pl.when(jnp.logical_and(has_far, t >= 2 * nq))
            def _():
                far_work(e, c, w_pair, g_pair)

            @pl.when(t < 2 * nq)
            def _():
                own_work(t)

            @pl.when(t < kept)
            def _():
                near_work(0, r_base + t, w_own, g_own)

            @pl.when(has_back)
            def _():
                q = r_base + back
                near_work(0, q, w_pair, g_pair)
                near_work(1, q, w_own, g_own)
                near_work(1, q, w_pair, g_pair)

            @pl.when(has_pair)
            def _():
                cross_work(pair_q(turn))

            @pl.when(t >= nq)
            def _():
                pair_work(pair_q(t - nq))

            @pl.when(t >= 2 * nq)
            def _():
                @pl.loop(0, 2)
                def _(first):
                    far_work(first, t - 2 * nq, w_pair, g_pair)

        share_part()

    parts = part.at[pl.ds(0, total // 2 - 1)]
    whole(parts, part_send, part_recv).wait_recv()

    base = hi * (total // 2)
    mine = part[base]
    for d in range(1, total // 2):
        mine = mine + part[base + d]
    side[hi] = mine

    def side_copy(which):
        ref = side.at[which]
        return remote(ref, ref, side_sem.at[0], side_sem.at[1], across_dev)

    side_copy(hi).start()
    side_copy(1 - hi).wait_recv()
    sums[core] = side[0] + side[1]
    base_copy = remote(sums.at[core], sums.at[core], base_sem.at[0], base_sem.at[1], core_dev)
    base_copy.start()

    whole(g_pair, pair_send, pair_recv).wait_send()
    whole(w_pair.at[:, :, my_rows, :], wp_send, wp_recv).wait_send()
    sibling_copy(my_rows).wait_send()
    whole(parts, part_send, part_recv).wait_send()

    def sent(count, send_sem):
        whole(far.at[pl.ds(0, count)], send_sem, far_recv).wait_send()

    @pl.when(inner)
    def _():
        sent(2 * nq + 2 * kept, down_send)
        sent(2 * kept, back_send)
        edge_sibling_copy(my_rows).wait_send()
        for other in range(2):
            ref = extras.at[pl.ds(0, total - 1 + other)]
            remote(ref, ref, extra_send.at[other], extra_recv.at[0], core_dev).wait_send()

        @pl.when(core == 0)
        def _():
            sent(steps - 1, in_send)
            fold_copy().wait_send()
            lend_copy().wait_send()

        @pl.when(core == 1)
        def _():
            sent(steps + 1, in_send)

    @pl.when(outer)
    def _():
        sent(steps - 2 * kept, in_send)
        whole(w_edge.at[:, :, :, my_rows, :], we_send, we_recv).wait_send()

    side_copy(hi).wait_send()

    def wait_extras(which, groups):
        ref = extras.at[pl.ds(which * 4 * n_freq, groups)]
        remote(ref, ref, extra_send.at[0], extra_recv.at[which], core_dev).wait_recv()

    @pl.when(inner)
    def _():
        wait_extras(core, 4 * n_freq - 1)
        wait_extras(1 - core, 4 * n_freq)

    @pl.when(outer)
    def _():
        wait_extras(0, 4 * n_freq)
        wait_extras(1, 4 * n_freq)

    base_copy.wait_send()
    sum_ref = sums.at[1 - core]
    remote(sum_ref, sum_ref, base_sem.at[0], base_sem.at[1], core_dev).wait_recv()

    def late_sum(which, low, c):
        first = (2 * which + low) * 2 * n_freq
        row = extras[first, c]
        for g in range(1, 2 * n_freq):
            row = row + extras[first + g, c]
        return row

    for which in range(2):
        for low in range(2):
            gathered = [late_sum(which, low, c) for c in range(late_rows)]
            if which == 0:
                for s in range(sub):
                    gathered[late_rows - sub + s] += late_sum(1, low, late_rows + s)
            at = ((1 - low) * nq + nq - late) * sub
            sums[which, at:at + late_rows, :] += jnp.concatenate(gathered, axis=0)

    largest = jnp.max(jnp.maximum(jnp.abs(sums[0]), jnp.abs(sums[1])), keepdims=True)
    out[...] = sums[core] / (largest + 1e-6)


def line_body(n_freq, chunk, nq, blocked, greens, weights):
    _, _, h, points = greens.shape
    n = 8
    kept, late = 3 * nq // 8, 3
    stations = n * h
    dma = pltpu.SemaphoreType.DMA
    one, two = dma((1,)), dma((2,))
    near_groups = nq + (nq - kept + 1) // 2 + nq - kept + 2
    regular = pltpu.SemaphoreType.REGULAR
    bf16, f32 = jnp.bfloat16, jnp.float32
    rows = points // LANES
    late_rows = late * (chunk // LANES)
    total = n * n_freq
    out = pl.pallas_call(
        functools.partial(line_kernel, n_freq, h, stations, chunk, nq, kept, late, blocked),
        out_shape=pltpu.VMEM((rows, LANES), f32),
        in_specs=[pl.BlockSpec(memory_space=pl.ANY)] * 2,
        out_specs=pl.BlockSpec(memory_space=pltpu.VMEM),
        scratch_shapes=[
            pltpu.VMEM((2 * nq, 2, h, chunk), bf16),
            pltpu.VMEM((2 * nq, 2, h, chunk), bf16),
            pltpu.VMEM((2, 2 * nq, 2, h, chunk), bf16),
            pltpu.VMEM((4 * nq + 1, 2, h, chunk), bf16),
            pltpu.VMEM((n, 2, h, h), bf16),
            pltpu.VMEM((n, 2, h, h), bf16),
            pltpu.VMEM((2, 2, 2, h, h), bf16),
            pltpu.VMEM((2, 2, h, chunk), f32),
            pltpu.VMEM((2, h, chunk), bf16),
            pltpu.VMEM((rows, 8, LANES), f32),
            pltpu.VMEM((total, rows, LANES), f32),
            pltpu.VMEM((2, rows, LANES), f32),
            pltpu.VMEM((2, rows, LANES), f32),
            pltpu.VMEM((8 * n_freq, late_rows + chunk // LANES, 1, LANES), f32),
            one, one, one, dma((nq,)), one, one, two,
            one, one, two,
            one, dma((near_groups,)), dma((3 * nq + 1 - kept,)), one, one,
            one, one, two,
            two, two, two, two, two,
            regular((1,)), regular((2,)), regular((3,)),
        ],
        compiler_params=pltpu.CompilerParams(
            collective_id=0, has_side_effects=True, vmem_limit_bytes=60 * 1024 * 1024
        ),
    )(greens, weights)
    return out.reshape(points)


def passed_along(x, axis, by):
    size = lax.axis_size(axis)
    return lax.ppermute(x, axis, [(i, (i + by) % size) for i in range(size)])


def mixing_of(weights):
    negated = -weights[1]
    return jnp.stack([jnp.stack([weights[0], negated]), jnp.stack([weights[1], weights[0]])])


def body(greens, noise_weights):
    station_rows = greens.shape[2]
    stations = noise_weights.shape[3]
    device_index = lax.axis_index("stn")
    cycle_length = lax.axis_size("stn")
    mixing = mixing_of(noise_weights)

    def block_product(columns_start, arriving):
        block_rows = arriving.shape[2]
        weights_block = lax.dynamic_slice_in_dim(mixing, columns_start, block_rows, 4)
        return jnp.einsum(
            "ocfin,cfnx->ofix", weights_block, arriving, preferred_element_type=jnp.float32
        )

    half_way = cycle_length // 2
    diagonal = block_product(device_index * station_rows, greens)

    def advance(offset, loop_state):
        running, current = loop_state
        current = passed_along(current, "stn", -1)
        source = (device_index + offset) % cycle_length
        weight = jnp.where(offset == half_way, 1.0, 2.0).astype(jnp.float32)
        running = running + weight * block_product(source * station_rows, current)
        return (running, current)

    summed, current = lax.fori_loop(1, half_way + 1, advance, (diagonal, greens))
    green_real = greens[0].astype(jnp.float32)
    green_imag = greens[1].astype(jnp.float32)
    partial_kernel = (
        jnp.sum(green_real * summed[0] + green_imag * summed[1], axis=(0, 1)) / stations
    )
    raw_kernel = lax.psum(partial_kernel, "stn")
    raw_kernel = lax.psum(raw_kernel, "freq")
    largest = lax.pmax(jnp.max(jnp.abs(raw_kernel)), "pts")
    return raw_kernel / (largest + 1e-06)


def solution(mesh):
    n, cores, n_freq = mesh.shape["stn"], mesh.shape["pts"], mesh.shape["freq"]

    def either(greens, noise_weights):
        _, freqs, rows, points = greens.shape
        fits = n % 4 == 0 and cores == 2 and freqs == 2 and n_freq == 2 and rows % 32 == 0 and points % (2 * LANES) == 0
        if fits:
            return kernel_body(n, n_freq, greens, noise_weights)
        return body(greens, noise_weights)

    in_specs = (P(None, "freq", "stn", "pts"), P(None, "freq", "stn", None))
    return jax.shard_map(either, mesh=mesh, in_specs=in_specs, out_specs=P("pts"), check_vma=False)
```

```python
import functools

import jax
import jax.numpy as jnp
from jax import lax
from jax.experimental import pallas as pl
from jax.experimental.pallas import tpu as pltpu
from jax.sharding import PartitionSpec as P

MESH = pl.DeviceIdType.MESH
LANES = 128


def remote(src, dst, send_sem, recv_sem, target):
    return pltpu.make_async_remote_copy(
        src_ref=src, dst_ref=dst, send_sem=send_sem, recv_sem=recv_sem,
        device_id=target, device_id_type=MESH,
    )


def ring_kernel(
    n, n_freq, h, stations, chunk, nq, blocked,
    greens, weights, out,
    g_own, g_pair, near, far, w_own, w_pair, acc, red, max_out, max_in,
    own_sem, w_own_sem, pair_send, pair_recv, wp_send, wp_recv, sib_sem,
    in_send, in_recv, out_send, far_recv, red_send, red_recv, max_sem, hello_sem, pair_hello,
):
    m = n // 2
    side_len = m // 2
    sub = chunk // LANES
    half_rows = h // 2
    me = lax.axis_index("stn")
    core = lax.axis_index("pts")
    fq = lax.axis_index("freq")
    parity = lax.rem(me, 2)
    z = me // 2
    hi = (z >= side_len).astype(jnp.int32)
    edge = jnp.where(hi == 1, m - 1 - z, z)
    inward = jnp.where(hi == 1, -2, 2)
    inner = edge == side_len - 1
    s_base = hi * nq
    r_base = (1 - hi) * nq
    pair_dev = {"stn": me + 1 - 2 * parity}
    in_dev = {"stn": me + inward}
    out_dev = {"stn": me - inward}
    n_far = side_len * 2 * nq
    n_near = edge * 4 * nq
    n_near_max = (side_len - 1) * 4 * nq
    steps = max(n_far, n_near_max, 3 * nq + 2)
    spread = side_len == 2
    catch_up = 2 * nq + 1 if spread else max((steps * 25) // 32, 3 * nq + 1)
    left = steps - catch_up
    per_step = -(-steps // (steps - catch_up))

    def columns(q):
        return pl.ds(pl.multiple_of(q * chunk, LANES), chunk)

    def w_src(freq, j, rows):
        if blocked:
            return weights.at[:, freq, j, rows, :]
        return weights.at[:, freq, rows, pl.ds(pl.multiple_of(j * h, LANES), h)]

    def global_block(e, opposite):
        low = jnp.where(opposite, 1 - hi, hi) == 0
        return jnp.where(low, e, m - 1 - e)

    def near_slot(receiver_edge, p, half, b, c):
        return ((p * 2 + half) * receiver_edge + (receiver_edge - 1 - b)) * nq + c

    def far_slot(p, b, c):
        return (p * side_len + (side_len - 1 - b)) * nq + c

    def send_inward(src, p, half, b, c):
        q = jnp.where(half == 0, s_base, r_base) + c

        if side_len > 1:
            @pl.when(jnp.logical_not(inner))
            def _():
                slot = near_slot(edge + 1, p, half, b, c)
                remote(src, near.at[b, p, q], in_send.at[slot], in_recv.at[slot], in_dev).start()

        @pl.when(jnp.logical_and(inner, half == 0))
        def _():
            slot = far_slot(p, b, c)
            remote(src, far.at[b, p, c], in_send.at[slot], far_recv.at[slot], in_dev).start()

    freq_dev = {"freq": n_freq - 1 - fq}
    barrier = pltpu.get_barrier_semaphore()
    up, down = z < m - 1, z > 0
    greeted = [pair_dev, {"pts": 1 - core}, freq_dev]

    def greet(sem, device):
        pl.semaphore_signal(sem, inc=1, device_id=device, device_id_type=MESH)

    def along_z(sem_down, sem_up):
        @pl.when(up)
        def _():
            greet(sem_up, {"stn": me + 2})

        @pl.when(down)
        def _():
            greet(sem_down, {"stn": me - 2})

    for device in greeted:
        greet(barrier, device)
    along_z(barrier, barrier)
    pl.semaphore_wait(barrier, len(greeted) + up.astype(jnp.int32) + down.astype(jnp.int32))

    def hello():
        @pl.loop(0, m - 1)
        def _(r):
            along_z(hello_sem.at[0, r], hello_sem.at[1, r])

            @pl.when(up)
            def _():
                pl.semaphore_wait(hello_sem.at[0, r], 1)

            @pl.when(down)
            def _():
                pl.semaphore_wait(hello_sem.at[1, r], 1)

        for i, device in enumerate((pair_dev, freq_dev)):
            greet(pair_hello.at[i], device)
            pl.semaphore_wait(pair_hello.at[i], 1)

    every_row = pl.ds(0, h)
    pair_rows = pl.ds(pl.multiple_of(core * half_rows, 8), half_rows)

    def pair_q(i):
        return jnp.where(i < nq, s_base + i, r_base + i - nq)

    def pair_copy(i):
        q = pair_q(i)
        return remote(
            greens.at[:, 1 - parity, :, columns(q)], g_pair.at[q],
            pair_send.at[i], pair_recv.at[i], pair_dev,
        )

    def w_pair_copy(j):
        return remote(
            w_src(1 - parity, j, pair_rows), w_pair.at[j, :, pair_rows, :],
            wp_send.at[j], wp_recv.at[j], pair_dev,
        )

    def sibling_copy(rows):
        return remote(
            w_pair.at[:, :, rows, :], w_pair.at[:, :, rows, :],
            sib_sem.at[0], sib_sem.at[1], {"pts": 1 - core},
        )

    def own_copy(q):
        return pltpu.make_async_copy(
            greens.at[:, parity, :, columns(q)], g_own.at[q], own_sem.at[q]
        )

    def w_own_copy(j):
        return pltpu.make_async_copy(w_src(parity, j, every_row), w_own.at[j], w_own_sem.at[j])

    @pl.loop(0, 2 * nq)
    def _(i):
        @pl.when(i < nq)
        def _():
            pair_copy(i).start()

        half = i // nq
        c = lax.rem(i, nq)
        send_inward(greens.at[:, parity, :, columns(pair_q(i))], 0, half, edge, c)
        own_copy(i).start()

    @pl.loop(0, n)
    def _(j):
        w_pair_copy(j).start()
        w_own_copy(j).start()

    @pl.loop(nq, 2 * nq)
    def _(i):
        pair_copy(i).start()

    hello()

    acc[...] = jnp.zeros_like(acc)

    @pl.loop(0, 2 * nq)
    def _(q):
        own_copy(q).wait()

    @pl.loop(0, n)
    def _(j):
        w_own_copy(j).wait()

    def contribute(w, gi, gj, q, weight):
        for s in range(sub):
            part = slice(s * LANES, (s + 1) * LANES)
            both = jnp.concatenate([gj[0, :, part], gj[1, :, part]], axis=1)
            ab = jnp.dot(w[...].reshape(2 * h, h), both, preferred_element_type=jnp.float32)
            a, b = ab[:h], ab[h:]
            t = gi[0, :, part].astype(jnp.float32) * (a[:, :LANES] - b[:, LANES:])
            t = t + gi[1, :, part].astype(jnp.float32) * (a[:, LANES:] + b[:, :LANES])
            t = jnp.sum(t.reshape(h // 8, 8, LANES), axis=0)
            acc[q * sub + s] += t * weight

    def far_at(t):
        p = t // (side_len * nq)
        rest = lax.rem(t, side_len * nq)
        return p, side_len - 1 - rest // nq, lax.rem(rest, nq)

    def near_at(t):
        width = jnp.maximum(edge, 1) * nq
        p = t // (2 * width)
        half = lax.rem(t // width, 2)
        rest = lax.rem(t, width)
        return p, half, jnp.maximum(edge, 1) - 1 - rest // nq, lax.rem(rest, nq)

    def part_of(p):
        return jnp.where(p == 0, parity, 1 - parity)

    def far_work(t, w, g):
        p, b, c = far_at(t)
        q = r_base + c
        j = global_block(b, True) * 2 + part_of(p)
        contribute(w.at[j], g.at[q], far.at[b, p, c], q, 2.0)

    def near_work(t, w, g):
        p, half, b, c = near_at(t)
        q = jnp.where(half == 0, s_base, r_base) + c
        j = global_block(b, False) * 2 + part_of(p)
        contribute(w.at[j], g.at[q], near.at[b, p, q], q, 2.0)

    def far_wait(t):
        p, b, c = far_at(t)
        ref = far.at[b, p, c]
        remote(ref, ref, out_send.at[t], far_recv.at[t], in_dev).wait_recv()

        @pl.when(edge > 0)
        def _():
            remote(ref, ref, out_send.at[t], far_recv.at[t], out_dev).start()

    def near_wait(t):
        p, half, b, c = near_at(t)
        q = jnp.where(half == 0, s_base, r_base) + c
        ref = near.at[b, p, q]
        remote(ref, ref, in_send.at[t], in_recv.at[t], out_dev).wait_recv()
        send_inward(ref, p, half, b, c)

    def newest(u):
        far_work(u, w_pair, g_pair)

        @pl.when(u < n_near)
        def _():
            near_work(u, w_pair, g_pair)

    @pl.loop(0, steps)
    def _(t):
        has_pair = jnp.logical_and(jnp.logical_and(t >= nq, t <= 3 * nq), t != 2 * nq)
        turn = t - nq - (t > 2 * nq).astype(jnp.int32)

        @pl.when(has_pair)
        def _():
            i = turn
            pair_copy(i).wait_recv()
            send_inward(g_pair.at[pair_q(i)], 1, i // nq, edge, lax.rem(i, nq))

        @pl.when(t < n_far)
        def _():
            far_wait(t)

        if side_len > 1:
            @pl.when(t < n_near)
            def _():
                near_wait(t)

        @pl.when(t == catch_up - 1)
        def _():
            @pl.loop(0, n)
            def _(j):
                w_pair_copy(j).wait_recv()

            sibling_copy(pair_rows).start()

        @pl.when(t < 2 * nq)
        def _():
            contribute(w_own.at[2 * z + parity], g_own.at[t], g_own.at[t], t, 1.0)

        @pl.when(has_pair)
        def _():
            q = pair_q(turn)
            contribute(w_own.at[2 * z + 1 - parity], g_own.at[q], g_pair.at[q], q, 2.0)

        @pl.when(t < n_far)
        def _():
            far_work(t, w_own, g_own)

        if side_len > 1:
            @pl.when(t < n_near)
            def _():
                near_work(t, w_own, g_own)

        @pl.when(t == catch_up)
        def _():
            sibling_copy(pl.ds(pl.multiple_of((1 - core) * half_rows, 8), half_rows)).wait_recv()

        @pl.when(t >= catch_up)
        def _():
            first = (t - catch_up) * per_step
            last = jnp.minimum(first + per_step, steps)
            if spread:
                first = ((t - catch_up) * 2 * nq) // left
                last = ((t - catch_up + 1) * 2 * nq) // left

            @pl.loop(first, last)
            def _(u):
                @pl.when(u < 2 * nq)
                def _():
                    q = pair_q(u)
                    contribute(w_pair.at[2 * z + 1 - parity], g_pair.at[q], g_pair.at[q], q, 1.0)

                if spread:
                    far_work(lax.rem(u, side_len) * nq + u // side_len, w_pair, g_pair)
                else:
                    @pl.when(u < n_far)
                    def _():
                        far_work(u, w_pair, g_pair)

                if side_len > 1:
                    @pl.when(u < n_near)
                    def _():
                        near_work(u, w_pair, g_pair)

            if spread:
                newest(t - 1)

    if spread:
        newest(steps - 1)

    total = n * n_freq
    rank = me * n_freq + fq
    red[rank] = jnp.sum(acc[...], axis=1) / stations

    def share_copy(k, source):
        target = lax.rem(rank + k, total)
        return remote(
            red.at[source], red.at[source], red_send.at[k - 1], red_recv.at[k - 1],
            {"stn": target // n_freq, "freq": lax.rem(target, n_freq)},
        )

    @pl.loop(1, total)
    def _(k):
        share_copy(k, rank).start()

    @pl.loop(1, total)
    def _(k):
        share_copy(k, lax.rem(rank - k + total, total)).wait_recv()

    raw = red[0]
    for d in range(1, total):
        raw = raw + red[d]
    max_out[...] = jnp.broadcast_to(jnp.max(jnp.abs(raw)), max_out.shape)
    max_copy = remote(max_out, max_in, max_sem.at[0], max_sem.at[1], {"pts": 1 - core})
    max_copy.start()

    @pl.loop(1, total)
    def _(k):
        share_copy(k, rank).wait_send()

    @pl.loop(0, 2 * nq)
    def _(i):
        pair_copy(i).wait_send()

    @pl.loop(0, n)
    def _(j):
        w_pair_copy(j).wait_send()

    sibling_copy(pair_rows).wait_send()
    ref = far.at[0, 0, 0]

    @pl.loop(0, jnp.where(inner, n_far, (edge + 1) * 4 * nq))
    def _(t):
        remote(ref, ref, in_send.at[t], far_recv.at[0], in_dev).wait_send()

    @pl.when(edge > 0)
    def _():
        @pl.loop(0, n_far)
        def _(t):
            remote(ref, ref, out_send.at[t], far_recv.at[0], out_dev).wait_send()

    max_copy.wait()
    largest = jnp.maximum(max_out[0:1, 0:1], max_in[0:1, 0:1])
    out[...] = raw / (largest + 1e-6)


def kernel_body(n, n_freq, greens, weights):
    _, _, h, points = greens.shape
    stations = weights.shape[3]
    half = points // 2
    chunk = LANES
    while chunk * 2 * h <= 32768 and half % (chunk * 2) == 0:
        chunk *= 2
    nq = half // chunk
    side_len = n // 4
    n_far = side_len * 2 * nq
    n_near = max(side_len - 1, 1) * 4 * nq
    blocked = h % LANES != 0
    if blocked:
        weights = weights.reshape(2, weights.shape[1], h, n, h).swapaxes(2, 3)
    if side_len == 2 and nq >= 8 and nq % 2 == 0:
        return line_body(n_freq, chunk, nq, blocked, greens, weights)
    dma = pltpu.SemaphoreType.DMA
    bf16, f32 = jnp.bfloat16, jnp.float32
    rows = points // LANES
    out = pl.pallas_call(
        functools.partial(ring_kernel, n, n_freq, h, stations, chunk, nq, blocked),
        out_shape=jax.ShapeDtypeStruct((rows, LANES), f32),
        in_specs=[pl.BlockSpec(memory_space=pl.ANY)] * 2,
        out_specs=pl.BlockSpec(memory_space=pltpu.VMEM),
        scratch_shapes=[
            pltpu.VMEM((2 * nq, 2, h, chunk), bf16),
            pltpu.VMEM((2 * nq, 2, h, chunk), bf16),
            pltpu.VMEM((max(side_len - 1, 1), 2, 2 * nq, 2, h, chunk), bf16),
            pltpu.VMEM((side_len, 2, nq, 2, h, chunk), bf16),
            pltpu.VMEM((n, 2, h, h), bf16),
            pltpu.VMEM((n, 2, h, h), bf16),
            pltpu.VMEM((rows, 8, LANES), f32),
            pltpu.VMEM((n * n_freq, rows, LANES), f32),
            pltpu.VMEM((8, LANES), f32),
            pltpu.VMEM((8, LANES), f32),
            dma((2 * nq,)), dma((n,)), dma((2 * nq,)), dma((2 * nq,)), dma((n,)), dma((n,)), dma((2,)),
            dma((max(n_near, n_far),)), dma((n_near,)), dma((n_far,)), dma((n_far,)),
            dma((n * n_freq - 1,)), dma((n * n_freq - 1,)), dma((2,)),
            pltpu.SemaphoreType.REGULAR((2, n // 2 - 1)), pltpu.SemaphoreType.REGULAR((2,)),
        ],
        compiler_params=pltpu.CompilerParams(
            collective_id=0, has_side_effects=True, vmem_limit_bytes=60 * 1024 * 1024
        ),
    )(greens, weights)
    return out.reshape(points)


FAR_FIRST = (11, 9, 10, 8, 7, 5, 6, 4, 15, 13, 14, 12, 3, 1, 2, 0)


def line_kernel(
    n_freq, h, stations, chunk, nq, kept, late, blocked,
    greens, weights, out,
    g_own, g_pair, near, far, w_own, w_pair, w_edge, folded, lent, acc, part, side, sums, extras,
    own_sem, w_own_sem, pair_send, pair_recv, wp_send, wp_recv, sib_sem, we_send, we_recv, we_sib,
    in_send, near_recv, far_recv, down_send, back_send, part_send, part_recv, side_sem,
    extra_send, extra_recv, base_sem, fold_sem, lend_sem, reply_sem, hello_sem, pair_hello,
):
    n = 8
    sub = chunk // LANES
    half_rows = h // 2
    steps = 4 * nq
    me = lax.axis_index("stn")
    core = lax.axis_index("pts")
    fq = lax.axis_index("freq")
    parity = lax.rem(me, 2)
    z = me // 2
    hi = z // 2
    inner = jnp.logical_or(z == 1, z == 2)
    outer = jnp.logical_not(inner)
    s_base = hi * nq
    r_base = (1 - hi) * nq
    rank = me * n_freq + fq
    total = n * n_freq
    inward = jnp.where(hi == 1, -2, 2)
    pair_dev = {"stn": me + 1 - 2 * parity}
    in_dev = {"stn": me + inward}
    out_dev = {"stn": me - inward}
    core_dev = {"pts": 1 - core}
    freq_dev = {"freq": n_freq - 1 - fq}
    across_dev = {"stn": 2 * (3 - z) + parity}
    other_inner = 2 - hi
    other_edge = 3 - 3 * hi
    near_z = jnp.where(inner, z - inward // 2, z + inward // 2)

    def columns(q):
        return pl.ds(pl.multiple_of(q * chunk, LANES), chunk)

    def w_src(freq, j, rows):
        if blocked:
            return weights.at[:, freq, j, rows, :]
        return weights.at[:, freq, rows, pl.ds(pl.multiple_of(j * h, LANES), h)]

    def block_of(where, p):
        return 2 * where + jnp.where(p == 0, parity, 1 - parity)

    def far_block(e):
        return block_of(jnp.where(lax.rem(e, 2) == 0, other_inner, other_edge), e // 2)

    def position(e, c):
        late_c = c >= jnp.where(e < 2, nq - 1, kept)
        pair_half = jnp.where(e == 2, 2 * nq, 2 * nq + kept) + c
        pair_late = jnp.where(e == 2, 2 * nq + kept, 3 * nq) + c
        early = jnp.where(late_c, 2 * nq - 2 + e, e * (nq - 1) + c)
        return jnp.where(e < 2, early, jnp.where(late_c, pair_late, pair_half))

    def block_at(t):
        e = (t >= nq - 1).astype(jnp.int32)
        c = t - e * (nq - 1)
        corner = t >= 2 * nq - 2
        e = jnp.where(corner, t - (2 * nq - 2), e)
        c = jnp.where(corner, nq - 1, c)
        pairs = t - 2 * nq
        third = jnp.logical_and(pairs >= kept, pairs < 2 * kept)
        third = jnp.logical_or(third, pairs >= nq + kept)
        pair_c = jnp.where(pairs < kept, pairs, jnp.where(pairs < nq + kept, pairs - kept, pairs - nq))
        e = jnp.where(pairs >= 0, 2 + third.astype(jnp.int32), e)
        c = jnp.where(pairs >= 0, pair_c, c)
        return e, c

    every_row = pl.ds(0, h)
    my_rows = pl.ds(pl.multiple_of(core * half_rows, 8), half_rows)
    sib_rows = pl.ds(pl.multiple_of((1 - core) * half_rows, 8), half_rows)

    def pair_q(i):
        return jnp.where(i < nq, s_base + i, r_base + i - nq)

    def g_src(q):
        return greens.at[:, parity, :, columns(q)]

    def own_copy(q):
        return pltpu.make_async_copy(g_src(q), g_own.at[q], own_sem.at[0])

    def w_own_copy(j):
        return pltpu.make_async_copy(w_src(parity, j, every_row), w_own.at[j], w_own_sem.at[0])

    def pair_copy(i):
        q = pair_q(i)
        return remote(
            greens.at[:, 1 - parity, :, columns(q)], g_pair.at[q],
            pair_send.at[0], pair_recv.at[i // 2], pair_dev,
        )

    def w_pair_copy(j):
        return remote(
            w_src(1 - parity, j, my_rows), w_pair.at[j, :, my_rows, :],
            wp_send.at[0], wp_recv.at[0], pair_dev,
        )

    def sibling_copy(rows):
        part_of_w = w_pair.at[:, :, rows, :]
        return remote(part_of_w, part_of_w, sib_sem.at[0], sib_sem.at[1], core_dev)

    def edge_sibling_copy(rows):
        part_of_w = w_edge.at[:, :, :, rows, :]
        return remote(part_of_w, part_of_w, we_sib.at[0], we_sib.at[1], core_dev)

    first_groups = nq // 2 + (nq - kept + 1) // 2
    back_group = first_groups + nq // 2 + nq - kept
    singles = 2 * nq + 2 * kept

    def near_slot(p, i):
        m = i - nq - kept
        return p * first_groups + jnp.where(i < nq, i // 2, nq // 2 + jnp.where(p == 0, m // 2, m))

    def far_slot(slot):
        return jnp.where(slot < singles, slot // 2, slot - singles // 2)

    def whole(ref, send_sem, recv_sem):
        return remote(ref, ref, send_sem.at[0], recv_sem.at[0], pair_dev)

    def up_copy(src, p, i):
        return remote(src, near.at[p, pair_q(i)], in_send.at[0], near_recv.at[near_slot(p, i)], in_dev)

    def up_weights(src, b, p):
        return remote(src, w_edge.at[b, p, :, my_rows, :], we_send.at[0], we_recv.at[0], in_dev)

    def mid_copy(src, slot):
        return remote(src, far.at[slot], in_send.at[0], far_recv.at[far_slot(slot)], in_dev)

    def lend_copy():
        src = near.at[1, pair_q(nq - 1)]
        return remote(src, lent, lend_sem.at[0], lend_sem.at[1], core_dev)

    corner = 2 * nq - 2

    def down_copy(slot):
        return remote(far.at[slot], far.at[slot], down_send.at[0], far_recv.at[far_slot(slot)], out_dev)

    def back_copy(src, p, c):
        return remote(
            src, near.at[p, r_base + c], back_send.at[0], near_recv.at[back_group + p], out_dev,
        )

    barrier = pltpu.get_barrier_semaphore()
    up, down = z < 3, z > 0
    greeted = [pair_dev, core_dev, freq_dev]

    def greet(sem, device):
        pl.semaphore_signal(sem, inc=1, device_id=device, device_id_type=MESH)

    def along_z(sem_down, sem_up):
        @pl.when(up)
        def _():
            greet(sem_up, {"stn": me + 2})

        @pl.when(down)
        def _():
            greet(sem_down, {"stn": me - 2})

    @pl.when(inner)
    def _():
        greet(barrier, in_dev)
        greet(barrier, out_dev)

    for device in greeted:
        greet(barrier, device)
    pl.semaphore_wait(barrier, len(greeted) + 1)

    @pl.when(outer)
    def _():
        greet(reply_sem.at[0], in_dev)

    @pl.loop(0, nq)
    def _(i):
        src = g_src(pair_q(i))

        @pl.when(jnp.logical_and(inner, i < nq - 1))
        def _():
            mid_copy(src, i).start()

        @pl.when(outer)
        def _():
            up_copy(src, 0, i).start()

    corner_src = g_src(pair_q(nq - 1))

    @pl.loop(0, n)
    def _(j):
        w_pair_copy(j).start()
        w_own_copy(j).start()

    @pl.loop(0, 2 * nq)
    def _(i):
        own_copy(pair_q(i)).start()
        pair_copy(i).start()

    @pl.when(inner)
    def _():
        pl.semaphore_wait(reply_sem.at[0], 1)

        @pl.loop(0, kept)
        def _(c):
            back_copy(g_src(pair_q(nq + c)), 0, c).start()

    @pl.when(outer)
    def _():
        for b in range(2):
            up_weights(w_src(parity, far_block(2 + b), my_rows), b, 0).start()

    @pl.loop(0, 2)
    def _(r):
        along_z(hello_sem.at[0], hello_sem.at[1])

        @pl.when(up)
        def _():
            pl.semaphore_wait(hello_sem.at[0], 1)

        @pl.when(down)
        def _():
            pl.semaphore_wait(hello_sem.at[1], 1)

    for i, device in enumerate((pair_dev, freq_dev, core_dev)):
        greet(pair_hello.at[i], device)
        pl.semaphore_wait(pair_hello.at[i], 1)

    acc[...] = jnp.zeros_like(acc)

    pltpu.make_async_copy(g_own, g_own, own_sem.at[0]).wait()
    pltpu.make_async_copy(w_own, w_own, w_own_sem.at[0]).wait()

    def product(w, gi, gj, s):
        lanes = slice(s * LANES, (s + 1) * LANES)
        both = jnp.concatenate([gj[0, :, lanes], gj[1, :, lanes]], axis=1)
        ab = jnp.dot(w[...].reshape(2 * h, h), both, preferred_element_type=jnp.float32)
        a, b = ab[:h], ab[h:]
        t = gi[0, :, lanes].astype(jnp.float32) * (a[:, :LANES] - b[:, LANES:])
        t = t + gi[1, :, lanes].astype(jnp.float32) * (a[:, LANES:] + b[:, :LANES])
        return jnp.sum(t.reshape(h // 8, 8, LANES), axis=0)

    def contribute(w, gi, gj, q, weight):
        for s in range(sub):
            acc[q * sub + s] += product(w, gi, gj, s) * weight

    own_pair_block = block_of(z, 1)

    def own_work(q):
        contribute(w_own.at[me], g_own.at[q], g_own.at[q], q, 1.0)

    def cross_work(q):
        contribute(w_own.at[own_pair_block], g_own.at[q], g_pair.at[q], q, 2.0)

    def pair_work(q):
        contribute(w_pair.at[own_pair_block], g_pair.at[q], g_pair.at[q], q, 1.0)

    def far_work(e, c, w, g):
        q = r_base + c
        contribute(w.at[far_block(e)], g.at[q], far.at[position(e, c)], q, 2.0)

    def near_work(p, q, w, g):
        contribute(w.at[block_of(near_z, p)], g.at[q], near.at[p, q], q, 2.0)

    def edge_work(b, c):
        q = r_base + c

        @pl.loop(0, 2)
        def _(p):
            contribute(w_edge.at[b, p], near.at[p, q], far.at[position(2 + b, c)], q, 2.0)

    def transposed(w, g):
        return lax.dot_general(w, g, (((0,), (0,)), ((), ())), preferred_element_type=jnp.float32)

    def fold(w, gi, s):
        lanes = slice(s * LANES, (s + 1) * LANES)
        both = jnp.concatenate([gi[0, :, lanes], gi[1, :, lanes]], axis=1)
        a, b = transposed(w[0], both), transposed(w[1], both)
        return a[:, :LANES] + b[:, LANES:], a[:, LANES:] - b[:, :LANES]

    def fold_last():
        q, j = r_base + nq - 1, far_block(3)
        for s in range(sub):
            lanes = slice(s * LANES, (s + 1) * LANES)
            re, im = fold(w_own.at[j], g_own.at[q], s)
            folded[core, 0, :, lanes] = re
            folded[core, 1, :, lanes] = im
            for w, g in ((w_pair.at[j], g_pair.at[q]), (w_edge.at[1, 0], near.at[0, q]), (w_edge.at[1, 1], near.at[1, q])):
                re, im = fold(w, g, s)
                folded[core, 0, :, lanes] += re
                folded[core, 1, :, lanes] += im

        @pl.when(core == 0)
        def _():
            fold_copy().start()

    def fold_copy():
        return remote(folded.at[0], folded.at[0], fold_sem.at[0], fold_sem.at[1], core_dev)

    def unfold(which, slot, s):
        lanes = slice(s * LANES, (s + 1) * LANES)
        t = far[slot, 0, :, lanes].astype(jnp.float32) * folded[which, 0, :, lanes]
        t = t + far[slot, 1, :, lanes].astype(jnp.float32) * folded[which, 1, :, lanes]
        return 2.0 * jnp.sum(t.reshape(h // 8, 8, LANES), axis=0)

    def passed_down(t):
        return t < 2 * nq + 2 * kept

    def wait_blocks(count, recv_sem):
        ref = far.at[pl.ds(0, count)]
        remote(ref, ref, in_send.at[0], recv_sem, in_dev).wait_recv()

    def wait_far(t):
        @pl.when(jnp.logical_and(t < singles, lax.rem(t, 2) == 0))
        def _():
            wait_blocks(2, far_recv.at[t // 2])

        @pl.when(t >= singles)
        def _():
            wait_blocks(1, far_recv.at[t - singles // 2])

    def wait_pair(i):
        @pl.when(lax.rem(i, 2) == 0)
        def _():
            wait_blocks(2, pair_recv.at[i // 2])

    def wait_near(p, i):
        m = jnp.where(i < nq, i, i - nq - kept)
        even = lax.rem(m, 2) == 0
        alone = jnp.logical_and(i >= nq, p == 1)
        two = even & jnp.logical_not(alone) & (i < 2 * nq - 1)
        lone = jnp.logical_or(alone, even & (i == 2 * nq - 1))

        @pl.when(two)
        def _():
            wait_blocks(2, near_recv.at[near_slot(p, i)])

        @pl.when(lone)
        def _():
            wait_blocks(1, near_recv.at[near_slot(p, i)])

    def wait_back(p):
        wait_blocks(kept, near_recv.at[back_group + p])

    def wait_w_pair():
        whole(w_pair.at[:, :, my_rows, :], wp_send, wp_recv).wait_recv()
        sibling_copy(my_rows).start()

    def share_part():
        part[rank] = jnp.sum(acc[...], axis=1) / stations

        @pl.loop(0, total // 2 - 1)
        def _(k):
            part_copy(total // 2 - 1 - k, rank).start()

    def at_rank(target):
        return {"stn": target // n_freq, "freq": lax.rem(target, n_freq)}

    def flipped(k):
        bit, flip = total // 2, jnp.int32(0)
        while bit:
            mine = lax.rem(rank // bit, 2)
            turn = lax.rem(k // bit, 2)
            flip = flip + bit * (mine + turn - 2 * mine * turn)
            bit //= 2
        return flip

    def part_copy(k, source):
        ref = part.at[source]
        return remote(ref, ref, part_send.at[0], part_recv.at[0], at_rank(flipped(k)))

    my_group = (hi * 2 + parity) * n_freq + fq
    late_rows = late * sub

    sends = [(k, other) for k in FAR_FIRST for other in range(2) if k or other]

    def extra_copy(k, other):
        def turned(v, bit):
            return 1 - v if k & bit else v

        message = extras.at[core * 4 * n_freq + my_group]
        target_z = 2 * turned(hi, 8) + turned(lax.rem(z, 2), 4)
        target = {
            "stn": 2 * target_z + turned(parity, 2), "freq": turned(fq, 1),
            "pts": 1 - core if other else core,
        }
        return remote(
            message, message, extra_send.at[other], extra_recv.at[core], target,
        )

    def late_row(t):
        return jnp.sum(t, axis=0, keepdims=True) / stations

    def finish():
        first = (r_base + nq - late) * sub
        for c in range(late_rows):
            extras[core * 4 * n_freq + my_group, c] = late_row(acc[first + c])
        for s in range(sub):
            extras[core * 4 * n_freq + my_group, late_rows + s] = jnp.zeros((1, LANES), jnp.float32)

        @pl.when(core == 1)
        def _():
            fold_copy().wait_recv()
            wait_blocks(1, far_recv.at[steps - singles // 2])
            wait_blocks(1, far_recv.at[steps - 1 - singles // 2])
            for s in range(sub):
                c = late_rows - sub + s
                extras[4 * n_freq + my_group, c] = late_row(acc[first + c] + unfold(1, steps - 1, s))
                extras[4 * n_freq + my_group, late_rows + s] = late_row(unfold(0, steps, s))

        for k, other in sends:
            extra_copy(k, other).start()

    near_second = nq + 4
    near_third = near_second + nq
    near_fourth = near_third + nq - kept
    near_end = near_fourth + nq - kept

    def near_at(t):
        i = jnp.where(t >= near_second, t - near_second, t)
        i = jnp.where(t >= near_third, t - near_third + nq + kept, i)
        i = jnp.where(t >= near_fourth, t - near_fourth + nq + kept, i)
        second = jnp.logical_and(t >= near_second, t < near_third)
        p = jnp.logical_or(second, t >= near_fourth).astype(jnp.int32)
        present = jnp.logical_or(t < nq, jnp.logical_and(t >= near_second, t < near_end))
        return present, p, i

    @pl.when(inner)
    def _():
        @pl.loop(0, steps - 1)
        def _(t):
            has_near, p, i = near_at(t)
            has_pair = jnp.logical_and(t >= nq, t < 3 * nq)
            turn = t - nq
            wait_far(t)

            @pl.when(passed_down(t))
            def _():
                down_copy(t).start()

            @pl.when(has_near)
            def _():
                wait_near(p, i)

            @pl.when(t < nq)
            def _():
                mid_copy(near.at[0, pair_q(t)], position(1, t)).start()

            @pl.when(t == nq - 2)
            def _():
                mid_copy(corner_src, corner).start()

            @pl.when(t == nq)
            def _():
                wait_w_pair()

            @pl.when(has_pair)
            def _():
                wait_pair(turn)

                @pl.when(turn < kept)
                def _():
                    mid_copy(g_pair.at[pair_q(turn)], 2 * nq + turn).start()

                @pl.when(jnp.logical_and(turn >= nq, turn < nq + kept))
                def _():
                    back_copy(g_pair.at[pair_q(turn)], 1, turn - nq).start()

            third = t - near_second
            fourth = third - (nq - kept)

            @pl.when(jnp.logical_and(third >= 0, third < kept))
            def _():
                mid_copy(near.at[1, pair_q(third)], 2 * nq + kept + third).start()

            send_third = jnp.logical_and(third >= kept, third < nq)

            @pl.when(send_third)
            def _():
                mid_copy(g_pair.at[pair_q(third)], 2 * nq + kept + third).start()

            @pl.when(jnp.logical_and(third == nq - 1, core == 0))
            def _():
                lend_copy().start()

            @pl.when(jnp.logical_and(fourth >= kept, fourth < nq - 1 + core))
            def _():
                mid_copy(near.at[1, pair_q(fourth)], 3 * nq + fourth).start()

            @pl.when(jnp.logical_and(fourth == nq - 1, core == 1))
            def _():
                lend_copy().wait_recv()
                mid_copy(lent, steps).start()

            @pl.when(t == nq + 2)
            def _():
                sibling_copy(sib_rows).wait_recv()

            @pl.when(t == near_second)
            def _():
                whole(w_edge.at[:, :, :, my_rows, :], we_send, we_recv).wait_recv()
                edge_sibling_copy(my_rows).start()

            @pl.when(t == near_second + 2)
            def _():
                edge_sibling_copy(sib_rows).wait_recv()

            e, c = block_at(t)
            far_work(e, c, w_own, g_own)

            @pl.when(t < 2 * nq)
            def _():
                own_work(t)

            @pl.when(has_near)
            def _():
                q = pair_q(i)
                near_work(p, q, w_own, g_own)

                @pl.when(t >= nq)
                def _():
                    near_work(p, q, w_pair, g_pair)

                @pl.when(t >= near_fourth)
                def _():
                    edge_work(0, i - nq)

            @pl.when(has_pair)
            def _():
                cross_work(pair_q(turn))

            lag = t - nq - 2

            @pl.when(jnp.logical_and(lag >= 0, lag < 2 * nq))
            def _():
                pair_work(pair_q(lag))

                @pl.when(lag < nq)
                def _():
                    near_work(0, pair_q(lag), w_pair, g_pair)

            @pl.when(t >= 2 * nq)
            def _():
                far_work(e, c, w_pair, g_pair)

                @pl.when(t < 3 * nq)
                def _():
                    @pl.loop(0, 2)
                    def _(first):
                        far_work(first, t - 2 * nq, w_pair, g_pair)

            @pl.when(t >= 3 * nq + kept)
            def _():
                edge_work(1, t - 3 * nq)

            @pl.when(t == steps - late - 1)
            def _():
                share_part()

                @pl.loop((nq - late) * sub, nq * sub)
                def _(c):
                    acc[r_base * sub + c] = jnp.zeros((8, LANES), jnp.float32)

            @pl.when(t == near_end - 1)
            def _():
                fold_last()

        finish()

    @pl.when(outer)
    def _():
        @pl.loop(0, 3 * nq)
        def _(t):
            turn = t - nq + 2
            has_pair = jnp.logical_and(turn >= 0, turn < 2 * nq)
            back = t - 2 * nq - 4
            has_back = jnp.logical_and(back >= 0, back < kept)
            e, c = block_at(t)
            has_far = t < 2 * nq + 2 * kept

            @pl.when(turn == 0)
            def _():
                wait_w_pair()
                for b in range(2):
                    up_weights(w_pair.at[far_block(2 + b), :, my_rows, :], b, 1).start()

            @pl.when(has_pair)
            def _():
                wait_pair(turn)

                @pl.when(jnp.logical_or(turn < nq, turn >= nq + kept))
                def _():
                    up_copy(g_pair.at[pair_q(turn)], 1, turn).start()

                @pl.when(turn == nq - 1)
                def _():
                    @pl.loop(nq + kept, 2 * nq)
                    def _(i):
                        up_copy(g_src(pair_q(i)), 0, i).start()

            @pl.when(t == nq)
            def _():
                sibling_copy(sib_rows).wait_recv()

            @pl.when(t == 0)
            def _():
                wait_back(0)

            @pl.when(back == 0)
            def _():
                wait_back(1)

            @pl.when(has_far)
            def _():
                wait_far(t)
                far_work(e, c, w_own, g_own)

            @pl.when(jnp.logical_and(has_far, t >= 2 * nq))
            def _():
                far_work(e, c, w_pair, g_pair)

            @pl.when(t < 2 * nq)
            def _():
                own_work(t)

            @pl.when(t < kept)
            def _():
                near_work(0, r_base + t, w_own, g_own)

            @pl.when(has_back)
            def _():
                q = r_base + back
                near_work(0, q, w_pair, g_pair)
                near_work(1, q, w_own, g_own)
                near_work(1, q, w_pair, g_pair)

            @pl.when(has_pair)
            def _():
                cross_work(pair_q(turn))

            @pl.when(t >= nq)
            def _():
                pair_work(pair_q(t - nq))

            @pl.when(t >= 2 * nq)
            def _():
                @pl.loop(0, 2)
                def _(first):
                    far_work(first, t - 2 * nq, w_pair, g_pair)

        share_part()

    parts = part.at[pl.ds(0, total // 2 - 1)]
    whole(parts, part_send, part_recv).wait_recv()

    base = hi * (total // 2)
    mine = part[base]
    for d in range(1, total // 2):
        mine = mine + part[base + d]
    side[hi] = mine

    def side_copy(which):
        ref = side.at[which]
        return remote(ref, ref, side_sem.at[0], side_sem.at[1], across_dev)

    side_copy(hi).start()
    side_copy(1 - hi).wait_recv()
    sums[core] = side[0] + side[1]
    base_copy = remote(sums.at[core], sums.at[core], base_sem.at[0], base_sem.at[1], core_dev)
    base_copy.start()

    whole(g_pair, pair_send, pair_recv).wait_send()
    whole(w_pair.at[:, :, my_rows, :], wp_send, wp_recv).wait_send()
    sibling_copy(my_rows).wait_send()
    whole(parts, part_send, part_recv).wait_send()

    def sent(count, send_sem):
        whole(far.at[pl.ds(0, count)], send_sem, far_recv).wait_send()

    @pl.when(inner)
    def _():
        sent(2 * nq + 2 * kept, down_send)
        sent(2 * kept, back_send)
        edge_sibling_copy(my_rows).wait_send()
        for other in range(2):
            ref = extras.at[pl.ds(0, total - 1 + other)]
            remote(ref, ref, extra_send.at[other], extra_recv.at[0], core_dev).wait_send()

        @pl.when(core == 0)
        def _():
            sent(steps - 1, in_send)
            fold_copy().wait_send()
            lend_copy().wait_send()

        @pl.when(core == 1)
        def _():
            sent(steps + 1, in_send)

    @pl.when(outer)
    def _():
        sent(steps - 2 * kept, in_send)
        whole(w_edge.at[:, :, :, my_rows, :], we_send, we_recv).wait_send()

    side_copy(hi).wait_send()

    def wait_extras(which, groups):
        ref = extras.at[pl.ds(which * 4 * n_freq, groups)]
        remote(ref, ref, extra_send.at[0], extra_recv.at[which], core_dev).wait_recv()

    @pl.when(inner)
    def _():
        wait_extras(core, 4 * n_freq - 1)
        wait_extras(1 - core, 4 * n_freq)

    @pl.when(outer)
    def _():
        wait_extras(0, 4 * n_freq)
        wait_extras(1, 4 * n_freq)

    base_copy.wait_send()
    sum_ref = sums.at[1 - core]
    remote(sum_ref, sum_ref, base_sem.at[0], base_sem.at[1], core_dev).wait_recv()

    def late_sum(which, low, c):
        first = (2 * which + low) * 2 * n_freq
        row = extras[first, c]
        for g in range(1, 2 * n_freq):
            row = row + extras[first + g, c]
        return row

    for which in range(2):
        for low in range(2):
            gathered = [late_sum(which, low, c) for c in range(late_rows)]
            if which == 0:
                for s in range(sub):
                    gathered[late_rows - sub + s] += late_sum(1, low, late_rows + s)
            at = ((1 - low) * nq + nq - late) * sub
            sums[which, at:at + late_rows, :] += jnp.concatenate(gathered, axis=0)

    largest = jnp.max(jnp.maximum(jnp.abs(sums[0]), jnp.abs(sums[1])), keepdims=True)
    out[...] = sums[core] / (largest + 1e-6)


def line_body(n_freq, chunk, nq, blocked, greens, weights):
    _, _, h, points = greens.shape
    n = 8
    kept, late = 3 * nq // 8, 3
    stations = n * h
    dma = pltpu.SemaphoreType.DMA
    one, two = dma((1,)), dma((2,))
    near_groups = nq + (nq - kept + 1) // 2 + nq - kept + 2
    regular = pltpu.SemaphoreType.REGULAR
    bf16, f32 = jnp.bfloat16, jnp.float32
    rows = points // LANES
    late_rows = late * (chunk // LANES)
    total = n * n_freq
    out = pl.pallas_call(
        functools.partial(line_kernel, n_freq, h, stations, chunk, nq, kept, late, blocked),
        out_shape=pltpu.VMEM((rows, LANES), f32),
        in_specs=[pl.BlockSpec(memory_space=pl.ANY)] * 2,
        out_specs=pl.BlockSpec(memory_space=pltpu.VMEM),
        scratch_shapes=[
            pltpu.VMEM((2 * nq, 2, h, chunk), bf16),
            pltpu.VMEM((2 * nq, 2, h, chunk), bf16),
            pltpu.VMEM((2, 2 * nq, 2, h, chunk), bf16),
            pltpu.VMEM((4 * nq + 1, 2, h, chunk), bf16),
            pltpu.VMEM((n, 2, h, h), bf16),
            pltpu.VMEM((n, 2, h, h), bf16),
            pltpu.VMEM((2, 2, 2, h, h), bf16),
            pltpu.VMEM((2, 2, h, chunk), f32),
            pltpu.VMEM((2, h, chunk), bf16),
            pltpu.VMEM((rows, 8, LANES), f32),
            pltpu.VMEM((total, rows, LANES), f32),
            pltpu.VMEM((2, rows, LANES), f32),
            pltpu.VMEM((2, rows, LANES), f32),
            pltpu.VMEM((8 * n_freq, late_rows + chunk // LANES, 1, LANES), f32),
            one, one, one, dma((nq,)), one, one, two,
            one, one, two,
            one, dma((near_groups,)), dma((3 * nq + 1 - kept,)), one, one,
            one, one, two,
            two, two, two, two, two,
            regular((1,)), regular((2,)), regular((3,)),
        ],
        compiler_params=pltpu.CompilerParams(
            collective_id=0, has_side_effects=True, vmem_limit_bytes=60 * 1024 * 1024
        ),
    )(greens, weights)
    return out.reshape(points)


def passed_along(x, axis, by):
    size = lax.axis_size(axis)
    return lax.ppermute(x, axis, [(i, (i + by) % size) for i in range(size)])


def mixing_of(weights):
    negated = -weights[1]
    return jnp.stack([jnp.stack([weights[0], negated]), jnp.stack([weights[1], weights[0]])])


def body(greens, noise_weights):
    station_rows = greens.shape[2]
    stations = noise_weights.shape[3]
    device_index = lax.axis_index("stn")
    cycle_length = lax.axis_size("stn")
    mixing = mixing_of(noise_weights)

    def block_product(columns_start, arriving):
        block_rows = arriving.shape[2]
        weights_block = lax.dynamic_slice_in_dim(mixing, columns_start, block_rows, 4)
        return jnp.einsum(
            "ocfin,cfnx->ofix", weights_block, arriving, preferred_element_type=jnp.float32
        )

    half_way = cycle_length // 2
    diagonal = block_product(device_index * station_rows, greens)

    def advance(offset, loop_state):
        running, current = loop_state
        current = passed_along(current, "stn", -1)
        source = (device_index + offset) % cycle_length
        weight = jnp.where(offset == half_way, 1.0, 2.0).astype(jnp.float32)
        running = running + weight * block_product(source * station_rows, current)
        return (running, current)

    summed, current = lax.fori_loop(1, half_way + 1, advance, (diagonal, greens))
    green_real = greens[0].astype(jnp.float32)
    green_imag = greens[1].astype(jnp.float32)
    partial_kernel = (
        jnp.sum(green_real * summed[0] + green_imag * summed[1], axis=(0, 1)) / stations
    )
    raw_kernel = lax.psum(partial_kernel, "stn")
    raw_kernel = lax.psum(raw_kernel, "freq")
    largest = lax.pmax(jnp.max(jnp.abs(raw_kernel)), "pts")
    return raw_kernel / (largest + 1e-06)


def solution(mesh):
    n, cores, n_freq = mesh.shape["stn"], mesh.shape["pts"], mesh.shape["freq"]

    def either(greens, noise_weights):
        _, freqs, rows, points = greens.shape
        fits = n % 4 == 0 and cores == 2 and freqs == 2 and n_freq == 2 and rows % 32 == 0 and points % (2 * LANES) == 0
        if fits:
            return kernel_body(n, n_freq, greens, noise_weights)
        return body(greens, noise_weights)

    in_specs = (P(None, "freq", "stn", "pts"), P(None, "freq", "stn", None))
    return jax.shard_map(either, mesh=mesh, in_specs=in_specs, out_specs=P("pts"), check_vma=False)
```
